256 devices in a mesh: grp: 2 (over z), tp: 128 (over y, x, core).
Axes of the slice: x: 8, y: 8, z: 2, core: 2. Of those that a mesh axis runs over, the one named last changes fastest.
The devices are a block of a 8x8x16 slice.
Arguments:
- hidden: bfloat16 [1024, 16384], P('grp', 'tp'), parts along dimension 0, may hold values from -36 to 36
- norm_gain: float32 [16384], P('tp'), may hold values from 0.3 to 10, as said below
- prefix: int32 [2], P('grp'), parts along dimension 0, may hold values from 0 to 8192
- w_query: bfloat16 [16384, 16384], P(None, 'tp'), may hold values from -0.046875 to 0.046875
- w_kv: bfloat16 [2048, 16384], P('tp'), may hold values from -0.046875 to 0.046875
- w_scale: float32 [18432], P('tp'), may hold values from 0.25 to 4
Outputs:
- queries: bfloat16 [1024, 16384], P('grp', 'tp'), parts along dimension 0
- keys: bfloat16 [1024, 16384], P('grp', 'tp'), parts along dimension 0
- values: bfloat16 [1024, 16384], P('grp', 'tp'), parts along dimension 0
- payload: bfloat16 [1024, 16384], P('grp', 'tp'), parts along dimension 0
- row_scale: float32 [1024], P('grp'), parts along dimension 0
The draws below stay inside these ranges and needn't reach their ends.
There are 2 independent parts, one for each index of `grp`. The reference program is written for one: setup_inputs(seed, part) draws one part's arguments, and reference() takes and returns one part's arrays. A program takes and returns all parts, laid end to end along the dimension named above; an argument that names none is the same for every part. Nothing has to cross between parts.
Inputs may be any that keep to these rules, and one draw needn't show every extreme that they name: `norm_gain`: positive.
All inputs are finite; a program needn't handle non-finite values. Where the reference program divides by a largest or mean magnitude, that divisor is 1e-20 or more.
Results may differ from the reference program's by a relative error of at most 0.012.
Values may be sent and summed in bfloat16 or wider, within the bound.
No kernel may reach another device: no remote copies, remote signals or barrier semaphores. Data moves between devices by JAX's collectives and lax.ppermute only.
A program may use at most 64 MiB of HBM per device.

```python
import math
import jax
import jax.numpy as jnp
from jax import lax

D = 16384
HD = 128
HQ_DEV = 1
KV_COLS_DEV = 8
TOKENS = 512
PREFIX_MAX = 8192
H = 128
KVH = 8
COLS_DEV = 144
N_TP = 128


def draw_norm_gain(key, part):
    columns = jnp.arange(D, dtype=jnp.float32)
    rising = 1.0 + 2.0 * columns / (D - 1)
    rough = jnp.exp(jax.random.uniform(key, (D,), jnp.float32, -0.7, 0.7))
    return rising * rough


def draw_hidden(key, part):
    columns = jnp.arange(D, dtype=jnp.float32) / (D - 1)
    noise = jax.random.normal(jax.random.fold_in(key, 11), (TOKENS, D), jnp.float32)
    noise = jnp.clip(noise, -6.0, 6.0)
    column_scale = 0.5 + columns
    values = noise * column_scale[None, :]
    return values.astype(jnp.bfloat16)


def steps_of(stream_key, shape, split, smallest, top_value):
    factor_of, own = 1.0, jax.random.fold_in(stream_key, 6)
    for position, blocks in split:
        steps = jnp.exp(jax.random.uniform(jax.random.fold_in(own, position), (blocks,), jnp.float32, smallest / len(split), top_value / len(split)))
        factor_of = factor_of * jnp.repeat(steps, shape[position] // blocks).reshape([-1 if axis == position else 1 for axis in range(len(shape))])
    return factor_of


def bell_draw(own_key, dims, scale, bound, shards=(), kind=jnp.bfloat16):
    level = steps_of(own_key, dims, shards, -0.22, 0.18) if shards else 1.0
    array = jax.random.normal(own_key, dims, jnp.float32) * scale * level
    return jnp.minimum(jnp.maximum(array, -bound), bound).astype(kind)


def setup_inputs(seed: int = 0, part: int = 0) -> dict:
    splits = jax.random.split(jax.random.key(seed), 7)
    part_keys = jax.random.split(jax.random.fold_in(splits[6], part), 7)
    return {
        "hidden": draw_hidden(jax.random.fold_in(jax.random.fold_in(splits[6], part), 71), part),
        "norm_gain": draw_norm_gain(jax.random.fold_in(splits[6], 71), part),
        "prefix": jax.random.randint(part_keys[2], (1,), 0, PREFIX_MAX + 1).astype(jnp.int32),
        "w_query": bell_draw(splits[3], (D, H * HD), D ** -0.5, 0.046875, ((1, 128),)),
        "w_kv": bell_draw(splits[4], (N_TP * 2 * KV_COLS_DEV, D), D ** -0.5, 0.046875, ((0, 128),)),
        "w_scale": jnp.clip(jnp.exp(math.log(4.0) - 2.7725887 * jax.random.uniform(splits[5], (N_TP * COLS_DEV,), jnp.float32) ** steps_of(splits[5], (N_TP * COLS_DEV,), ((0, 128),), -0.2, 0.2)), 0.25, 4.0),
    }


norm_eps = 1e-05
tiny_eps = 1e-06
rope_base = 500000.0

def rotate(matrix, positions, offset):
    count, width = matrix.shape
    pairs = matrix.reshape(count, width // 2, 2)
    columns = offset + 2 * jnp.arange(width // 2, dtype=jnp.int32)
    pair_index = (columns % HD // 2).astype(jnp.float32)
    inverse_freq = jnp.power(jnp.float32(rope_base), -(2.0 * pair_index) / HD)
    angle = positions.astype(jnp.float32)[:, None] * inverse_freq[None, :]
    cosine = jnp.cos(angle)
    sine = jnp.sin(angle)
    first = pairs[:, :, 0]
    second = pairs[:, :, 1]
    turned = jnp.stack([first * cosine - second * sine, second * cosine + first * sine], axis=-1)
    return turned.reshape(count, width)

def repeat_heads(matrix):
    heads = matrix.reshape(TOKENS, KVH, 1, HD)
    spread = jnp.broadcast_to(heads, (TOKENS, KVH, N_TP // KVH, HD)).reshape(TOKENS, N_TP, 1, HD)
    spread = jnp.broadcast_to(spread, (TOKENS, N_TP, HQ_DEV, HD))
    return spread.reshape(TOKENS, N_TP * HQ_DEV * HD)

def head_order(blocks):
    pieces = N_TP // KVH
    grouped = blocks.reshape(TOKENS, pieces, KVH, KV_COLS_DEV)
    return jnp.transpose(grouped, (0, 2, 1, 3)).reshape(TOKENS, KVH * HD)

def reference(hidden, norm_gain, prefix, w_query, w_kv, w_scale):
    widened = hidden.astype(jnp.float32)
    square_sum = lax.optimization_barrier(jnp.sum(widened * widened, axis=1))
    inverse = 1.0 / jnp.sqrt(square_sum / D + norm_eps)
    weighted = widened * norm_gain[None, :]
    normed = weighted * inverse[:, None]
    row_scale = lax.optimization_barrier(jnp.max(jnp.abs(normed), axis=1)) + tiny_eps
    payload = (normed / row_scale[:, None]).astype(jnp.bfloat16)
    qwidth = HQ_DEV * HD
    query_raw = jnp.dot(payload, w_query, preferred_element_type=jnp.float32)
    kv_raw = jnp.dot(payload, w_kv.T, preferred_element_type=jnp.float32)
    raw = jnp.concatenate([query_raw.reshape(TOKENS, N_TP, qwidth), kv_raw.reshape(TOKENS, N_TP, 2 * KV_COLS_DEV)], axis=2)
    blocks = raw * row_scale[:, None, None] * w_scale.reshape(1, N_TP, COLS_DEV)
    query_cols = blocks[:, :, :qwidth].reshape(TOKENS, N_TP * qwidth)
    key_cols = head_order(blocks[:, :, qwidth:qwidth + KV_COLS_DEV])
    value_cols = head_order(blocks[:, :, qwidth + KV_COLS_DEV:])
    positions = prefix[0] + jnp.arange(TOKENS, dtype=jnp.int32)
    queries = rotate(query_cols, positions, 0).astype(jnp.bfloat16)
    rotated_keys = rotate(key_cols, positions, 0).astype(jnp.bfloat16)
    value_round = value_cols.astype(jnp.bfloat16)
    keys = repeat_heads(rotated_keys)
    values = repeat_heads(value_round)
    return (queries, keys, values, payload, row_scale)
```

```python
import math

import jax
import jax.numpy as jnp
from jax import lax
from jax.experimental import pallas as pl
from jax.experimental.pallas import tpu as pltpu
from jax.sharding import PartitionSpec as P

HD = 128
KV_COLS_DEV = 8
norm_eps = 1e-05
tiny_eps = 1e-06
rope_base = 500000.0


F32 = jnp.float32
BF16 = jnp.bfloat16
STAT = 16


def split2(v):
    hi = v.astype(BF16)
    return hi, (v - hi.astype(F32)).astype(BF16)


def prep_kernel(core, hidden, gain, keep, send):
    half = keep.shape[0] - STAT
    for out, which in ((keep, core[0]), (send, 1 - core[0])):
        h = hidden[pl.ds(pl.multiple_of(which * half, half), half), :].astype(F32)
        weighted = h * gain[...]
        out[:half, :] = weighted.astype(BF16)
        squares = jnp.sum(jnp.transpose(h * h), axis=0, keepdims=True)
        largest = jnp.max(jnp.transpose(jnp.abs(weighted)), axis=0, keepdims=True)
        rows = []
        for v in (squares, largest):
            for part in split2(v):
                part = part.astype(F32)
                rows += [part[:, :128], part[:, 128:]]
        rows.append(jnp.zeros((STAT - len(rows), 128), F32))
        out[half:, :] = jnp.concatenate(rows, axis=0).astype(BF16)


def combine_kernel(core, keep, recv, out):
    half = keep.shape[0] - STAT
    first = core[0] == 0
    mine, other = keep[:half, :], recv[:half, :]
    left = jnp.where(first, mine.astype(F32), other.astype(F32)).astype(BF16)
    right = jnp.where(first, other.astype(F32), mine.astype(F32)).astype(BF16)
    a, b = keep[half:, :].astype(F32), recv[half:, :].astype(F32)

    def wide(s, r):
        return jnp.concatenate([s[r : r + 1], s[r + 1 : r + 2]], axis=1)

    squares = (wide(a, 0) + wide(a, 2)) + (wide(b, 0) + wide(b, 2))
    largest = jnp.maximum(wide(a, 4) + wide(a, 6), wide(b, 4) + wide(b, 6))
    rows = [p.astype(F32) for v in (squares, largest) for p in split2(v)]
    rows.append(jnp.zeros((STAT - len(rows), rows[0].shape[1]), F32))
    stats = jnp.concatenate(rows, axis=0).astype(BF16)
    for s in range(out.shape[0]):
        out[s, :half, :128] = left
        out[s, :half, 128:] = right
        out[s, half:, :] = stats


def matmul_kernel(m, n, first, table, *refs):
    xs = refs[:m]
    refs = refs[m:]
    wq, wo, kv, ko = refs[:n], refs[n : 2 * n], refs[2 * n : 3 * n], refs[3 * n : 4 * n]
    refs = refs[4 * n :]
    if not first:
        q_in, kv_in, st_in = refs[:3]
        refs = refs[3:]
    q_out, kv_out, st_out = refs
    step = pl.program_id(0)
    half = q_out.shape[0]

    @pl.when(step == 0)
    def _():
        if first:
            q_out[...] = jnp.zeros_like(q_out)
            kv_out[...] = jnp.zeros_like(kv_out)
            st_out[...] = jnp.zeros_like(st_out)
        else:
            q_out[...] = q_in[...]
            kv_out[...] = kv_in[...]
            st_out[...] = st_in[...]

    w = jnp.concatenate([jnp.concatenate([wq[i][0], wo[i][0]], axis=1) for i in range(n)], axis=0)
    wkv = jnp.concatenate(
        [jnp.concatenate([kv[i][...], ko[i][...]], axis=0) for i in range(n)], axis=1
    )
    for k in range(m):

        @pl.when(step == k)
        def _(k=k):
            x = jnp.concatenate([xs[k][i, :half, :] for i in range(n)], axis=1)
            q_out[...] += jnp.dot(x, w, preferred_element_type=F32)
            kv_out[...] += lax.dot_general(
                x, wkv, (((1,), (1,)), ((), ())), preferred_element_type=F32
            )
            squares, largest = st_out[0:1, :], st_out[1:2, :]
            for i in range(n):
                s = xs[k][i, half:, :].astype(F32)
                squares = squares + (s[0:1] + s[1:2])
                largest = jnp.maximum(largest, s[2:3] + s[3:4])
            st_out[0:1, :] = squares
            st_out[1:2, :] = largest


def matmul(table, xs, wq, wo, kv, ko, acc):
    m, n = len(xs), xs[0].shape[0]
    half = xs[0].shape[1] - STAT
    kb = xs[0].shape[2]
    first = acc is None
    full = lambda a: pl.BlockSpec(a.shape, lambda s, t, r=len(a.shape): (0,) * r)
    in_specs = [full(x) for x in xs]
    for _ in range(2):
        in_specs += [
            pl.BlockSpec((1, kb, wq.shape[2]), lambda s, t, i=i: (t[s * n + i], 0, 0))
            for i in range(n)
        ]
    for _ in range(2):
        in_specs += [
            pl.BlockSpec((kv.shape[0], kb), lambda s, t, i=i: (0, t[s * n + i])) for i in range(n)
        ]
    out_shape = (
        jax.ShapeDtypeStruct((half, 2 * wq.shape[2]), F32),
        jax.ShapeDtypeStruct((half, 2 * kv.shape[0]), F32),
        jax.ShapeDtypeStruct((8, half), F32),
    )
    args = [*xs, *([wq] * n), *([wo] * n), *([kv] * n), *([ko] * n)]
    aliases = {}
    if not first:
        aliases = {1 + len(args) + i: i for i in range(3)}
        in_specs += [full(a) for a in acc]
        args += list(acc)
    flops = 2 * m * n * kb * half * 288
    return pl.pallas_call(
        lambda *refs: matmul_kernel(m, n, first, *refs),
        out_shape=out_shape,
        grid_spec=pltpu.PrefetchScalarGridSpec(
            num_scalar_prefetch=1,
            grid=(m,),
            in_specs=in_specs,
            out_specs=tuple(full(o) for o in out_shape),
        ),
        input_output_aliases=aliases,
        cost_estimate=pl.CostEstimate(
            flops=flops, bytes_accessed=m * n * kb * (half + 288) * 2, transcendentals=0
        ),
    )(table, *args)


def turn(v, cosine, sine):
    lane = lax.broadcasted_iota(jnp.int32, v.shape, 1)
    width = v.shape[1]
    swapped = jnp.where(
        lane % 2 == 0, -pltpu.roll(v, width - 1, 1), pltpu.roll(v, 1, 1)
    )
    return v * cosine + swapped * sine


def columns_of(row, width):
    return jnp.transpose(jnp.broadcast_to(row, (width, row.shape[1])))


def finish_kernel(d, core, q, kv, st, wscale, cosine, sine, kvscale, kcos, ksin, mine, msg, kvt):
    half = q.shape[0]
    squares, largest = st[0:1, :], st[1:2, :]
    inverse = 1.0 / jnp.sqrt(squares / d + norm_eps)
    inv = columns_of(inverse, 128)
    mine[...] = turn(q[:, :128] * inv * wscale[...], cosine[...], sine[...]).astype(BF16)
    msg[:half, :] = q[:, 128:] * inv
    msg[half:, :] = jnp.concatenate(
        [
            squares[:, :128],
            squares[:, 128:],
            largest[:, :128],
            largest[:, 128:],
            jnp.zeros((4, 128), F32),
        ],
        axis=0,
    )
    t = jnp.transpose(kv[...]) * inverse
    first = core[0] == 0
    mk, mv, ok, ov = t[0:8], t[8:16], t[16:24], t[24:32]
    a = jnp.concatenate([jnp.where(first, mk, ok), jnp.where(first, ok, mk)], axis=0)
    b = jnp.concatenate([jnp.where(first, mv, ov), jnp.where(first, ov, mv)], axis=0)
    a = a * kvscale[:16, :]
    b = b * kvscale[16:, :]
    row = lax.broadcasted_iota(jnp.int32, a.shape, 0)
    swapped = jnp.where(row % 2 == 0, -pltpu.roll(a, a.shape[0] - 1, 0), pltpu.roll(a, 1, 0))
    a = a * kcos[...] + swapped * ksin[...]
    both = jnp.concatenate([a, b], axis=0).astype(BF16)
    for s in range(kvt.shape[0]):
        kvt[s] = both


def output_kernel(
    d, core, mine, msg, st, kvr, hidden, gain, wscale, cosine, sine, queries, keys, values, payload, scale
):
    half = mine.shape[0]
    c = core[0]
    own = pl.ds(pl.multiple_of(c * half, half), half)
    far = pl.ds(pl.multiple_of((1 - c) * half, half), half)
    queries[own, :] = mine[...]
    queries[far, :] = turn(msg[:half, :] * wscale[...], cosine[...], sine[...]).astype(BF16)
    wide = lambda r: jnp.concatenate([msg[half + r : half + r + 1], msg[half + r + 1 : half + r + 2]], axis=1)
    for rows, squares, largest, place in (
        (own, st[0:1, :], st[1:2, :], c),
        (far, wide(0), wide(2), 1 - c),
    ):
        inverse = 1.0 / jnp.sqrt(squares / d + norm_eps)
        row_scale = largest * inverse + tiny_eps
        scale[pl.ds(place, 1), :] = row_scale
        inv = columns_of(inverse, 128)
        rs = columns_of(row_scale, 128)
        normed = hidden[rows, :].astype(F32) * gain[...] * inv
        payload[rows, :] = (normed / rs).astype(BF16)
    pieces = kvr.shape[0] // 2
    for part in range(2):
        at = slice(part * half, (part + 1) * half)
        for out, lo in ((keys, 0), (values, 16)):
            t = jnp.concatenate(
                [kvr[2 * i + part, lo : lo + 16, :] for i in range(pieces)], axis=0
            )
            out[at, :] = jnp.transpose(t.astype(F32)).astype(BF16)


def call(kernel, out_shape, core, *args, flops=0):
    return pl.pallas_call(
        kernel,
        out_shape=out_shape,
        in_specs=[pl.BlockSpec(memory_space=pltpu.SMEM)]
        + [pl.BlockSpec(memory_space=pltpu.VMEM)] * len(args),
        cost_estimate=pl.CostEstimate(flops=flops or 10**8, bytes_accessed=10**6, transcendentals=0),
    )(core, *args)


def solution(mesh):
    tp = mesh.shape["tp"]
    side = math.isqrt(tp // 2)
    row = 2 * side

    def index(y, x, c):
        return (y % side) * row + (x % side) * 2 + c

    everyone = [(y, x, c) for y in range(side) for x in range(side) for c in range(2)]
    to_partner = [(index(y, x, c), index(y, x, 1 - c)) for y, x, c in everyone]
    to_row = [(p * side + g, g * row + p) for p in range(row) for g in range(side)]
    first_groups = [[index(y, x, 0) for x in range(side)] for y in range(side)]
    first_groups += [[index(y, x, 1) for y in range(side)] for x in range(side)]
    rows = [[y * row + i for i in range(row)] for y in range(side)]

    def second(v, s):
        pairs = [
            (index(y, x, c), index(y + s, x, c) if c == 0 else index(y, x + s, c))
            for y, x, c in everyone
        ]
        return lax.ppermute(v, "tp", pairs)

    def swap(v):
        return lax.ppermute(v, "tp", to_partner)

    def local(hidden, norm_gain, prefix, w_query, w_kv, w_scale):
        count, width = hidden.shape
        d = width * tp
        half = count // 2
        me = lax.axis_index("tp")
        core = me % 2
        x = (me // 2) % side
        y = me // row
        core1 = core[None].astype(jnp.int32)
        gain = norm_gain[None, :]

        kv_mine = lax.ppermute(w_kv, "tp", to_row)
        kvs_mine = lax.ppermute(w_scale[None, HD:], "tp", to_row)
        wq_other = swap(w_query)

        blk = jax.ShapeDtypeStruct((half + STAT, width), BF16)
        keep, send = call(prep_kernel, (blk, blk), core1, hidden, gain)
        recv = swap(send)
        slots = call(
            combine_kernel,
            jax.ShapeDtypeStruct((side, half + STAT, 2 * width), BF16),
            core1,
            keep,
            recv,
        )
        gathered = lax.all_to_all(
            slots, "tp", split_axis=0, concat_axis=0, tiled=False, axis_index_groups=first_groups
        )
        kv_other = swap(kv_mine)
        kvs_other = swap(kvs_mine)

        n = side // 2
        lows, highs = gathered[:n], gathered[n:]
        lane = jnp.arange(n, dtype=jnp.int32)

        def blocks_of(s, k):
            a = (jnp.where(core == 0, y, x) - s) % side
            b = k * n + lane
            return jnp.where(core == 0, a * side + b, b * side + a)

        wq3 = w_query.reshape(-1, 2 * width, w_query.shape[1])
        wo3 = wq_other.reshape(wq3.shape)

        def mm(acc, items):
            table = jnp.concatenate([blocks_of(s, k) for s, k, _ in items]).astype(jnp.int32)
            return matmul(table, [v for _, _, v in items], wq3, wo3, kv_mine, kv_other, acc)

        up = [lows, highs]
        down = [lows, highs]
        arrivals = [(0, 0, lows), (0, 1, highs)]
        acc = None
        for r in range(1, side // 2):
            up = [second(v, 1) for v in up]
            down = [second(v, -1) for v in down]
            acc = mm(acc, arrivals)
            arrivals = [(r, k, v) for k, v in enumerate(up)] + [
                (-r, k, v) for k, v in enumerate(down)
            ]
        r = side // 2
        last = [(r, 0, second(up[0], 1)), (-r, 1, second(down[1], -1))]
        acc = mm(acc, arrivals)
        acc = mm(acc, last)

        positions = (prefix[0] + jnp.arange(count, dtype=jnp.int32)).astype(F32)
        pos_own = lax.dynamic_slice_in_dim(positions, core * half, half)
        pos_far = lax.dynamic_slice_in_dim(positions, (1 - core) * half, half)

        def freq(columns):
            pair = (columns % HD // 2).astype(F32)
            return jnp.power(F32(rope_base), -(2.0 * pair) / HD)

        fq = freq(jnp.arange(HD, dtype=jnp.int32))
        ang_own = pos_own[:, None] * fq[None, :]
        ang_far = pos_far[:, None] * fq[None, :]
        fk = freq(x * 2 * KV_COLS_DEV + jnp.arange(2 * KV_COLS_DEV, dtype=jnp.int32))
        ang_k = fk[:, None] * pos_own[None, :]
        ordered = jnp.where(
            core == 0,
            jnp.concatenate([kvs_mine, kvs_other], 0),
            jnp.concatenate([kvs_other, kvs_mine], 0),
        )
        kvscale = jnp.broadcast_to(
            jnp.concatenate(
                [ordered[:, :KV_COLS_DEV].reshape(-1), ordered[:, KV_COLS_DEV:].reshape(-1)]
            )[:, None],
            (4 * KV_COLS_DEV, half),
        )
        qscale = w_scale[None, :HD]

        mine, msg, kvt = call(
            lambda *r: finish_kernel(d, *r),
            (
                jax.ShapeDtypeStruct((half, HD), BF16),
                jax.ShapeDtypeStruct((half + 8, HD), F32),
                jax.ShapeDtypeStruct((row, 4 * KV_COLS_DEV, half), BF16),
            ),
            core1,
            *acc,
            qscale,
            jnp.cos(ang_own),
            jnp.sin(ang_own),
            kvscale,
            jnp.cos(ang_k),
            jnp.sin(ang_k),
        )
        far = swap(msg)
        kvr = lax.all_to_all(
            kvt, "tp", split_axis=0, concat_axis=0, tiled=False, axis_index_groups=rows
        )
        out = jax.ShapeDtypeStruct((count, HD), BF16)
        queries, keys, values, payload, scale = call(
            lambda *r: output_kernel(d, *r),
            (out, out, out, out, jax.ShapeDtypeStruct((2, half), F32)),
            core1,
            mine,
            far,
            acc[2],
            kvr,
            hidden,
            gain,
            qscale,
            jnp.cos(ang_far),
            jnp.sin(ang_far),
        )
        return queries, keys, values, payload, scale.reshape(count)

    return jax.shard_map(
        local,
        mesh=mesh,
        in_specs=(P("grp", "tp"), P("tp"), P("grp"), P(None, "tp"), P("tp", None), P("tp")),
        out_specs=(P("grp", "tp"), P("grp", "tp"), P("grp", "tp"), P("grp", "tp"), P("grp")),
        check_vma=False,
    )
```

```python
import math

import jax
import jax.numpy as jnp
from jax import lax
from jax.experimental import pallas as pl
from jax.experimental.pallas import tpu as pltpu
from jax.sharding import PartitionSpec as P


HD = 128
KV_COLS_DEV = 8
norm_eps = 1e-05
tiny_eps = 1e-06
rope_base = 500000.0

VMEM = 24 * 2**20

F32 = jnp.float32
BF16 = jnp.bfloat16
STAT = 16


def split2(v):
    hi = v.astype(BF16)
    return hi, (v - hi.astype(F32)).astype(BF16)


def prep_kernel(core, hidden, gain, keep, send):
    half = keep.shape[0] - STAT
    for out, which in ((keep, core[0]), (send, 1 - core[0])):
        h = hidden[pl.ds(pl.multiple_of(which * half, half), half), :].astype(F32)
        weighted = h * gain[...]
        out[:half, :] = weighted.astype(BF16)
        squares = jnp.sum(jnp.transpose(h * h), axis=0, keepdims=True)
        largest = jnp.max(jnp.transpose(jnp.abs(weighted)), axis=0, keepdims=True)
        rows = []
        for v in (squares, largest):
            for part in split2(v):
                part = part.astype(F32)
                rows += [part[:, :128], part[:, 128:]]
        rows.append(jnp.zeros((STAT - len(rows), 128), F32))
        out[half:, :] = jnp.concatenate(rows, axis=0).astype(BF16)


def combine_kernel(core, keep, recv, out):
    half = keep.shape[0] - STAT
    first = core[0] == 0
    mine, other = keep[:half, :], recv[:half, :]
    left = jnp.where(first, mine.astype(F32), other.astype(F32)).astype(BF16)
    right = jnp.where(first, other.astype(F32), mine.astype(F32)).astype(BF16)
    a, b = keep[half:, :].astype(F32), recv[half:, :].astype(F32)

    def wide(s, r):
        return jnp.concatenate([s[r : r + 1], s[r + 1 : r + 2]], axis=1)

    squares = (wide(a, 0) + wide(a, 2)) + (wide(b, 0) + wide(b, 2))
    largest = jnp.maximum(wide(a, 4) + wide(a, 6), wide(b, 4) + wide(b, 6))
    rows = [p.astype(F32) for v in (squares, largest) for p in split2(v)]
    rows.append(jnp.zeros((STAT - len(rows), rows[0].shape[1]), F32))
    stats = jnp.concatenate(rows, axis=0).astype(BF16)
    for s in range(out.shape[0]):
        out[s, :half, :128] = left
        out[s, :half, 128:] = right
        out[s, half:, :] = stats


def weights_kernel(core, wq, wo, kv, ko, w_all, kv_all, w_buf, kv_buf, sems):
    n = w_buf.shape[0]
    kb = w_buf.shape[1]
    hw = wq.shape[2]
    rows = kv.shape[0]
    side = math.isqrt(n)

    def fetches(i):
        b = jnp.where(core[0] == 0, i, (i % side) * side + i // side)
        at = pl.ds(pl.multiple_of(b * kb, kb), kb)
        return (
            pltpu.make_async_copy(wq.at[b], w_buf.at[i, :, pl.ds(0, hw)], sems.at[0, i]),
            pltpu.make_async_copy(wo.at[b], w_buf.at[i, :, pl.ds(hw, hw)], sems.at[1, i]),
            pltpu.make_async_copy(kv.at[:, at], kv_buf.at[i, pl.ds(0, rows), :], sems.at[2, i]),
            pltpu.make_async_copy(ko.at[:, at], kv_buf.at[i, pl.ds(rows, rows), :], sems.at[3, i]),
        )

    def stores(i):
        return (
            pltpu.make_async_copy(w_buf.at[i], w_all.at[i], sems.at[4, i]),
            pltpu.make_async_copy(kv_buf.at[i], kv_all.at[i], sems.at[5, i]),
        )

    @pl.loop(0, n)
    def _(i):
        for c in fetches(i):
            c.start()

    @pl.loop(0, n)
    def _(i):
        for c in fetches(i):
            c.wait()
        for c in stores(i):
            c.start()

    @pl.loop(0, n)
    def _(i):
        for c in stores(i):
            c.wait()


def arrange_weights(core, wq, wo, kv, ko):
    n, kb, hw = wq.shape
    hbm = pl.BlockSpec(memory_space=pltpu.HBM)
    out_shape = (
        jax.ShapeDtypeStruct((n, kb, 2 * hw), BF16),
        jax.ShapeDtypeStruct((n, 2 * kv.shape[0], kb), BF16),
    )
    return pl.pallas_call(
        weights_kernel,
        out_shape=out_shape,
        in_specs=[pl.BlockSpec(memory_space=pltpu.SMEM), hbm, hbm, hbm, hbm],
        out_specs=(hbm, hbm),
        scratch_shapes=[pltpu.VMEM(o.shape, o.dtype) for o in out_shape]
        + [pltpu.SemaphoreType.DMA((6, n))],
        compiler_params=pltpu.CompilerParams(vmem_limit_bytes=VMEM),
        cost_estimate=pl.CostEstimate(flops=10**9, bytes_accessed=2 * 10**7, transcendentals=0),
    )(core, wq, wo, kv, ko)


def high_kernel(gathered, high):
    n = gathered.shape[0] // 2
    half = gathered.shape[1] - STAT
    squares, largest = 0.0, 0.0
    for i in range(2 * n):
        s = gathered[i, half:, :].astype(F32)
        squares = squares + (s[0:1] + s[1:2])
        largest = jnp.maximum(largest, s[2:3] + s[3:4])
        if i >= n:
            high[(i - n) * half : (i - n + 1) * half, :] = gathered[i, :half, :]
    rows = [p.astype(F32) for v in (squares, largest) for p in split2(v)]
    rows.append(jnp.zeros((STAT - len(rows), rows[0].shape[1]), F32))
    high[n * half :, :] = jnp.concatenate(rows, axis=0).astype(BF16)


def kv_rows(xs, kvs, kv_in, st_in):
    half = kv_in.shape[1]
    total = kv_in[...]
    squares, largest = st_in[0:1, :], st_in[1:2, :]
    for x, w in zip(xs, kvs):
        n = w.shape[0]
        for i in range(n):
            total = total + lax.dot_general(
                w[i],
                x[i * half : (i + 1) * half, :],
                (((1,), (1,)), ((), ())),
                preferred_element_type=F32,
            )
        if x.shape[0] > n * half:
            s = x[n * half :, :].astype(F32)
            squares = squares + (s[0:1] + s[1:2])
            largest = jnp.maximum(largest, s[2:3] + s[3:4])
    return total, squares, largest


def q_sum(xs, ws, q_in):
    half = q_in.shape[0]
    total = q_in[...]
    for x, w in zip(xs, ws):
        for i in range(w.shape[0]):
            total = total + jnp.dot(
                x[i * half : (i + 1) * half, :], w[i], preferred_element_type=F32
            )
    return total


def fetch(table, m, pairs, sems):
    copies = []
    for i in range(m):
        for j, (whole, buf) in enumerate(pairs):
            n = buf.shape[1]
            at = pl.ds(pl.multiple_of(table[i] * n, n), n)
            copies.append(pltpu.make_async_copy(whole.at[at], buf.at[i], sems.at[j, i]))
    for c in copies:
        c.start()
    for c in copies:
        c.wait()


def matmul_kernel(m, table, *refs):
    xs, w_all, kv_all = refs[:m], refs[m], refs[m + 1]
    q_in, kv_in, st_in, q_out, kv_out, st_out, w_buf, kv_buf, sems = refs[m + 2 :]
    fetch(table, m, ((w_all, w_buf), (kv_all, kv_buf)), sems)
    ws, kvs = [w_buf.at[i] for i in range(m)], [kv_buf.at[i] for i in range(m)]
    q_out[...] = q_sum(xs, ws, q_in)
    total, squares, largest = kv_rows(xs, kvs, kv_in, st_in)
    kv_out[...] = total
    st_out[0:1, :] = squares
    st_out[1:2, :] = largest


def arrivals_call(kernel, out_shape, table, xs, weights, rest, flops, aliases=None):
    m = len(xs)
    n = xs[0].shape[0] // xs[0].shape[1]
    hbm = pl.BlockSpec(memory_space=pltpu.HBM)
    vmem = pl.BlockSpec(memory_space=pltpu.VMEM)
    smem = pl.BlockSpec(memory_space=pltpu.SMEM)
    specs = [smem] + [vmem] * m + [hbm] * len(weights)
    specs += [smem if a.dtype == jnp.int32 else vmem for a in rest]
    return pl.pallas_call(
        kernel,
        out_shape=out_shape,
        in_specs=specs,
        out_specs=tuple(vmem for _ in out_shape),
        scratch_shapes=[pltpu.VMEM((m, n) + w.shape[1:], w.dtype) for w in weights]
        + [pltpu.SemaphoreType.DMA((len(weights), m))],
        input_output_aliases=aliases or {},
        compiler_params=pltpu.CompilerParams(vmem_limit_bytes=VMEM),
        cost_estimate=pl.CostEstimate(flops=flops, bytes_accessed=10**6, transcendentals=0),
    )(table, *xs, *weights, *rest)


def matmul(table, xs, w_all, kv_all, acc):
    m = len(xs)
    out_shape = tuple(jax.ShapeDtypeStruct(a.shape, a.dtype) for a in acc)
    return arrivals_call(
        lambda *refs: matmul_kernel(m, *refs),
        out_shape,
        table,
        xs,
        (w_all, kv_all),
        acc,
        2 * m * xs[0].shape[0] * xs[0].shape[1] * 288,
        {3 + m + i: i for i in range(3)},
    )


def last_kv_kernel(d, m, table, *refs):
    xs, kv_all = refs[:m], refs[m]
    core, kv_in, st_in, kvscale, kcos, ksin, kvt, st_out, kv_buf, sems = refs[m + 1 :]
    fetch(table, m, ((kv_all, kv_buf),), sems)
    t, squares, largest = kv_rows(xs, [kv_buf.at[i] for i in range(m)], kv_in, st_in)
    st_out[0:1, :] = squares
    st_out[1:2, :] = largest
    t = t * (1.0 / jnp.sqrt(squares / d + norm_eps))
    first = core[0] == 0
    mk, mv, ok, ov = t[0:8], t[8:16], t[16:24], t[24:32]
    a = jnp.concatenate([jnp.where(first, mk, ok), jnp.where(first, ok, mk)], axis=0)
    b = jnp.concatenate([jnp.where(first, mv, ov), jnp.where(first, ov, mv)], axis=0)
    a = a * kvscale[:16, :]
    b = b * kvscale[16:, :]
    row = lax.broadcasted_iota(jnp.int32, a.shape, 0)
    swapped = jnp.where(row % 2 == 0, -pltpu.roll(a, a.shape[0] - 1, 0), pltpu.roll(a, 1, 0))
    a = a * kcos[...] + swapped * ksin[...]
    both = jnp.concatenate([a, b], axis=0).astype(BF16)
    for s in range(kvt.shape[0]):
        kvt[s] = both


def last_kv(d, copies, table, core, xs, kv_all, kv, st, kvscale, kcos, ksin):
    m = len(xs)
    out_shape = (
        jax.ShapeDtypeStruct((copies,) + kv.shape, BF16),
        jax.ShapeDtypeStruct(st.shape, F32),
    )
    return arrivals_call(
        lambda *refs: last_kv_kernel(d, m, *refs),
        out_shape,
        table,
        xs,
        (kv_all,),
        [core, kv, st, kvscale, kcos, ksin],
        10**9,
    )


def last_q_kernel(d, m, table, *refs):
    xs, w_all = refs[:m], refs[m]
    q_in, st, wscale, cosine, sine, mine, msg, w_buf, sems = refs[m + 1 :]
    fetch(table, m, ((w_all, w_buf),), sems)
    q = q_sum(xs, [w_buf.at[i] for i in range(m)], q_in)
    half = q.shape[0]
    squares, largest = st[0:1, :], st[1:2, :]
    inv = columns_of(1.0 / jnp.sqrt(squares / d + norm_eps), 128)
    mine[...] = turn(q[:, :128] * inv * wscale[...], cosine[...], sine[...]).astype(BF16)
    msg[:half, :] = q[:, 128:] * inv
    msg[half:, :] = jnp.concatenate(
        [
            squares[:, :128],
            squares[:, 128:],
            largest[:, :128],
            largest[:, 128:],
            jnp.zeros((4, 128), F32),
        ],
        axis=0,
    )


def last_q(d, table, xs, w_all, q, st, wscale, cosine, sine):
    m = len(xs)
    half = q.shape[0]
    out_shape = (
        jax.ShapeDtypeStruct((half, HD), BF16),
        jax.ShapeDtypeStruct((half + 8, HD), F32),
    )
    return arrivals_call(
        lambda *refs: last_q_kernel(d, m, *refs),
        out_shape,
        table,
        xs,
        (w_all,),
        [q, st, wscale, cosine, sine],
        10**9,
    )


def turn(v, cosine, sine):
    lane = lax.broadcasted_iota(jnp.int32, v.shape, 1)
    width = v.shape[1]
    swapped = jnp.where(
        lane % 2 == 0, -pltpu.roll(v, width - 1, 1), pltpu.roll(v, 1, 1)
    )
    return v * cosine + swapped * sine


def columns_of(row, width):
    return jnp.transpose(jnp.broadcast_to(row, (width, row.shape[1])))


def token_kernel(d, core, mine, msg, st, hidden, gain, wscale, cosine, sine, queries, payload, scale):
    half = mine.shape[0]
    c = core[0]
    own = pl.ds(pl.multiple_of(c * half, half), half)
    far = pl.ds(pl.multiple_of((1 - c) * half, half), half)
    queries[own, :] = mine[...]
    queries[far, :] = turn(msg[:half, :] * wscale[...], cosine[...], sine[...]).astype(BF16)
    wide = lambda r: jnp.concatenate(
        [msg[half + r : half + r + 1], msg[half + r + 1 : half + r + 2]], axis=1
    )
    for rows, squares, largest, place in (
        (own, st[0:1, :], st[1:2, :], c),
        (far, wide(0), wide(2), 1 - c),
    ):
        inverse = 1.0 / jnp.sqrt(squares / d + norm_eps)
        row_scale = largest * inverse + tiny_eps
        scale[pl.ds(2 * place, 1), :] = row_scale[:, :128]
        scale[pl.ds(2 * place + 1, 1), :] = row_scale[:, 128:]
        inv = columns_of(inverse, 128)
        rs = columns_of(row_scale, 128)
        normed = hidden[rows, :].astype(F32) * gain[...] * inv
        payload[rows, :] = (normed / rs).astype(BF16)


def head_kernel(core, kvr, keys, values):
    half = kvr.shape[2]
    pieces = kvr.shape[0] // 2
    for part in range(2):
        at = slice(part * half, (part + 1) * half)
        for out, lo in ((keys, 0), (values, 16)):
            t = jnp.concatenate(
                [kvr[2 * i + part, lo : lo + 16, :] for i in range(pieces)], axis=0
            )
            out[at, :] = jnp.transpose(t.astype(F32)).astype(BF16)


def call(kernel, out_shape, core, *args, flops=0):
    return pl.pallas_call(
        kernel,
        out_shape=out_shape,
        in_specs=[pl.BlockSpec(memory_space=pltpu.SMEM)]
        + [pl.BlockSpec(memory_space=pltpu.VMEM)] * len(args),
        compiler_params=pltpu.CompilerParams(vmem_limit_bytes=VMEM),
        cost_estimate=pl.CostEstimate(flops=flops or 10**8, bytes_accessed=10**6, transcendentals=0),
    )(core, *args)


def solution(mesh):
    tp = mesh.shape["tp"]
    side = math.isqrt(tp // 2)
    row = 2 * side

    def index(y, x, c):
        return (y % side) * row + (x % side) * 2 + c

    everyone = [(y, x, c) for y in range(side) for x in range(side) for c in range(2)]
    to_partner = [(index(y, x, c), index(y, x, 1 - c)) for y, x, c in everyone]
    to_row = [(p * side + g, g * row + p) for p in range(row) for g in range(side)]
    first_groups = [[index(y, x, 0) for x in range(side)] for y in range(side)]
    first_groups += [[index(y, x, 1) for y in range(side)] for x in range(side)]
    rows = [[y * row + i for i in range(row)] for y in range(side)]

    def second(v, s):
        pairs = [
            (index(y, x, c), index(y + s, x, c) if c == 0 else index(y, x + s, c))
            for y, x, c in everyone
        ]
        return lax.ppermute(v, "tp", pairs)

    def swap(v):
        return lax.ppermute(v, "tp", to_partner)

    def body(hidden, norm_gain, prefix, w_query, w_kv, w_scale):
        count, width = hidden.shape
        d = width * tp
        half = count // 2
        me = lax.axis_index("tp")
        core = me % 2
        x = (me // 2) % side
        y = me // row
        core1 = core[None].astype(jnp.int32)
        gain = norm_gain[None, :]

        kv_mine = lax.ppermute(w_kv, "tp", to_row)
        wq_other = swap(w_query)
        kvs_mine = lax.ppermute(w_scale[None, HD:], "tp", to_row)

        blk = jax.ShapeDtypeStruct((half + STAT, width), BF16)
        keep, send = call(prep_kernel, (blk, blk), core1, hidden, gain)
        recv = swap(send)
        slots = call(
            combine_kernel,
            jax.ShapeDtypeStruct((side, half + STAT, 2 * width), BF16),
            core1,
            keep,
            recv,
        )
        gathered = lax.all_to_all(
            slots, "tp", split_axis=0, concat_axis=0, tiled=False, axis_index_groups=first_groups
        )
        kv_other = swap(kv_mine)
        kvs_other = swap(kvs_mine)
        w_all, kv_all = arrange_weights(
            core1, w_query.reshape(-1, 2 * width, HD), wq_other.reshape(-1, 2 * width, HD), kv_mine, kv_other
        )

        positions = (prefix[0] + jnp.arange(count, dtype=jnp.int32)).astype(F32)
        pos_own = lax.dynamic_slice_in_dim(positions, core * half, half)
        pos_far = lax.dynamic_slice_in_dim(positions, (1 - core) * half, half)

        def freq(columns):
            pair = (columns % HD // 2).astype(F32)
            return jnp.power(F32(rope_base), -(2.0 * pair) / HD)

        fq = freq(jnp.arange(HD, dtype=jnp.int32))
        ang_own = pos_own[:, None] * fq[None, :]
        ang_far = pos_far[:, None] * fq[None, :]
        fk = freq(x * 2 * KV_COLS_DEV + jnp.arange(2 * KV_COLS_DEV, dtype=jnp.int32))
        ang_k = fk[:, None] * pos_own[None, :]
        ordered = jnp.where(
            core == 0,
            jnp.concatenate([kvs_mine, kvs_other], 0),
            jnp.concatenate([kvs_other, kvs_mine], 0),
        )
        kvscale = jnp.broadcast_to(
            jnp.concatenate(
                [ordered[:, :KV_COLS_DEV].reshape(-1), ordered[:, KV_COLS_DEV:].reshape(-1)]
            )[:, None],
            (4 * KV_COLS_DEV, half),
        )
        qscale = w_scale[None, :HD]
        tables = (
            jnp.cos(ang_own),
            jnp.sin(ang_own),
            jnp.cos(ang_far),
            jnp.sin(ang_far),
            jnp.cos(ang_k),
            jnp.sin(ang_k),
            kvscale,
        )
        zeros = (
            jnp.zeros((half, 2 * HD), F32),
            jnp.zeros((4 * KV_COLS_DEV, half), F32),
            jnp.zeros((8, half), F32),
        )
        coord = jnp.where(core == 0, y, x)

        def table_of(items):
            return jnp.stack([(coord - s) % side * 2 + k for s, k, _ in items]).astype(jnp.int32)

        shifts = [(s, k) for s in range(side) for k in range(2)]
        places = {sk: table_of([(*sk, None)]) for sk in shifts}
        gathered, w_all, kv_all, tables, zeros, places = lax.optimization_barrier(
            (gathered, w_all, kv_all, tables, zeros, places)
        )
        cos_own, sin_own, cos_far, sin_far, cos_k, sin_k, kvscale = tables

        n = side // 2
        low = gathered[:n, :half].reshape(n * half, -1)
        high = pl.pallas_call(
            high_kernel,
            out_shape=jax.ShapeDtypeStruct((n * half + STAT, gathered.shape[2]), BF16),
            compiler_params=pltpu.CompilerParams(vmem_limit_bytes=VMEM),
            cost_estimate=pl.CostEstimate(flops=10**8, bytes_accessed=10**6, transcendentals=0),
        )(gathered)

        def mm(acc, items):
            table = jnp.concatenate([places[s % side, k] for s, k, _ in items])
            return matmul(table, [v for _, _, v in items], w_all, kv_all, acc)

        up = [second(low, 1), second(high, 1)]
        down = [second(low, -1), second(high, -1)]
        acc = mm(zeros, [(0, 0, low), (0, 1, high)])
        last_round = side // 2
        for r in range(1, last_round):
            for k in range(2):
                items = [(r, k, up[k]), (-r, k, down[k])]
                up[k], down[k], acc = lax.optimization_barrier((up[k], down[k], acc))
                if r + 1 < last_round:
                    up[k], down[k] = second(up[k], 1), second(down[k], -1)
                elif k == 0:
                    up[k] = second(up[k], 1)
                else:
                    down[k] = second(down[k], -1)
                acc = mm(acc, items)
        items = [(last_round, 0, up[0]), (-last_round, 1, down[1])]
        xs = [v for _, _, v in items]
        table = jnp.concatenate([places[s % side, k] for s, k, _ in items])
        kvt, st = last_kv(
            d, row, table, core1, xs, kv_all, acc[1], acc[2], kvscale, cos_k, sin_k
        )
        kvr = lax.all_to_all(
            kvt, "tp", split_axis=0, concat_axis=0, tiled=False, axis_index_groups=rows
        )
        mine, msg = last_q(d, table, xs, w_all, acc[0], st, qscale, cos_own, sin_own)
        far = swap(msg)
        out = jax.ShapeDtypeStruct((count, HD), BF16)
        queries, payload, scale = call(
            lambda *r: token_kernel(d, *r),
            (out, out, jax.ShapeDtypeStruct((count // HD, HD), F32)),
            core1,
            mine,
            far,
            st,
            hidden,
            gain,
            qscale,
            cos_far,
            sin_far,
        )
        keys, values = call(head_kernel, (out, out), core1, kvr)
        return queries, keys, values, payload, scale.reshape(count)

    return jax.shard_map(
        body,
        mesh=mesh,
        in_specs=(P("grp", "tp"), P("tp"), P("grp"), P(None, "tp"), P("tp", None), P("tp")),
        out_specs=(P("grp", "tp"), P("grp", "tp"), P("grp", "tp"), P("grp", "tp"), P("grp")),
        check_vma=False,
    )
```

```python
import math

import jax
import jax.numpy as jnp
from jax import lax
from jax.experimental import pallas as pl
from jax.experimental.pallas import tpu as pltpu
from jax.sharding import PartitionSpec as P


HD = 128
KV_COLS_DEV = 8
norm_eps = 1e-05
tiny_eps = 1e-06
rope_base = 500000.0

VMEM = 24 * 2**20

F32 = jnp.float32
BF16 = jnp.bfloat16
STAT = 16


def split2(v):
    hi = v.astype(BF16)
    return hi, (v - hi.astype(F32)).astype(BF16)


def prep_kernel(core, hidden, gain, keep, send):
    half = keep.shape[0] - STAT
    for out, which in ((keep, core[0]), (send, 1 - core[0])):
        h = hidden[pl.ds(pl.multiple_of(which * half, half), half), :].astype(F32)
        weighted = h * gain[...]
        out[:half, :] = weighted.astype(BF16)
        squares = jnp.sum(jnp.transpose(h * h), axis=0, keepdims=True)
        largest = jnp.max(jnp.transpose(jnp.abs(weighted)), axis=0, keepdims=True)
        rows = []
        for v in (squares, largest):
            for part in split2(v):
                part = part.astype(F32)
                rows += [part[:, :128], part[:, 128:]]
        rows.append(jnp.zeros((STAT - len(rows), 128), F32))
        out[half:, :] = jnp.concatenate(rows, axis=0).astype(BF16)


def combine_kernel(core, keep, recv, out):
    half = keep.shape[0] - STAT
    first = core[0] == 0
    mine, other = keep[:half, :], recv[:half, :]
    left = jnp.where(first, mine.astype(F32), other.astype(F32)).astype(BF16)
    right = jnp.where(first, other.astype(F32), mine.astype(F32)).astype(BF16)
    a, b = keep[half:, :].astype(F32), recv[half:, :].astype(F32)

    def wide(s, r):
        return jnp.concatenate([s[r : r + 1], s[r + 1 : r + 2]], axis=1)

    squares = (wide(a, 0) + wide(a, 2)) + (wide(b, 0) + wide(b, 2))
    largest = jnp.maximum(wide(a, 4) + wide(a, 6), wide(b, 4) + wide(b, 6))
    rows = [p.astype(F32) for v in (squares, largest) for p in split2(v)]
    rows.append(jnp.zeros((STAT - len(rows), rows[0].shape[1]), F32))
    stats = jnp.concatenate(rows, axis=0).astype(BF16)
    for s in range(out.shape[0]):
        out[s, :half, :128] = left
        out[s, :half, 128:] = right
        out[s, half:, :] = stats


def weights_kernel(core, wq, wo, kv, ko, w_all, kv_all, w_buf, kv_buf, sems):
    n = w_buf.shape[0]
    kb = w_buf.shape[1]
    hw = wq.shape[2]
    rows = kv.shape[0]
    side = math.isqrt(n)

    def fetches(i):
        b = jnp.where(core[0] == 0, i, (i % side) * side + i // side)
        at = pl.ds(pl.multiple_of(b * kb, kb), kb)
        return (
            pltpu.make_async_copy(wq.at[b], w_buf.at[i, :, pl.ds(0, hw)], sems.at[0, i]),
            pltpu.make_async_copy(wo.at[b], w_buf.at[i, :, pl.ds(hw, hw)], sems.at[1, i]),
            pltpu.make_async_copy(kv.at[:, at], kv_buf.at[i, pl.ds(0, rows), :], sems.at[2, i]),
            pltpu.make_async_copy(ko.at[:, at], kv_buf.at[i, pl.ds(rows, rows), :], sems.at[3, i]),
        )

    def stores(i):
        return (
            pltpu.make_async_copy(w_buf.at[i], w_all.at[i], sems.at[4, i]),
            pltpu.make_async_copy(kv_buf.at[i], kv_all.at[i], sems.at[5, i]),
        )

    @pl.loop(0, n)
    def _(i):
        for c in fetches(i):
            c.start()

    @pl.loop(0, n)
    def _(i):
        for c in fetches(i):
            c.wait()
        for c in stores(i):
            c.start()

    @pl.loop(0, n)
    def _(i):
        for c in stores(i):
            c.wait()


def arrange_weights(core, wq, wo, kv, ko):
    n, kb, hw = wq.shape
    hbm = pl.BlockSpec(memory_space=pltpu.HBM)
    out_shape = (
        jax.ShapeDtypeStruct((n, kb, 2 * hw), BF16),
        jax.ShapeDtypeStruct((n, 2 * kv.shape[0], kb), BF16),
    )
    return pl.pallas_call(
        weights_kernel,
        out_shape=out_shape,
        in_specs=[pl.BlockSpec(memory_space=pltpu.SMEM), hbm, hbm, hbm, hbm],
        out_specs=(hbm, hbm),
        scratch_shapes=[pltpu.VMEM(o.shape, o.dtype) for o in out_shape]
        + [pltpu.SemaphoreType.DMA((6, n))],
        compiler_params=pltpu.CompilerParams(vmem_limit_bytes=60 * 2**20),
        cost_estimate=pl.CostEstimate(flops=10**9, bytes_accessed=2 * 10**7, transcendentals=0),
    )(core, wq, wo, kv, ko)


def high_kernel(gathered, high):
    n = gathered.shape[0] // 2
    half = gathered.shape[1] - STAT
    squares, largest = 0.0, 0.0
    for i in range(2 * n):
        s = gathered[i, half:, :].astype(F32)
        squares = squares + (s[0:1] + s[1:2])
        largest = jnp.maximum(largest, s[2:3] + s[3:4])
        if i >= n:
            high[(i - n) * half : (i - n + 1) * half, :] = gathered[i, :half, :]
    rows = [p.astype(F32) for v in (squares, largest) for p in split2(v)]
    rows.append(jnp.zeros((STAT - len(rows), rows[0].shape[1]), F32))
    high[n * half :, :] = jnp.concatenate(rows, axis=0).astype(BF16)


def kv_rows(xs, kvs, kv_in, st_in):
    half = kv_in.shape[1]
    total = kv_in[...]
    squares, largest = st_in[0:1, :], st_in[1:2, :]
    for x, w in zip(xs, kvs):
        n = w.shape[0]
        for i in range(n):
            total = total + lax.dot_general(
                w[i],
                x[i * half : (i + 1) * half, :],
                (((1,), (1,)), ((), ())),
                preferred_element_type=F32,
            )
        if x.shape[0] > n * half:
            s = x[n * half :, :].astype(F32)
            squares = squares + (s[0:1] + s[1:2])
            largest = jnp.maximum(largest, s[2:3] + s[3:4])
    return total, squares, largest


def q_sum(xs, ws, q_in):
    half = q_in.shape[0]
    total = q_in[...]
    for x, w in zip(xs, ws):
        for i in range(w.shape[0]):
            total = total + jnp.dot(
                x[i * half : (i + 1) * half, :], w[i], preferred_element_type=F32
            )
    return total


def fetch(table, m, pairs, sems):
    copies = []
    for i in range(m):
        for j, (whole, buf) in enumerate(pairs):
            n = buf.shape[1]
            at = pl.ds(pl.multiple_of(table[i] * n, n), n)
            copies.append(pltpu.make_async_copy(whole.at[at], buf.at[i], sems.at[j, i]))
    for c in copies:
        c.start()
    for c in copies:
        c.wait()


def matmul_kernel(m, table, *refs):
    xs, w_all, kv_all = refs[:m], refs[m], refs[m + 1]
    q_in, kv_in, st_in, q_out, kv_out, st_out, w_buf, kv_buf, sems = refs[m + 2 :]
    fetch(table, m, ((w_all, w_buf), (kv_all, kv_buf)), sems)
    ws, kvs = [w_buf.at[i] for i in range(m)], [kv_buf.at[i] for i in range(m)]
    q_out[...] = q_sum(xs, ws, q_in)
    total, squares, largest = kv_rows(xs, kvs, kv_in, st_in)
    kv_out[...] = total
    st_out[0:1, :] = squares
    st_out[1:2, :] = largest


def arrivals_call(kernel, out_shape, table, xs, weights, rest, flops, aliases=None):
    m = len(xs)
    n = xs[0].shape[0] // xs[0].shape[1]
    hbm = pl.BlockSpec(memory_space=pltpu.HBM)
    vmem = pl.BlockSpec(memory_space=pltpu.VMEM)
    smem = pl.BlockSpec(memory_space=pltpu.SMEM)
    specs = [smem] + [vmem] * m + [hbm] * len(weights)
    specs += [smem if a.dtype == jnp.int32 else vmem for a in rest]
    return pl.pallas_call(
        kernel,
        out_shape=out_shape,
        in_specs=specs,
        out_specs=tuple(vmem for _ in out_shape),
        scratch_shapes=[pltpu.VMEM((m, n) + w.shape[1:], w.dtype) for w in weights]
        + [pltpu.SemaphoreType.DMA((len(weights), m))],
        input_output_aliases=aliases or {},
        compiler_params=pltpu.CompilerParams(vmem_limit_bytes=VMEM),
        cost_estimate=pl.CostEstimate(flops=flops, bytes_accessed=10**6, transcendentals=0),
    )(table, *xs, *weights, *rest)


def matmul(table, xs, w_all, kv_all, acc):
    m = len(xs)
    out_shape = tuple(jax.ShapeDtypeStruct(a.shape, a.dtype) for a in acc)
    return arrivals_call(
        lambda *refs: matmul_kernel(m, *refs),
        out_shape,
        table,
        xs,
        (w_all, kv_all),
        acc,
        2 * m * xs[0].shape[0] * xs[0].shape[1] * 288,
        {3 + m + i: i for i in range(3)},
    )


def last_kv_kernel(d, m, table, *refs):
    xs, kv_all = refs[:m], refs[m]
    core, kv_in, st_in, kvscale, kcos, ksin, kvt, st_out, kv_buf, sems = refs[m + 1 :]
    fetch(table, m, ((kv_all, kv_buf),), sems)
    t, squares, largest = kv_rows(xs, [kv_buf.at[i] for i in range(m)], kv_in, st_in)
    st_out[0:1, :] = squares
    st_out[1:2, :] = largest
    t = t * (1.0 / jnp.sqrt(squares / d + norm_eps))
    first = core[0] == 0
    mk, mv, ok, ov = t[0:8], t[8:16], t[16:24], t[24:32]
    a = jnp.concatenate([jnp.where(first, mk, ok), jnp.where(first, ok, mk)], axis=0)
    b = jnp.concatenate([jnp.where(first, mv, ov), jnp.where(first, ov, mv)], axis=0)
    a = a * kvscale[:16, :]
    b = b * kvscale[16:, :]
    row = lax.broadcasted_iota(jnp.int32, a.shape, 0)
    swapped = jnp.where(row % 2 == 0, -pltpu.roll(a, a.shape[0] - 1, 0), pltpu.roll(a, 1, 0))
    a = a * kcos[...] + swapped * ksin[...]
    both = jnp.concatenate([a, b], axis=0).astype(BF16)
    for s in range(kvt.shape[0]):
        kvt[s] = both


def last_kv(d, copies, table, core, xs, kv_all, kv, st, kvscale, kcos, ksin):
    m = len(xs)
    out_shape = (
        jax.ShapeDtypeStruct((copies,) + kv.shape, BF16),
        jax.ShapeDtypeStruct(st.shape, F32),
    )
    return arrivals_call(
        lambda *refs: last_kv_kernel(d, m, *refs),
        out_shape,
        table,
        xs,
        (kv_all,),
        [core, kv, st, kvscale, kcos, ksin],
        10**9,
    )


def last_q_kernel(d, m, table, *refs):
    xs, w_all = refs[:m], refs[m]
    q_in, st, wscale, cosine, sine, mine, msg, w_buf, sems = refs[m + 1 :]
    fetch(table, m, ((w_all, w_buf),), sems)
    q = q_sum(xs, [w_buf.at[i] for i in range(m)], q_in)
    half = q.shape[0]
    squares, largest = st[0:1, :], st[1:2, :]
    inv = columns_of(1.0 / jnp.sqrt(squares / d + norm_eps), 128)
    mine[...] = turn(q[:, :128] * inv * wscale[...], cosine[...], sine[...]).astype(BF16)
    msg[:half, :] = q[:, 128:] * inv
    msg[half:, :] = jnp.concatenate(
        [
            squares[:, :128],
            squares[:, 128:],
            largest[:, :128],
            largest[:, 128:],
            jnp.zeros((4, 128), F32),
        ],
        axis=0,
    )


def last_q(d, table, xs, w_all, q, st, wscale, cosine, sine):
    m = len(xs)
    half = q.shape[0]
    out_shape = (
        jax.ShapeDtypeStruct((half, HD), BF16),
        jax.ShapeDtypeStruct((half + 8, HD), F32),
    )
    return arrivals_call(
        lambda *refs: last_q_kernel(d, m, *refs),
        out_shape,
        table,
        xs,
        (w_all,),
        [q, st, wscale, cosine, sine],
        10**9,
    )


def turn(v, cosine, sine):
    lane = lax.broadcasted_iota(jnp.int32, v.shape, 1)
    width = v.shape[1]
    swapped = jnp.where(
        lane % 2 == 0, -pltpu.roll(v, width - 1, 1), pltpu.roll(v, 1, 1)
    )
    return v * cosine + swapped * sine


def columns_of(row, width):
    return jnp.transpose(jnp.broadcast_to(row, (width, row.shape[1])))


def token_kernel(d, core, mine, msg, st, hidden, gain, wscale, cosine, sine, queries, payload, scale):
    half = mine.shape[0]
    c = core[0]
    own = pl.ds(pl.multiple_of(c * half, half), half)
    far = pl.ds(pl.multiple_of((1 - c) * half, half), half)
    queries[own, :] = mine[...]
    queries[far, :] = turn(msg[:half, :] * wscale[...], cosine[...], sine[...]).astype(BF16)
    wide = lambda r: jnp.concatenate(
        [msg[half + r : half + r + 1], msg[half + r + 1 : half + r + 2]], axis=1
    )
    for rows, squares, largest, place in (
        (own, st[0:1, :], st[1:2, :], c),
        (far, wide(0), wide(2), 1 - c),
    ):
        inverse = 1.0 / jnp.sqrt(squares / d + norm_eps)
        row_scale = largest * inverse + tiny_eps
        scale[pl.ds(2 * place, 1), :] = row_scale[:, :128]
        scale[pl.ds(2 * place + 1, 1), :] = row_scale[:, 128:]
        inv = columns_of(inverse, 128)
        rs = columns_of(row_scale, 128)
        normed = hidden[rows, :].astype(F32) * gain[...] * inv
        payload[rows, :] = (normed / rs).astype(BF16)


def head_kernel(order, kvr, keys, values, whole):
    half = kvr.shape[2]
    chips = kvr.shape[0] // 2
    n = KV_COLS_DEV
    for part in range(2):
        at = slice(part * half, (part + 1) * half)
        for i in range(chips):
            rows = kvr[2 * i + part].astype(F32)
            for which in range(2):
                for slot in range(2):
                    to = pl.ds(pl.multiple_of(order[2 * i + slot] * n, n), n)
                    lo = (2 * which + slot) * n
                    whole[which, to, :] = rows[lo : lo + n]
        for which, out in enumerate((keys, values)):
            out[at, :] = jnp.transpose(whole[which]).astype(BF16)


def call(kernel, out_shape, core, *args, flops=0, scratch=()):
    return pl.pallas_call(
        kernel,
        out_shape=out_shape,
        in_specs=[pl.BlockSpec(memory_space=pltpu.SMEM)]
        + [pl.BlockSpec(memory_space=pltpu.VMEM)] * len(args),
        scratch_shapes=list(scratch),
        compiler_params=pltpu.CompilerParams(vmem_limit_bytes=VMEM),
        cost_estimate=pl.CostEstimate(flops=flops or 10**8, bytes_accessed=10**6, transcendentals=0),
    )(core, *args)


def solution(mesh):
    tp = mesh.shape["tp"]
    side = math.isqrt(tp // 2)
    row = 2 * side

    def index(y, x, c):
        return (y % side) * row + (x % side) * 2 + c

    everyone = [(y, x, c) for y in range(side) for x in range(side) for c in range(2)]
    to_partner = [(index(y, x, c), index(y, x, 1 - c)) for y, x, c in everyone]
    heads = tp * KV_COLS_DEV // HD
    columns = side // 2

    def home(j):
        y, x = j // row, (j // 2) % side
        return index(j % heads, x - 1 + (y + x) % columns, y // columns)

    to_row = [(j, home(j)) for j in range(tp)]
    first_groups = [[index(y, x, 0) for x in range(side)] for y in range(side)]
    first_groups += [[index(y, x, 1) for y in range(side)] for x in range(side)]
    rows = [[y * row + i for i in range(row)] for y in range(side)]

    def second(v, s):
        pairs = [
            (index(y, x, c), index(y + s, x, c) if c == 0 else index(y, x + s, c))
            for y, x, c in everyone
        ]
        return lax.ppermute(v, "tp", pairs)

    def swap(v):
        return lax.ppermute(v, "tp", to_partner)

    def body(hidden, norm_gain, prefix, w_query, w_kv, w_scale):
        count, width = hidden.shape
        d = width * tp
        half = count // 2
        me = lax.axis_index("tp")
        core = me % 2
        x = (me // 2) % side
        y = me // row
        core1 = core[None].astype(jnp.int32)
        gain = norm_gain[None, :]

        def piece_at(xs, slot):
            base = y // 2
            h = jnp.where((xs - base + 1) % side < columns, 0, 1)
            source = base + columns * h
            o = (xs - source + 1) % side
            return 2 * ((o - source) % columns + columns * slot) + h

        kv_mine = lax.ppermute(w_kv, "tp", to_row)
        wq_other = swap(w_query)
        kvs_mine = lax.ppermute(w_scale[None, HD:], "tp", to_row)

        blk = jax.ShapeDtypeStruct((half + STAT, width), BF16)
        keep, send = call(prep_kernel, (blk, blk), core1, hidden, gain)
        recv = swap(send)
        slots = call(
            combine_kernel,
            jax.ShapeDtypeStruct((side, half + STAT, 2 * width), BF16),
            core1,
            keep,
            recv,
        )
        gathered = lax.all_to_all(
            slots, "tp", split_axis=0, concat_axis=0, tiled=False, axis_index_groups=first_groups
        )
        kv_other = swap(kv_mine)
        kvs_other = swap(kvs_mine)
        w_all, kv_all = arrange_weights(
            core1, w_query.reshape(-1, 2 * width, HD), wq_other.reshape(-1, 2 * width, HD), kv_mine, kv_other
        )

        positions = (prefix[0] + jnp.arange(count, dtype=jnp.int32)).astype(F32)
        pos_own = lax.dynamic_slice_in_dim(positions, core * half, half)
        pos_far = lax.dynamic_slice_in_dim(positions, (1 - core) * half, half)

        def freq(columns):
            pair = (columns % HD // 2).astype(F32)
            return jnp.power(F32(rope_base), -(2.0 * pair) / HD)

        fq = freq(jnp.arange(HD, dtype=jnp.int32))
        ang_own = pos_own[:, None] * fq[None, :]
        ang_far = pos_far[:, None] * fq[None, :]
        slots_of = jnp.arange(2 * KV_COLS_DEV, dtype=jnp.int32)
        fk = freq(piece_at(x, slots_of // KV_COLS_DEV) * KV_COLS_DEV + slots_of % KV_COLS_DEV)
        seats = jnp.arange(row, dtype=jnp.int32)
        order = piece_at(seats // 2, seats % 2).astype(jnp.int32)
        ang_k = fk[:, None] * pos_own[None, :]
        ordered = jnp.where(
            core == 0,
            jnp.concatenate([kvs_mine, kvs_other], 0),
            jnp.concatenate([kvs_other, kvs_mine], 0),
        )
        kvscale = jnp.broadcast_to(
            jnp.concatenate(
                [ordered[:, :KV_COLS_DEV].reshape(-1), ordered[:, KV_COLS_DEV:].reshape(-1)]
            )[:, None],
            (4 * KV_COLS_DEV, half),
        )
        qscale = w_scale[None, :HD]
        tables = (
            jnp.cos(ang_own),
            jnp.sin(ang_own),
            jnp.cos(ang_far),
            jnp.sin(ang_far),
            jnp.cos(ang_k),
            jnp.sin(ang_k),
            kvscale,
        )
        zeros = (
            jnp.zeros((half, 2 * HD), F32),
            jnp.zeros((4 * KV_COLS_DEV, half), F32),
            jnp.zeros((8, half), F32),
        )
        coord = jnp.where(core == 0, y, x)

        def table_of(items):
            return jnp.stack([(coord - s) % side * 2 + k for s, k, _ in items]).astype(jnp.int32)

        shifts = [(s, k) for s in range(side) for k in range(2)]
        places = {sk: table_of([(*sk, None)]) for sk in shifts}
        gathered, w_all, kv_all, tables, zeros, places, order = lax.optimization_barrier(
            (gathered, w_all, kv_all, tables, zeros, places, order)
        )
        cos_own, sin_own, cos_far, sin_far, cos_k, sin_k, kvscale = tables

        n = side // 2
        low = gathered[:n, :half].reshape(n * half, -1)
        high = pl.pallas_call(
            high_kernel,
            out_shape=jax.ShapeDtypeStruct((n * half + STAT, gathered.shape[2]), BF16),
            compiler_params=pltpu.CompilerParams(vmem_limit_bytes=VMEM),
            cost_estimate=pl.CostEstimate(flops=10**8, bytes_accessed=10**6, transcendentals=0),
        )(gathered)

        def mm(acc, items):
            table = jnp.concatenate([places[s % side, k] for s, k, _ in items])
            return matmul(table, [v for _, _, v in items], w_all, kv_all, acc)

        up = [second(low, 1), second(high, 1)]
        down = [second(low, -1), second(high, -1)]
        acc = mm(zeros, [(0, 0, low), (0, 1, high)])
        last_round = side // 2
        for r in range(1, last_round):
            for k in range(2):
                items = [(r, k, up[k]), (-r, k, down[k])]
                up[k], down[k], acc = lax.optimization_barrier((up[k], down[k], acc))
                if r + 1 < last_round:
                    up[k], down[k] = second(up[k], 1), second(down[k], -1)
                elif k == 0:
                    up[k] = second(up[k], 1)
                else:
                    down[k] = second(down[k], -1)
                acc = mm(acc, items)
        items = [(last_round, 0, up[0]), (-last_round, 1, down[1])]
        xs = [v for _, _, v in items]
        table = jnp.concatenate([places[s % side, k] for s, k, _ in items])
        kvt, st = last_kv(
            d, row, table, core1, xs, kv_all, acc[1], acc[2], kvscale, cos_k, sin_k
        )
        kvr = lax.all_to_all(
            kvt, "tp", split_axis=0, concat_axis=0, tiled=False, axis_index_groups=rows
        )
        mine, msg = last_q(d, table, xs, w_all, acc[0], st, qscale, cos_own, sin_own)
        far = swap(msg)
        out = jax.ShapeDtypeStruct((count, HD), BF16)
        queries, payload, scale = call(
            lambda *r: token_kernel(d, *r),
            (out, out, jax.ShapeDtypeStruct((count // HD, HD), F32)),
            core1,
            mine,
            far,
            st,
            hidden,
            gain,
            qscale,
            cos_far,
            sin_far,
        )
        keys, values = call(
            head_kernel, (out, out), order, kvr, scratch=[pltpu.VMEM((2, HD, half), F32)]
        )
        return queries, keys, values, payload, scale.reshape(count)

    return jax.shard_map(
        body,
        mesh=mesh,
        in_specs=(P("grp", "tp"), P("tp"), P("grp"), P(None, "tp"), P("tp", None), P("tp")),
        out_specs=(P("grp", "tp"), P("grp", "tp"), P("grp", "tp"), P("grp", "tp"), P("grp")),
        check_vma=False,
    )
```

```python
import math

import jax
import jax.numpy as jnp
from jax import lax
from jax.experimental import pallas as pl
from jax.experimental.pallas import tpu as pltpu
from jax.sharding import PartitionSpec as P


HD = 128
KV_COLS_DEV = 8
norm_eps = 1e-05
tiny_eps = 1e-06
rope_base = 500000.0

VMEM = 24 * 2**20
RING_VMEM = 48 * 2**20

F32 = jnp.float32
BF16 = jnp.bfloat16
STAT = 16


def split2(v):
    hi = v.astype(BF16)
    return hi, (v - hi.astype(F32)).astype(BF16)


def prep_kernel(core, hidden, gain, keep, send):
    half = keep.shape[0] - STAT
    for out, which in ((keep, core[0]), (send, 1 - core[0])):
        h = hidden[pl.ds(pl.multiple_of(which * half, half), half), :].astype(F32)
        weighted = h * gain[...]
        out[:half, :] = weighted.astype(BF16)
        squares = jnp.sum(jnp.transpose(h * h), axis=0, keepdims=True)
        largest = jnp.max(jnp.transpose(jnp.abs(weighted)), axis=0, keepdims=True)
        rows = []
        for v in (squares, largest):
            for part in split2(v):
                part = part.astype(F32)
                rows += [part[:, :128], part[:, 128:]]
        rows.append(jnp.zeros((STAT - len(rows), 128), F32))
        out[half:, :] = jnp.concatenate(rows, axis=0).astype(BF16)


def combine_kernel(core, keep, recv, out):
    half = keep.shape[0] - STAT
    first = core[0] == 0
    mine, other = keep[:half, :], recv[:half, :]
    left = jnp.where(first, mine.astype(F32), other.astype(F32)).astype(BF16)
    right = jnp.where(first, other.astype(F32), mine.astype(F32)).astype(BF16)
    a, b = keep[half:, :].astype(F32), recv[half:, :].astype(F32)

    def wide(s, r):
        return jnp.concatenate([s[r : r + 1], s[r + 1 : r + 2]], axis=1)

    squares = (wide(a, 0) + wide(a, 2)) + (wide(b, 0) + wide(b, 2))
    largest = jnp.maximum(wide(a, 4) + wide(a, 6), wide(b, 4) + wide(b, 6))
    rows = [p.astype(F32) for v in (squares, largest) for p in split2(v)]
    rows.append(jnp.zeros((STAT - len(rows), rows[0].shape[1]), F32))
    stats = jnp.concatenate(rows, axis=0).astype(BF16)
    for s in range(out.shape[0]):
        out[s, :half, :128] = left
        out[s, :half, 128:] = right
        out[s, half:, :] = stats


def block_at(core, i, side):
    return jnp.where(core == 0, i, (i % side) * side + i // side)


def weights_kernel(core, wq, wo, w_all, w_buf, sems):
    n = w_buf.shape[0]
    side = math.isqrt(n)

    def fetches(i):
        b = block_at(core[0], i, side)
        return (
            pltpu.make_async_copy(wq.at[b], w_buf.at[i, 0], sems.at[0, i]),
            pltpu.make_async_copy(wo.at[b], w_buf.at[i, 1], sems.at[1, i]),
        )

    def store(i):
        return pltpu.make_async_copy(w_buf.at[i], w_all.at[i], sems.at[2, i])

    @pl.loop(0, n)
    def _(i):
        for c in fetches(i):
            c.start()

    @pl.loop(0, n)
    def _(i):
        for c in fetches(i):
            c.wait()
        store(i).start()

    @pl.loop(0, n)
    def _(i):
        store(i).wait()


def arrange_weights(core, wq, wo):
    n, kb, hw = wq.shape
    hbm = pl.BlockSpec(memory_space=pltpu.HBM)
    out = jax.ShapeDtypeStruct((n, 2, kb, hw), BF16)
    return pl.pallas_call(
        weights_kernel,
        out_shape=out,
        in_specs=[pl.BlockSpec(memory_space=pltpu.SMEM), hbm, hbm],
        out_specs=hbm,
        scratch_shapes=[pltpu.VMEM(out.shape, out.dtype), pltpu.SemaphoreType.DMA((3, n))],
        compiler_params=pltpu.CompilerParams(vmem_limit_bytes=60 * 2**20),
        cost_estimate=pl.CostEstimate(flops=10**9, bytes_accessed=2 * 10**7, transcendentals=0),
    )(core, wq, wo)


def kv_weights_kernel(core, kv, ko, kv_all, kvscale):
    n, rows2, kb = kv_all.shape
    rows = rows2 // 2
    side = math.isqrt(n)
    for i in range(n):
        at = pl.ds(pl.multiple_of(block_at(core[0], i, side) * kb, kb), kb)
        kv_all[i, :rows, :] = kv[:, at]
        kv_all[i, rows:, :] = ko[:, at]
    width = kvscale.shape[1]

    def scales(ref):
        s = ref[:, n * kb : n * kb + 128].astype(F32)
        s = (s[:, 0:1] + s[:, 1:2]) + s[:, 2:3]
        return jnp.broadcast_to(s, (rows, width))

    m, o = scales(kv), scales(ko)
    first = core[0] == 0
    k = rows // 2
    for j, (lo, hi) in enumerate(((0, k), (k, 2 * k))):
        a, b = m[lo:hi], o[lo:hi]
        kvscale[2 * j * k : (2 * j + 1) * k, :] = jnp.where(first, a, b)
        kvscale[(2 * j + 1) * k : (2 * j + 2) * k, :] = jnp.where(first, b, a)


def high_kernel(gathered, high):
    n = gathered.shape[0] // 2
    half = gathered.shape[1] - STAT
    squares, largest = 0.0, 0.0
    for i in range(2 * n):
        s = gathered[i, half:, :].astype(F32)
        squares = squares + (s[0:1] + s[1:2])
        largest = jnp.maximum(largest, s[2:3] + s[3:4])
        if i >= n:
            high[(i - n) * half : (i - n + 1) * half, :] = gathered[i, :half, :]
    rows = [p.astype(F32) for v in (squares, largest) for p in split2(v)]
    rows.append(jnp.zeros((STAT - len(rows), rows[0].shape[1]), F32))
    high[n * half :, :] = jnp.concatenate(rows, axis=0).astype(BF16)


def kv_rows(xs, kvs, kv_in, st_in):
    half = kv_in.shape[1]
    total = kv_in[...]
    squares, largest = st_in[0:1, :], st_in[1:2, :]
    for x, w in zip(xs, kvs):
        n = w.shape[0]
        for i in range(n):
            total = total + lax.dot_general(
                w[i],
                x[i * half : (i + 1) * half, :],
                (((1,), (1,)), ((), ())),
                preferred_element_type=F32,
            )
        if x.shape[0] > n * half:
            s = x[n * half :, :].astype(F32)
            squares = squares + (s[0:1] + s[1:2])
            largest = jnp.maximum(largest, s[2:3] + s[3:4])
    return total, squares, largest


def q_sum(xs, ws, q_in):
    half = q_in.shape[0]
    total = q_in[...]
    for x, w in zip(xs, ws):
        for i in range(w.shape[0]):
            total = total + jnp.dot(
                x[i * half : (i + 1) * half, :],
                jnp.concatenate([w[i, 0], w[i, 1]], axis=1),
                preferred_element_type=F32,
            )
    return total


def fetch(table, m, pairs, sems):
    copies = []
    for i in range(m):
        for j, (whole, buf) in enumerate(pairs):
            n = buf.shape[1]
            at = pl.ds(pl.multiple_of(table[i] * n, n), n)
            copies.append(pltpu.make_async_copy(whole.at[at], buf.at[i], sems.at[j, i]))
    for c in copies:
        c.start()
    for c in copies:
        c.wait()


def matmul_kernel(m, table, *refs):
    xs, w_all, kv_all = refs[:m], refs[m], refs[m + 1]
    q_in, kv_in, st_in, q_out, kv_out, st_out, w_buf, kv_buf, sems = refs[m + 2 :]
    fetch(table, m, ((w_all, w_buf), (kv_all, kv_buf)), sems)
    ws, kvs = [w_buf.at[i] for i in range(m)], [kv_buf.at[i] for i in range(m)]
    q_out[...] = q_sum(xs, ws, q_in)
    total, squares, largest = kv_rows(xs, kvs, kv_in, st_in)
    kv_out[...] = total
    st_out[0:1, :] = squares
    st_out[1:2, :] = largest


def arrivals_call(kernel, out_shape, table, xs, weights, rest, flops, aliases=None):
    m = len(xs)
    n = xs[0].shape[0] // xs[0].shape[1]
    hbm = pl.BlockSpec(memory_space=pltpu.HBM)
    vmem = pl.BlockSpec(memory_space=pltpu.VMEM)
    smem = pl.BlockSpec(memory_space=pltpu.SMEM)
    specs = [smem] + [vmem] * m + [hbm] * len(weights)
    specs += [smem if a.dtype == jnp.int32 else vmem for a in rest]
    return pl.pallas_call(
        kernel,
        out_shape=out_shape,
        in_specs=specs,
        out_specs=tuple(vmem for _ in out_shape),
        scratch_shapes=[pltpu.VMEM((m, n) + w.shape[1:], w.dtype) for w in weights]
        + [pltpu.SemaphoreType.DMA((len(weights), m))],
        input_output_aliases=aliases or {},
        compiler_params=pltpu.CompilerParams(vmem_limit_bytes=RING_VMEM),
        cost_estimate=pl.CostEstimate(flops=flops, bytes_accessed=10**6, transcendentals=0),
    )(table, *xs, *weights, *rest)


def matmul(table, xs, w_all, kv_all, acc):
    m = len(xs)
    out_shape = tuple(jax.ShapeDtypeStruct(a.shape, a.dtype) for a in acc)
    return arrivals_call(
        lambda *refs: matmul_kernel(m, *refs),
        out_shape,
        table,
        xs,
        (w_all, kv_all),
        acc,
        2 * m * xs[0].shape[0] * xs[0].shape[1] * 288,
        {3 + m + i: i for i in range(3)},
    )


def last_kv_kernel(d, m, table, *refs):
    xs, kv_all = refs[:m], refs[m]
    core, kv_in, st_in, kvscale, kcos, ksin, kvt, st_out, kv_buf, sems = refs[m + 1 :]
    fetch(table, m, ((kv_all, kv_buf),), sems)
    t, squares, largest = kv_rows(xs, [kv_buf.at[i] for i in range(m)], kv_in, st_in)
    st_out[0:1, :] = squares
    st_out[1:2, :] = largest
    t = t * (1.0 / jnp.sqrt(squares / d + norm_eps))
    first = core[0] == 0
    mk, mv, ok, ov = t[0:8], t[8:16], t[16:24], t[24:32]
    a = jnp.concatenate([jnp.where(first, mk, ok), jnp.where(first, ok, mk)], axis=0)
    b = jnp.concatenate([jnp.where(first, mv, ov), jnp.where(first, ov, mv)], axis=0)
    a = a * kvscale[:16, :]
    b = b * kvscale[16:, :]
    row = lax.broadcasted_iota(jnp.int32, a.shape, 0)
    swapped = jnp.where(row % 2 == 0, -pltpu.roll(a, a.shape[0] - 1, 0), pltpu.roll(a, 1, 0))
    a = a * kcos[...] + swapped * ksin[...]
    both = jnp.concatenate([a, b], axis=0).astype(BF16)
    for s in range(kvt.shape[0]):
        kvt[s] = both


def last_kv(d, copies, table, core, xs, kv_all, kv, st, kvscale, kcos, ksin):
    m = len(xs)
    out_shape = (
        jax.ShapeDtypeStruct((copies,) + kv.shape, BF16),
        jax.ShapeDtypeStruct(st.shape, F32),
    )
    return arrivals_call(
        lambda *refs: last_kv_kernel(d, m, *refs),
        out_shape,
        table,
        xs,
        (kv_all,),
        [core, kv, st, kvscale, kcos, ksin],
        10**9,
    )


def last_q_kernel(d, m, table, *refs):
    xs, w_all = refs[:m], refs[m]
    q_in, st, wscale, cosine, sine, mine, msg, w_buf, sems = refs[m + 1 :]
    fetch(table, m, ((w_all, w_buf),), sems)
    q = q_sum(xs, [w_buf.at[i] for i in range(m)], q_in)
    half = q.shape[0]
    squares, largest = st[0:1, :], st[1:2, :]
    inv = columns_of(1.0 / jnp.sqrt(squares / d + norm_eps), 128)
    mine[...] = turn(q[:, :128] * inv * wscale[...], cosine[...], sine[...]).astype(BF16)
    msg[:half, :] = q[:, 128:] * inv
    msg[half:, :] = jnp.concatenate(
        [
            squares[:, :128],
            squares[:, 128:],
            largest[:, :128],
            largest[:, 128:],
            jnp.zeros((4, 128), F32),
        ],
        axis=0,
    )


def last_q(d, table, xs, w_all, q, st, wscale, cosine, sine):
    m = len(xs)
    half = q.shape[0]
    out_shape = (
        jax.ShapeDtypeStruct((half, HD), BF16),
        jax.ShapeDtypeStruct((half + 8, HD), F32),
    )
    return arrivals_call(
        lambda *refs: last_q_kernel(d, m, *refs),
        out_shape,
        table,
        xs,
        (w_all,),
        [q, st, wscale, cosine, sine],
        10**9,
    )


def turn(v, cosine, sine):
    lane = lax.broadcasted_iota(jnp.int32, v.shape, 1)
    width = v.shape[1]
    swapped = jnp.where(
        lane % 2 == 0, -pltpu.roll(v, width - 1, 1), pltpu.roll(v, 1, 1)
    )
    return v * cosine + swapped * sine


def columns_of(row, width):
    return jnp.transpose(jnp.broadcast_to(row, (width, row.shape[1])))


def token_kernel(d, core, mine, msg, st, hidden, gain, wscale, cosine, sine, queries, payload, scale):
    half = mine.shape[0]
    c = core[0]
    own = pl.ds(pl.multiple_of(c * half, half), half)
    far = pl.ds(pl.multiple_of((1 - c) * half, half), half)
    queries[own, :] = mine[...]
    queries[far, :] = turn(msg[:half, :] * wscale[...], cosine[...], sine[...]).astype(BF16)
    wide = lambda r: jnp.concatenate(
        [msg[half + r : half + r + 1], msg[half + r + 1 : half + r + 2]], axis=1
    )
    for rows, squares, largest, place in (
        (own, st[0:1, :], st[1:2, :], c),
        (far, wide(0), wide(2), 1 - c),
    ):
        inverse = 1.0 / jnp.sqrt(squares / d + norm_eps)
        row_scale = largest * inverse + tiny_eps
        scale[pl.ds(2 * place, 1), :] = row_scale[:, :128]
        scale[pl.ds(2 * place + 1, 1), :] = row_scale[:, 128:]
        inv = columns_of(inverse, 128)
        rs = columns_of(row_scale, 128)
        normed = hidden[rows, :].astype(F32) * gain[...] * inv
        payload[rows, :] = (normed / rs).astype(BF16)


def head_kernel(order, kvr, keys, values, whole):
    half = kvr.shape[2]
    chips = kvr.shape[0] // 2
    n = KV_COLS_DEV
    for part in range(2):
        at = slice(part * half, (part + 1) * half)
        for i in range(chips):
            rows = kvr[2 * i + part].astype(F32)
            for which in range(2):
                for slot in range(2):
                    to = pl.ds(pl.multiple_of(order[2 * i + slot] * n, n), n)
                    lo = (2 * which + slot) * n
                    whole[which, to, :] = rows[lo : lo + n]
        for which, out in enumerate((keys, values)):
            out[at, :] = jnp.transpose(whole[which]).astype(BF16)


def call(kernel, out_shape, core, *args, flops=0, scratch=()):
    return pl.pallas_call(
        kernel,
        out_shape=out_shape,
        in_specs=[pl.BlockSpec(memory_space=pltpu.SMEM)]
        + [pl.BlockSpec(memory_space=pltpu.VMEM)] * len(args),
        scratch_shapes=list(scratch),
        compiler_params=pltpu.CompilerParams(vmem_limit_bytes=VMEM),
        cost_estimate=pl.CostEstimate(flops=flops or 10**8, bytes_accessed=10**6, transcendentals=0),
    )(core, *args)


def solution(mesh):
    tp = mesh.shape["tp"]
    side = math.isqrt(tp // 2)
    row = 2 * side

    def index(y, x, c):
        return (y % side) * row + (x % side) * 2 + c

    everyone = [(y, x, c) for y in range(side) for x in range(side) for c in range(2)]
    to_partner = [(index(y, x, c), index(y, x, 1 - c)) for y, x, c in everyone]
    heads = tp * KV_COLS_DEV // HD
    columns = side // 2

    def home(j):
        y, x = j // row, (j // 2) % side
        return index(j % heads, x - 1 + (y + x) % columns, y // columns)

    to_row = [(j, home(j)) for j in range(tp)]
    first_groups = [[index(y, x, 0) for x in range(side)] for y in range(side)]
    first_groups += [[index(y, x, 1) for y in range(side)] for x in range(side)]
    rows = [[y * row + i for i in range(row)] for y in range(side)]

    def second(v, s):
        pairs = [
            (index(y, x, c), index(y + s, x, c) if c == 0 else index(y, x + s, c))
            for y, x, c in everyone
        ]
        return lax.ppermute(v, "tp", pairs)

    def swap(v):
        return lax.ppermute(v, "tp", to_partner)

    def body(hidden, norm_gain, prefix, w_query, w_kv, w_scale):
        count, width = hidden.shape
        d = width * tp
        half = count // 2
        me = lax.axis_index("tp")
        core = me % 2
        x = (me // 2) % side
        y = me // row
        core1 = core[None].astype(jnp.int32)
        gain = norm_gain[None, :]

        def piece_at(xs, slot):
            base = y // 2
            h = jnp.where((xs - base + 1) % side < columns, 0, 1)
            source = base + columns * h
            o = (xs - source + 1) % side
            return 2 * ((o - source) % columns + columns * slot) + h

        blk = jax.ShapeDtypeStruct((half + STAT, width), BF16)
        keep, send = call(prep_kernel, (blk, blk), core1, hidden, gain)
        recv = swap(send)
        kvs = w_scale[HD:]
        hi = kvs.astype(BF16)
        mid = kvs - hi.astype(F32)
        mid, lo = mid.astype(BF16), (mid - mid.astype(BF16).astype(F32)).astype(BF16)
        scales = jnp.pad(jnp.stack([hi, mid, lo], axis=1), ((0, 0), (0, 125)))
        kv_mine = lax.ppermute(jnp.concatenate([w_kv, scales], axis=1), "tp", to_row)
        wq_other = swap(w_query)
        slots = call(
            combine_kernel,
            jax.ShapeDtypeStruct((side, half + STAT, 2 * width), BF16),
            core1,
            keep,
            recv,
        )
        gathered = lax.all_to_all(
            slots, "tp", split_axis=0, concat_axis=0, tiled=False, axis_index_groups=first_groups
        )
        w_all = arrange_weights(
            core1, w_query.reshape(-1, 2 * width, HD), wq_other.reshape(-1, 2 * width, HD)
        )

        positions = (prefix[0] + jnp.arange(count, dtype=jnp.int32)).astype(F32)
        pos_own = lax.dynamic_slice_in_dim(positions, core * half, half)
        pos_far = lax.dynamic_slice_in_dim(positions, (1 - core) * half, half)

        def freq(columns):
            pair = (columns % HD // 2).astype(F32)
            return jnp.power(F32(rope_base), -(2.0 * pair) / HD)

        fq = freq(jnp.arange(HD, dtype=jnp.int32))
        ang_own = pos_own[:, None] * fq[None, :]
        ang_far = pos_far[:, None] * fq[None, :]
        slots_of = jnp.arange(2 * KV_COLS_DEV, dtype=jnp.int32)
        fk = freq(piece_at(x, slots_of // KV_COLS_DEV) * KV_COLS_DEV + slots_of % KV_COLS_DEV)
        seats = jnp.arange(row, dtype=jnp.int32)
        order = piece_at(seats // 2, seats % 2).astype(jnp.int32)
        ang_k = fk[:, None] * pos_own[None, :]
        qscale = w_scale[None, :HD]
        tables = (
            jnp.cos(ang_own),
            jnp.sin(ang_own),
            jnp.cos(ang_far),
            jnp.sin(ang_far),
            jnp.cos(ang_k),
            jnp.sin(ang_k),
        )
        zeros = (
            jnp.zeros((half, 2 * HD), F32),
            jnp.zeros((4 * KV_COLS_DEV, half), F32),
            jnp.zeros((8, half), F32),
        )
        coord = jnp.where(core == 0, y, x)

        def table_of(items):
            return jnp.stack([(coord - s) % side * 2 + k for s, k, _ in items]).astype(jnp.int32)

        shifts = [(s, k) for s in range(side) for k in range(2)]
        places = {sk: table_of([(*sk, None)]) for sk in shifts}
        gathered, w_all, tables, zeros, places, order = lax.optimization_barrier(
            (gathered, w_all, tables, zeros, places, order)
        )
        cos_own, sin_own, cos_far, sin_far, cos_k, sin_k = tables

        n = side // 2
        low = gathered[:n, :half].reshape(n * half, -1)
        high = pl.pallas_call(
            high_kernel,
            out_shape=jax.ShapeDtypeStruct((n * half + STAT, gathered.shape[2]), BF16),
            compiler_params=pltpu.CompilerParams(vmem_limit_bytes=VMEM),
            cost_estimate=pl.CostEstimate(flops=10**8, bytes_accessed=10**6, transcendentals=0),
        )(gathered)

        def mm(acc, items):
            table = jnp.concatenate([places[s % side, k] for s, k, _ in items])
            return matmul(table, [v for _, _, v in items], w_all, kv_all, acc)

        up = [second(low, 1), second(high, 1)]
        down = [second(low, -1), second(high, -1)]
        kv_other = swap(kv_mine)
        kv_all, kvscale = call(
            kv_weights_kernel,
            (
                jax.ShapeDtypeStruct((d // (2 * width), 4 * KV_COLS_DEV, 2 * width), BF16),
                jax.ShapeDtypeStruct((4 * KV_COLS_DEV, half), F32),
            ),
            core1,
            kv_mine,
            kv_other,
        )
        acc = mm(zeros, [(0, 0, low), (0, 1, high)])
        last_round = side // 2
        for r in range(1, last_round):
            for k in range(2):
                items = [(r, k, up[k]), (-r, k, down[k])]
                up[k], down[k], acc = lax.optimization_barrier((up[k], down[k], acc))
                if r + 1 < last_round:
                    up[k], down[k] = second(up[k], 1), second(down[k], -1)
                elif k == 0:
                    up[k] = second(up[k], 1)
                else:
                    down[k] = second(down[k], -1)
                acc = mm(acc, items)
        items = [(last_round, 0, up[0]), (-last_round, 1, down[1])]
        xs = [v for _, _, v in items]
        table = jnp.concatenate([places[s % side, k] for s, k, _ in items])
        kvt, st = last_kv(
            d, row, table, core1, xs, kv_all, acc[1], acc[2], kvscale, cos_k, sin_k
        )
        kvr = lax.all_to_all(
            kvt, "tp", split_axis=0, concat_axis=0, tiled=False, axis_index_groups=rows
        )
        mine, msg = last_q(d, table, xs, w_all, acc[0], st, qscale, cos_own, sin_own)
        far = swap(msg)
        out = jax.ShapeDtypeStruct((count, HD), BF16)
        queries, payload, scale = call(
            lambda *r: token_kernel(d, *r),
            (out, out, jax.ShapeDtypeStruct((count // HD, HD), F32)),
            core1,
            mine,
            far,
            st,
            hidden,
            gain,
            qscale,
            cos_far,
            sin_far,
        )
        keys, values = call(
            head_kernel, (out, out), order, kvr, scratch=[pltpu.VMEM((2, HD, half), F32)]
        )
        return queries, keys, values, payload, scale.reshape(count)

    return jax.shard_map(
        body,
        mesh=mesh,
        in_specs=(P("grp", "tp"), P("tp"), P("grp"), P(None, "tp"), P("tp", None), P("tp")),
        out_specs=(P("grp", "tp"), P("grp", "tp"), P("grp", "tp"), P("grp", "tp"), P("grp")),
        check_vma=False,
    )
```

```python
import math

import jax
import jax.numpy as jnp
from jax import lax
from jax.experimental import pallas as pl
from jax.experimental.pallas import tpu as pltpu
from jax.sharding import PartitionSpec as P


HD = 128
KV_COLS_DEV = 8
norm_eps = 1e-05
tiny_eps = 1e-06
rope_base = 500000.0

VMEM = 24 * 2**20
RING_VMEM = 48 * 2**20

F32 = jnp.float32
BF16 = jnp.bfloat16
STAT = 16


def split2(v):
    hi = v.astype(BF16)
    return hi, (v - hi.astype(F32)).astype(BF16)


def prep_kernel(core, hidden, gain, keep, send):
    half = keep.shape[0] - STAT
    for out, which in ((keep, core[0]), (send, 1 - core[0])):
        h = hidden[pl.ds(pl.multiple_of(which * half, half), half), :].astype(F32)
        weighted = h * gain[...]
        out[:half, :] = weighted.astype(BF16)
        squares = jnp.sum(jnp.transpose(h * h), axis=0, keepdims=True)
        largest = jnp.max(jnp.transpose(jnp.abs(weighted)), axis=0, keepdims=True)
        rows = []
        for v in (squares, largest):
            for part in split2(v):
                part = part.astype(F32)
                rows += [part[:, :128], part[:, 128:]]
        rows.append(jnp.zeros((STAT - len(rows), 128), F32))
        out[half:, :] = jnp.concatenate(rows, axis=0).astype(BF16)


def combine_kernel(core, keep, recv, out):
    half = keep.shape[0] - STAT
    first = core[0] == 0
    mine, other = keep[:half, :], recv[:half, :]
    left = jnp.where(first, mine.astype(F32), other.astype(F32)).astype(BF16)
    right = jnp.where(first, other.astype(F32), mine.astype(F32)).astype(BF16)
    a, b = keep[half:, :].astype(F32), recv[half:, :].astype(F32)

    def wide(s, r):
        return jnp.concatenate([s[r : r + 1], s[r + 1 : r + 2]], axis=1)

    squares = (wide(a, 0) + wide(a, 2)) + (wide(b, 0) + wide(b, 2))
    largest = jnp.maximum(wide(a, 4) + wide(a, 6), wide(b, 4) + wide(b, 6))
    rows = [p.astype(F32) for v in (squares, largest) for p in split2(v)]
    rows.append(jnp.zeros((STAT - len(rows), rows[0].shape[1]), F32))
    stats = jnp.concatenate(rows, axis=0).astype(BF16)
    for s in range(out.shape[0]):
        out[s, :half, :128] = left
        out[s, :half, 128:] = right
        out[s, half:, :] = stats


def block_at(core, i, side):
    return jnp.where(core == 0, i, (i % side) * side + i // side)


def weights_kernel(core, wq, wo, w_all, w_buf, sems):
    n = w_buf.shape[0]
    side = math.isqrt(n)

    def fetches(i):
        b = block_at(core[0], i, side)
        return (
            pltpu.make_async_copy(wq.at[b], w_buf.at[i, 0], sems.at[0, i]),
            pltpu.make_async_copy(wo.at[b], w_buf.at[i, 1], sems.at[1, i]),
        )

    def store(i):
        return pltpu.make_async_copy(w_buf.at[i], w_all.at[i], sems.at[2, i])

    @pl.loop(0, n)
    def _(i):
        for c in fetches(i):
            c.start()

    @pl.loop(0, n)
    def _(i):
        for c in fetches(i):
            c.wait()
        store(i).start()

    @pl.loop(0, n)
    def _(i):
        store(i).wait()


def arrange_weights(core, wq, wo):
    n, kb, hw = wq.shape
    hbm = pl.BlockSpec(memory_space=pltpu.HBM)
    out = jax.ShapeDtypeStruct((n, 2, kb, hw), BF16)
    return pl.pallas_call(
        weights_kernel,
        out_shape=out,
        in_specs=[pl.BlockSpec(memory_space=pltpu.SMEM), hbm, hbm],
        out_specs=hbm,
        scratch_shapes=[pltpu.VMEM(out.shape, out.dtype), pltpu.SemaphoreType.DMA((3, n))],
        compiler_params=pltpu.CompilerParams(vmem_limit_bytes=60 * 2**20),
        cost_estimate=pl.CostEstimate(flops=10**9, bytes_accessed=2 * 10**7, transcendentals=0),
    )(core, wq, wo)


def kv_weights_kernel(core, kv, ko, kv_all, kvscale):
    n, rows2, kb = kv_all.shape
    rows = rows2 // 2
    side = math.isqrt(n)
    for i in range(n):
        at = pl.ds(pl.multiple_of(block_at(core[0], i, side) * kb, kb), kb)
        kv_all[i, :rows, :] = kv[:, at]
        kv_all[i, rows:, :] = ko[:, at]
    width = kvscale.shape[1]

    def scales(ref):
        s = ref[:, n * kb : n * kb + 128].astype(F32)
        s = (s[:, 0:1] + s[:, 1:2]) + s[:, 2:3]
        return jnp.broadcast_to(s, (rows, width))

    m, o = scales(kv), scales(ko)
    first = core[0] == 0
    k = rows // 2
    for j, (lo, hi) in enumerate(((0, k), (k, 2 * k))):
        a, b = m[lo:hi], o[lo:hi]
        kvscale[2 * j * k : (2 * j + 1) * k, :] = jnp.where(first, a, b)
        kvscale[(2 * j + 1) * k : (2 * j + 2) * k, :] = jnp.where(first, b, a)


def high_kernel(gathered, high):
    n = gathered.shape[0] // 2
    half = gathered.shape[1] - STAT
    squares, largest = 0.0, 0.0
    for i in range(2 * n):
        s = gathered[i, half:, :].astype(F32)
        squares = squares + (s[0:1] + s[1:2])
        largest = jnp.maximum(largest, s[2:3] + s[3:4])
        if i >= n:
            high[(i - n) * half : (i - n + 1) * half, :] = gathered[i, :half, :]
    rows = [p.astype(F32) for v in (squares, largest) for p in split2(v)]
    rows.append(jnp.zeros((STAT - len(rows), rows[0].shape[1]), F32))
    high[n * half :, :] = jnp.concatenate(rows, axis=0).astype(BF16)


def kv_rows(xs, kvs, kv_in, st_in):
    half = kv_in.shape[1]
    total = kv_in[...]
    squares, largest = st_in[0:1, :], st_in[1:2, :]
    for x, w in zip(xs, kvs):
        n = w.shape[0]
        for i in range(n):
            total = total + lax.dot_general(
                w[i],
                x[i * half : (i + 1) * half, :],
                (((1,), (1,)), ((), ())),
                preferred_element_type=F32,
            )
        if x.shape[0] > n * half:
            s = x[n * half :, :].astype(F32)
            squares = squares + (s[0:1] + s[1:2])
            largest = jnp.maximum(largest, s[2:3] + s[3:4])
    return total, squares, largest


def q_sum(xs, ws, q_in):
    half = q_in.shape[0]
    total = q_in[...]
    for x, w in zip(xs, ws):
        for i in range(w.shape[0]):
            total = total + jnp.dot(
                x[i * half : (i + 1) * half, :],
                jnp.concatenate([w[i, 0], w[i, 1]], axis=1),
                preferred_element_type=F32,
            )
    return total


def fetch(table, m, pairs, sems, xs, x_buf):
    copies = [
        pltpu.make_async_copy(x, x_buf.at[i, pl.ds(0, x.shape[0])], sems.at[len(pairs), i])
        for i, x in enumerate(xs)
    ]
    for i in range(m):
        for j, (whole, buf) in enumerate(pairs):
            n = buf.shape[1]
            at = pl.ds(pl.multiple_of(table[i] * n, n), n)
            copies.append(pltpu.make_async_copy(whole.at[at], buf.at[i], sems.at[j, i]))
    for c in copies:
        c.start()
    for c in copies:
        c.wait()
    return [x_buf.at[i, pl.ds(0, x.shape[0])] for i, x in enumerate(xs)]


def matmul_kernel(m, table, *refs):
    xs, w_all, kv_all = refs[:m], refs[m], refs[m + 1]
    q_in, kv_in, st_in, q_out, kv_out, st_out, x_buf, w_buf, kv_buf, sems = refs[m + 2 :]
    xs = fetch(table, m, ((w_all, w_buf), (kv_all, kv_buf)), sems, xs, x_buf)
    ws, kvs = [w_buf.at[i] for i in range(m)], [kv_buf.at[i] for i in range(m)]
    q_out[...] = q_sum(xs, ws, q_in)
    total, squares, largest = kv_rows(xs, kvs, kv_in, st_in)
    kv_out[...] = total
    st_out[0:1, :] = squares
    st_out[1:2, :] = largest


def arrivals_call(kernel, out_shape, table, xs, weights, rest, flops, aliases=None):
    m = len(xs)
    n = xs[0].shape[0] // xs[0].shape[1]
    hbm = pl.BlockSpec(memory_space=pltpu.HBM)
    vmem = pl.BlockSpec(memory_space=pltpu.VMEM)
    smem = pl.BlockSpec(memory_space=pltpu.SMEM)
    specs = [smem] + [hbm] * (m + len(weights))
    specs += [smem if a.dtype == jnp.int32 else vmem for a in rest]
    return pl.pallas_call(
        kernel,
        out_shape=out_shape,
        in_specs=specs,
        out_specs=tuple(vmem for _ in out_shape),
        scratch_shapes=[pltpu.VMEM((m, max(x.shape[0] for x in xs), xs[0].shape[1]), BF16)]
        + [pltpu.VMEM((m, n) + w.shape[1:], w.dtype) for w in weights]
        + [pltpu.SemaphoreType.DMA((len(weights) + 1, m))],
        input_output_aliases=aliases or {},
        compiler_params=pltpu.CompilerParams(vmem_limit_bytes=RING_VMEM),
        cost_estimate=pl.CostEstimate(flops=flops, bytes_accessed=10**6, transcendentals=0),
    )(table, *xs, *weights, *rest)


def matmul(table, xs, w_all, kv_all, acc):
    m = len(xs)
    out_shape = tuple(jax.ShapeDtypeStruct(a.shape, a.dtype) for a in acc)
    return arrivals_call(
        lambda *refs: matmul_kernel(m, *refs),
        out_shape,
        table,
        xs,
        (w_all, kv_all),
        acc,
        2 * m * xs[0].shape[0] * xs[0].shape[1] * 288,
        {3 + m + i: i for i in range(3)},
    )


def last_kv_kernel(d, m, table, *refs):
    xs, kv_all = refs[:m], refs[m]
    core, kv_in, st_in, kvscale, kcos, ksin, kvt, st_out, x_buf, kv_buf, sems = refs[m + 1 :]
    xs = fetch(table, m, ((kv_all, kv_buf),), sems, xs, x_buf)
    t, squares, largest = kv_rows(xs, [kv_buf.at[i] for i in range(m)], kv_in, st_in)
    st_out[0:1, :] = squares
    st_out[1:2, :] = largest
    t = t * (1.0 / jnp.sqrt(squares / d + norm_eps))
    first = core[0] == 0
    mk, mv, ok, ov = t[0:8], t[8:16], t[16:24], t[24:32]
    a = jnp.concatenate([jnp.where(first, mk, ok), jnp.where(first, ok, mk)], axis=0)
    b = jnp.concatenate([jnp.where(first, mv, ov), jnp.where(first, ov, mv)], axis=0)
    a = a * kvscale[:16, :]
    b = b * kvscale[16:, :]
    row = lax.broadcasted_iota(jnp.int32, a.shape, 0)
    swapped = jnp.where(row % 2 == 0, -pltpu.roll(a, a.shape[0] - 1, 0), pltpu.roll(a, 1, 0))
    a = a * kcos[...] + swapped * ksin[...]
    both = jnp.concatenate([a, b], axis=0).astype(BF16)
    for s in range(kvt.shape[0]):
        kvt[s] = both


def last_kv(d, copies, table, core, xs, kv_all, kv, st, kvscale, kcos, ksin):
    m = len(xs)
    out_shape = (
        jax.ShapeDtypeStruct((copies,) + kv.shape, BF16),
        jax.ShapeDtypeStruct(st.shape, F32),
    )
    return arrivals_call(
        lambda *refs: last_kv_kernel(d, m, *refs),
        out_shape,
        table,
        xs,
        (kv_all,),
        [core, kv, st, kvscale, kcos, ksin],
        10**9,
    )


def last_q_kernel(d, m, table, *refs):
    xs, w_all = refs[:m], refs[m]
    q_in, st, wscale, cosine, sine, mine, msg, x_buf, w_buf, sems = refs[m + 1 :]
    xs = fetch(table, m, ((w_all, w_buf),), sems, xs, x_buf)
    q = q_sum(xs, [w_buf.at[i] for i in range(m)], q_in)
    half = q.shape[0]
    squares, largest = st[0:1, :], st[1:2, :]
    inv = columns_of(1.0 / jnp.sqrt(squares / d + norm_eps), 128)
    mine[...] = turn(q[:, :128] * inv * wscale[...], cosine[...], sine[...]).astype(BF16)
    msg[:half, :] = q[:, 128:] * inv
    msg[half:, :] = jnp.concatenate(
        [
            squares[:, :128],
            squares[:, 128:],
            largest[:, :128],
            largest[:, 128:],
            jnp.zeros((4, 128), F32),
        ],
        axis=0,
    )


def last_q(d, table, xs, w_all, q, st, wscale, cosine, sine):
    m = len(xs)
    half = q.shape[0]
    out_shape = (
        jax.ShapeDtypeStruct((half, HD), BF16),
        jax.ShapeDtypeStruct((half + 8, HD), F32),
    )
    return arrivals_call(
        lambda *refs: last_q_kernel(d, m, *refs),
        out_shape,
        table,
        xs,
        (w_all,),
        [q, st, wscale, cosine, sine],
        10**9,
    )


def turn(v, cosine, sine):
    lane = lax.broadcasted_iota(jnp.int32, v.shape, 1)
    width = v.shape[1]
    swapped = jnp.where(
        lane % 2 == 0, -pltpu.roll(v, width - 1, 1), pltpu.roll(v, 1, 1)
    )
    return v * cosine + swapped * sine


def columns_of(row, width):
    return jnp.transpose(jnp.broadcast_to(row, (width, row.shape[1])))


def token_kernel(d, core, mine, msg, st, hidden, gain, wscale, cosine, sine, queries, payload, scale):
    half = mine.shape[0]
    c = core[0]
    own = pl.ds(pl.multiple_of(c * half, half), half)
    far = pl.ds(pl.multiple_of((1 - c) * half, half), half)
    queries[own, :] = mine[...]
    queries[far, :] = turn(msg[:half, :] * wscale[...], cosine[...], sine[...]).astype(BF16)
    wide = lambda r: jnp.concatenate(
        [msg[half + r : half + r + 1], msg[half + r + 1 : half + r + 2]], axis=1
    )
    for rows, squares, largest, place in (
        (own, st[0:1, :], st[1:2, :], c),
        (far, wide(0), wide(2), 1 - c),
    ):
        inverse = 1.0 / jnp.sqrt(squares / d + norm_eps)
        row_scale = largest * inverse + tiny_eps
        scale[pl.ds(2 * place, 1), :] = row_scale[:, :128]
        scale[pl.ds(2 * place + 1, 1), :] = row_scale[:, 128:]
        inv = columns_of(inverse, 128)
        rs = columns_of(row_scale, 128)
        normed = hidden[rows, :].astype(F32) * gain[...] * inv
        payload[rows, :] = (normed / rs).astype(BF16)


def head_kernel(order, kvr, keys, values, whole):
    half = kvr.shape[2]
    chips = kvr.shape[0] // 2
    n = KV_COLS_DEV
    for part in range(2):
        at = slice(part * half, (part + 1) * half)
        for i in range(chips):
            rows = kvr[2 * i + part].astype(F32)
            for which in range(2):
                for slot in range(2):
                    to = pl.ds(pl.multiple_of(order[2 * i + slot] * n, n), n)
                    lo = (2 * which + slot) * n
                    whole[which, to, :] = rows[lo : lo + n]
        for which, out in enumerate((keys, values)):
            out[at, :] = jnp.transpose(whole[which]).astype(BF16)


def call(kernel, out_shape, core, *args, flops=0, scratch=()):
    return pl.pallas_call(
        kernel,
        out_shape=out_shape,
        in_specs=[pl.BlockSpec(memory_space=pltpu.SMEM)]
        + [pl.BlockSpec(memory_space=pltpu.VMEM)] * len(args),
        scratch_shapes=list(scratch),
        compiler_params=pltpu.CompilerParams(vmem_limit_bytes=VMEM),
        cost_estimate=pl.CostEstimate(flops=flops or 10**8, bytes_accessed=10**6, transcendentals=0),
    )(core, *args)


def solution(mesh):
    tp = mesh.shape["tp"]
    side = math.isqrt(tp // 2)
    row = 2 * side

    def index(y, x, c):
        return (y % side) * row + (x % side) * 2 + c

    everyone = [(y, x, c) for y in range(side) for x in range(side) for c in range(2)]
    to_partner = [(index(y, x, c), index(y, x, 1 - c)) for y, x, c in everyone]
    heads = tp * KV_COLS_DEV // HD
    columns = side // 2

    def home(j):
        y, x = j // row, (j // 2) % side
        return index(j % heads, x - 1 + (y + x) % columns, y // columns)

    to_row = [(j, home(j)) for j in range(tp)]
    first_groups = [[index(y, x, 0) for x in range(side)] for y in range(side)]
    first_groups += [[index(y, x, 1) for y in range(side)] for x in range(side)]
    rows = [[y * row + i for i in range(row)] for y in range(side)]

    def second(v, s):
        pairs = [
            (index(y, x, c), index(y + s, x, c) if c == 0 else index(y, x + s, c))
            for y, x, c in everyone
        ]
        return lax.ppermute(v, "tp", pairs)

    def swap(v):
        return lax.ppermute(v, "tp", to_partner)

    def body(hidden, norm_gain, prefix, w_query, w_kv, w_scale):
        count, width = hidden.shape
        d = width * tp
        half = count // 2
        me = lax.axis_index("tp")
        core = me % 2
        x = (me // 2) % side
        y = me // row
        core1 = core[None].astype(jnp.int32)
        gain = norm_gain[None, :]

        def piece_at(xs, slot):
            base = y // 2
            h = jnp.where((xs - base + 1) % side < columns, 0, 1)
            source = base + columns * h
            o = (xs - source + 1) % side
            return 2 * ((o - source) % columns + columns * slot) + h

        blk = jax.ShapeDtypeStruct((half + STAT, width), BF16)
        keep, send = call(prep_kernel, (blk, blk), core1, hidden, gain)
        recv = swap(send)
        kvs = w_scale[HD:]
        hi = kvs.astype(BF16)
        mid = kvs - hi.astype(F32)
        mid, lo = mid.astype(BF16), (mid - mid.astype(BF16).astype(F32)).astype(BF16)
        scales = jnp.pad(jnp.stack([hi, mid, lo], axis=1), ((0, 0), (0, 125)))
        kv_mine = lax.ppermute(jnp.concatenate([w_kv, scales], axis=1), "tp", to_row)
        wq_other = swap(w_query)
        slots = call(
            combine_kernel,
            jax.ShapeDtypeStruct((side, half + STAT, 2 * width), BF16),
            core1,
            keep,
            recv,
        )
        gathered = lax.all_to_all(
            slots, "tp", split_axis=0, concat_axis=0, tiled=False, axis_index_groups=first_groups
        )
        w_all = arrange_weights(
            core1, w_query.reshape(-1, 2 * width, HD), wq_other.reshape(-1, 2 * width, HD)
        )

        positions = (prefix[0] + jnp.arange(count, dtype=jnp.int32)).astype(F32)
        pos_own = lax.dynamic_slice_in_dim(positions, core * half, half)
        pos_far = lax.dynamic_slice_in_dim(positions, (1 - core) * half, half)

        def freq(columns):
            pair = (columns % HD // 2).astype(F32)
            return jnp.power(F32(rope_base), -(2.0 * pair) / HD)

        fq = freq(jnp.arange(HD, dtype=jnp.int32))
        ang_own = pos_own[:, None] * fq[None, :]
        ang_far = pos_far[:, None] * fq[None, :]
        slots_of = jnp.arange(2 * KV_COLS_DEV, dtype=jnp.int32)
        fk = freq(piece_at(x, slots_of // KV_COLS_DEV) * KV_COLS_DEV + slots_of % KV_COLS_DEV)
        seats = jnp.arange(row, dtype=jnp.int32)
        order = piece_at(seats // 2, seats % 2).astype(jnp.int32)
        ang_k = fk[:, None] * pos_own[None, :]
        qscale = w_scale[None, :HD]
        tables = (
            jnp.cos(ang_own),
            jnp.sin(ang_own),
            jnp.cos(ang_far),
            jnp.sin(ang_far),
            jnp.cos(ang_k),
            jnp.sin(ang_k),
        )
        zeros = (
            jnp.zeros((half, 2 * HD), F32),
            jnp.zeros((4 * KV_COLS_DEV, half), F32),
            jnp.zeros((8, half), F32),
        )
        coord = jnp.where(core == 0, y, x)

        def table_of(items):
            return jnp.stack([(coord - s) % side * 2 + k for s, k, _ in items]).astype(jnp.int32)

        shifts = [(s, k) for s in range(side) for k in range(2)]
        places = {sk: table_of([(*sk, None)]) for sk in shifts}
        gathered, w_all, tables, zeros, places, order = lax.optimization_barrier(
            (gathered, w_all, tables, zeros, places, order)
        )
        cos_own, sin_own, cos_far, sin_far, cos_k, sin_k = tables

        n = side // 2
        low = gathered[:n, :half].reshape(n * half, -1)
        high = pl.pallas_call(
            high_kernel,
            out_shape=jax.ShapeDtypeStruct((n * half + STAT, gathered.shape[2]), BF16),
            compiler_params=pltpu.CompilerParams(vmem_limit_bytes=VMEM),
            cost_estimate=pl.CostEstimate(flops=10**8, bytes_accessed=10**6, transcendentals=0),
        )(gathered)

        def mm(acc, items):
            table = jnp.concatenate([places[s % side, k] for s, k, _ in items])
            return matmul(table, [v for _, _, v in items], w_all, kv_all, acc)

        up = [second(low, 1), second(high, 1)]
        down = [second(low, -1), second(high, -1)]
        kv_other = swap(kv_mine)
        kv_all, kvscale = call(
            kv_weights_kernel,
            (
                jax.ShapeDtypeStruct((d // (2 * width), 4 * KV_COLS_DEV, 2 * width), BF16),
                jax.ShapeDtypeStruct((4 * KV_COLS_DEV, half), F32),
            ),
            core1,
            kv_mine,
            kv_other,
        )
        acc = mm(zeros, [(0, 0, low), (0, 1, high)])
        last_round = side // 2
        for r in range(1, last_round):
            for k in range(2):
                items = [(r, k, up[k]), (-r, k, down[k])]
                up[k], down[k], acc = lax.optimization_barrier((up[k], down[k], acc))
                if r + 1 < last_round:
                    up[k], down[k] = second(up[k], 1), second(down[k], -1)
                elif k == 0:
                    up[k] = second(up[k], 1)
                else:
                    down[k] = second(down[k], -1)
                acc = mm(acc, items)
        items = [(last_round, 0, up[0]), (-last_round, 1, down[1])]
        xs = [v for _, _, v in items]
        table = jnp.concatenate([places[s % side, k] for s, k, _ in items])
        kvt, st = last_kv(
            d, row, table, core1, xs, kv_all, acc[1], acc[2], kvscale, cos_k, sin_k
        )
        kvr = lax.all_to_all(
            kvt, "tp", split_axis=0, concat_axis=0, tiled=False, axis_index_groups=rows
        )
        mine, msg = last_q(d, table, xs, w_all, acc[0], st, qscale, cos_own, sin_own)
        far = swap(msg)
        out = jax.ShapeDtypeStruct((count, HD), BF16)
        queries, payload, scale = call(
            lambda *r: token_kernel(d, *r),
            (out, out, jax.ShapeDtypeStruct((count // HD, HD), F32)),
            core1,
            mine,
            far,
            st,
            hidden,
            gain,
            qscale,
            cos_far,
            sin_far,
        )
        keys, values = call(
            head_kernel, (out, out), order, kvr, scratch=[pltpu.VMEM((2, HD, half), F32)]
        )
        return queries, keys, values, payload, scale.reshape(count)

    return jax.shard_map(
        body,
        mesh=mesh,
        in_specs=(P("grp", "tp"), P("tp"), P("grp"), P(None, "tp"), P("tp", None), P("tp")),
        out_specs=(P("grp", "tp"), P("grp", "tp"), P("grp", "tp"), P("grp", "tp"), P("grp")),
        check_vma=False,
    )
```

```python
import math

import jax
import jax.numpy as jnp
from jax import lax
from jax.experimental import pallas as pl
from jax.experimental.pallas import tpu as pltpu
from jax.sharding import PartitionSpec as P


HD = 128
KV_COLS_DEV = 8
norm_eps = 1e-05
tiny_eps = 1e-06
rope_base = 500000.0

VMEM = 24 * 2**20
RING_VMEM = 24 * 2**20

F32 = jnp.float32
BF16 = jnp.bfloat16
STAT = 16


def split2(v):
    hi = v.astype(BF16)
    return hi, (v - hi.astype(F32)).astype(BF16)


def prep_kernel(core, hidden, gain, keep, send):
    half = keep.shape[0] - STAT
    for out, which in ((keep, core[0]), (send, 1 - core[0])):
        h = hidden[pl.ds(pl.multiple_of(which * half, half), half), :].astype(F32)
        weighted = h * gain[...]
        out[:half, :] = weighted.astype(BF16)
        squares = jnp.sum(jnp.transpose(h * h), axis=0, keepdims=True)
        largest = jnp.max(jnp.transpose(jnp.abs(weighted)), axis=0, keepdims=True)
        rows = []
        for v in (squares, largest):
            for part in split2(v):
                part = part.astype(F32)
                rows += [part[:, :128], part[:, 128:]]
        rows.append(jnp.zeros((STAT - len(rows), 128), F32))
        out[half:, :] = jnp.concatenate(rows, axis=0).astype(BF16)


def combine_kernel(core, keep, recv, out):
    half = keep.shape[0] - STAT
    first = core[0] == 0
    mine, other = keep[:half, :], recv[:half, :]
    left = jnp.where(first, mine.astype(F32), other.astype(F32)).astype(BF16)
    right = jnp.where(first, other.astype(F32), mine.astype(F32)).astype(BF16)
    a, b = keep[half:, :].astype(F32), recv[half:, :].astype(F32)

    def wide(s, r):
        return jnp.concatenate([s[r : r + 1], s[r + 1 : r + 2]], axis=1)

    squares = (wide(a, 0) + wide(a, 2)) + (wide(b, 0) + wide(b, 2))
    largest = jnp.maximum(wide(a, 4) + wide(a, 6), wide(b, 4) + wide(b, 6))
    rows = [p.astype(F32) for v in (squares, largest) for p in split2(v)]
    rows.append(jnp.zeros((STAT - len(rows), rows[0].shape[1]), F32))
    stats = jnp.concatenate(rows, axis=0).astype(BF16)
    for s in range(out.shape[0]):
        out[s, :half, :128] = left
        out[s, :half, 128:] = right
        out[s, half:, :] = stats


def block_at(core, i, side):
    return jnp.where(core == 0, i, (i % side) * side + i // side)


def kv_weights_kernel(core, kv, ko, kv_all, kvscale):
    n, rows2, kb = kv_all.shape
    rows = rows2 // 2
    side = math.isqrt(n)
    for i in range(n):
        at = pl.ds(pl.multiple_of(block_at(core[0], i, side) * kb, kb), kb)
        kv_all[i, :rows, :] = kv[:, at]
        kv_all[i, rows:, :] = ko[:, at]
    width = kvscale.shape[1]

    def scales(ref):
        s = ref[:, n * kb : n * kb + 128].astype(F32)
        s = (s[:, 0:1] + s[:, 1:2]) + s[:, 2:3]
        return jnp.broadcast_to(s, (rows, width))

    m, o = scales(kv), scales(ko)
    first = core[0] == 0
    k = rows // 2
    for j, (lo, hi) in enumerate(((0, k), (k, 2 * k))):
        a, b = m[lo:hi], o[lo:hi]
        kvscale[2 * j * k : (2 * j + 1) * k, :] = jnp.where(first, a, b)
        kvscale[(2 * j + 1) * k : (2 * j + 2) * k, :] = jnp.where(first, b, a)


def high_kernel(gathered, high):
    n = gathered.shape[0] // 2
    half = gathered.shape[1] - STAT
    squares, largest = 0.0, 0.0
    for i in range(2 * n):
        s = gathered[i, half:, :].astype(F32)
        squares = squares + (s[0:1] + s[1:2])
        largest = jnp.maximum(largest, s[2:3] + s[3:4])
        if i >= n:
            high[(i - n) * half : (i - n + 1) * half, :] = gathered[i, :half, :]
    rows = [p.astype(F32) for v in (squares, largest) for p in split2(v)]
    rows.append(jnp.zeros((STAT - len(rows), rows[0].shape[1]), F32))
    high[n * half :, :] = jnp.concatenate(rows, axis=0).astype(BF16)


def kv_rows(xs, kvs, kv_in, st_in):
    half = kv_in.shape[1]
    total = kv_in[...]
    squares, largest = st_in[0:1, :], st_in[1:2, :]
    for x, w in zip(xs, kvs):
        n = w.shape[0]
        for i in range(n):
            total = total + lax.dot_general(
                w[i],
                x[i * half : (i + 1) * half, :],
                (((1,), (1,)), ((), ())),
                preferred_element_type=F32,
            )
        if x.shape[0] > n * half:
            s = x[n * half :, :].astype(F32)
            squares = squares + (s[0:1] + s[1:2])
            largest = jnp.maximum(largest, s[2:3] + s[3:4])
    return total, squares, largest


def q_sum(xs, ws, q_in):
    half = q_in.shape[0]
    total = q_in[...]
    for x, w in zip(xs, ws):
        for i in range(w.shape[0]):
            total = total + jnp.dot(
                x[i * half : (i + 1) * half, :],
                jnp.concatenate([w[i, 0], w[i, 1]], axis=1),
                preferred_element_type=F32,
            )
    return total


def fetch(info, shifts, sems, xs, x_buf, weights=None, kv=None):
    copies = []
    used = iter(range(sems.shape[0]))

    def add(src, dst):
        copies.append(pltpu.make_async_copy(src, dst, sems.at[next(used)]))

    for i, (x, (s, k)) in enumerate(zip(xs, shifts)):
        add(x, x_buf.at[i, pl.ds(0, x.shape[0])])
        if kv is not None:
            whole, buf = kv
            n, side = buf.shape[1], math.isqrt(whole.shape[0])
            place = lax.rem(info[1] + (side - s % side), side)
            add(whole.at[pl.ds(place * side + k * n, n)], buf.at[i])
        if weights is not None:
            wq, wo, buf = weights
            n, side = buf.shape[1], math.isqrt(wq.shape[0])
            place = lax.rem(info[1] + (side - s % side), side)
            for j in range(n):
                b = jnp.where(info[0] == 0, place * side + k * n + j, (k * n + j) * side + place)
                add(wq.at[b], buf.at[i, j, 0])
                add(wo.at[b], buf.at[i, j, 1])
    for c in copies:
        c.start()
    for c in copies:
        c.wait()
    return [x_buf.at[i, pl.ds(0, x.shape[0])] for i, x in enumerate(xs)]


def matmul_kernel(shifts, info, *refs):
    m = len(shifts)
    xs, wq, wo, kv_all = refs[:m], *refs[m : m + 3]
    q_out, kv_out, st_out, x_buf, w_buf, kv_buf, sems = refs[-7:]
    if len(refs) == m + 10:
        q_in, kv_in, st_in = q_out, kv_out, st_out
        for out in (q_out, kv_out, st_out):
            out[...] = jnp.zeros_like(out)
    else:
        q_in, kv_in, st_in = refs[m + 3 : m + 6]
    xs = fetch(info, shifts, sems, xs, x_buf, (wq, wo, w_buf), (kv_all, kv_buf))
    ws, kvs = [w_buf.at[i] for i in range(m)], [kv_buf.at[i] for i in range(m)]
    q_out[...] = q_sum(xs, ws, q_in)
    total, squares, largest = kv_rows(xs, kvs, kv_in, st_in)
    kv_out[...] = total
    st_out[0:1, :] = squares
    st_out[1:2, :] = largest


def arrivals_call(kernel, out_shape, info, xs, weights, kv, rest, flops, aliases=None):
    m = len(xs)
    n = xs[0].shape[0] // xs[0].shape[1]
    big = [*weights, *kv]
    hbm = pl.BlockSpec(memory_space=pltpu.HBM)
    vmem = pl.BlockSpec(memory_space=pltpu.VMEM)
    smem = pl.BlockSpec(memory_space=pltpu.SMEM)
    scratch = [pltpu.VMEM((m, max(x.shape[0] for x in xs), xs[0].shape[1]), BF16)]
    if weights:
        scratch.append(pltpu.VMEM((m, n, 2) + weights[0].shape[1:], BF16))
    if kv:
        scratch.append(pltpu.VMEM((m, n) + kv[0].shape[1:], BF16))
    count = m * (1 + len(kv) + n * len(weights))
    return pl.pallas_call(
        kernel,
        out_shape=out_shape,
        in_specs=[smem] + [hbm] * (m + len(big)) + [vmem] * len(rest),
        out_specs=tuple(vmem for _ in out_shape),
        scratch_shapes=scratch + [pltpu.SemaphoreType.DMA((count,))],
        input_output_aliases=aliases or {},
        compiler_params=pltpu.CompilerParams(vmem_limit_bytes=RING_VMEM),
        cost_estimate=pl.CostEstimate(flops=flops, bytes_accessed=10**6, transcendentals=0),
    )(info, *xs, *big, *rest)


def matmul(half, info, shifts, xs, wq, wo, kv_all, acc):
    m = len(xs)
    out_shape = (
        jax.ShapeDtypeStruct((half, 2 * wq.shape[2]), F32),
        jax.ShapeDtypeStruct((kv_all.shape[1], half), F32),
        jax.ShapeDtypeStruct((8, half), F32),
    )
    return arrivals_call(
        lambda *refs: matmul_kernel(shifts, *refs),
        out_shape,
        info,
        xs,
        (wq, wo),
        (kv_all,),
        acc,
        2 * m * xs[0].shape[0] * xs[0].shape[1] * 288,
        {4 + m + i: i for i in range(len(acc))},
    )


def last_kv_kernel(d, shifts, info, *refs):
    m = len(shifts)
    xs, kv_all = refs[:m], refs[m]
    kv_in, st_in, kvscale, kcos, ksin, kvt, st_out, x_buf, kv_buf, sems = refs[m + 1 :]
    xs = fetch(info, shifts, sems, xs, x_buf, kv=(kv_all, kv_buf))
    t, squares, largest = kv_rows(xs, [kv_buf.at[i] for i in range(m)], kv_in, st_in)
    st_out[0:1, :] = squares
    st_out[1:2, :] = largest
    t = t * (1.0 / jnp.sqrt(squares / d + norm_eps))
    first = info[0] == 0
    mk, mv, ok, ov = t[0:8], t[8:16], t[16:24], t[24:32]
    a = jnp.concatenate([jnp.where(first, mk, ok), jnp.where(first, ok, mk)], axis=0)
    b = jnp.concatenate([jnp.where(first, mv, ov), jnp.where(first, ov, mv)], axis=0)
    a = a * kvscale[:16, :]
    b = b * kvscale[16:, :]
    row = lax.broadcasted_iota(jnp.int32, a.shape, 0)
    swapped = jnp.where(row % 2 == 0, -pltpu.roll(a, a.shape[0] - 1, 0), pltpu.roll(a, 1, 0))
    a = a * kcos[...] + swapped * ksin[...]
    both = jnp.concatenate([a, b], axis=0).astype(BF16)
    for s in range(kvt.shape[0]):
        kvt[s] = both


def last_kv(d, copies, info, shifts, xs, kv_all, kv, st, kvscale, kcos, ksin):
    out_shape = (
        jax.ShapeDtypeStruct((copies,) + kv.shape, BF16),
        jax.ShapeDtypeStruct(st.shape, F32),
    )
    return arrivals_call(
        lambda *refs: last_kv_kernel(d, shifts, *refs),
        out_shape,
        info,
        xs,
        (),
        (kv_all,),
        [kv, st, kvscale, kcos, ksin],
        10**9,
    )


def last_q_kernel(d, shifts, info, *refs):
    m = len(shifts)
    xs, wq, wo = refs[:m], refs[m], refs[m + 1]
    q_in, st, wscale, cosine, sine, mine, msg, x_buf, w_buf, sems = refs[m + 2 :]
    xs = fetch(info, shifts, sems, xs, x_buf, weights=(wq, wo, w_buf))
    q = q_sum(xs, [w_buf.at[i] for i in range(m)], q_in)
    half = q.shape[0]
    squares, largest = st[0:1, :], st[1:2, :]
    inv = columns_of(1.0 / jnp.sqrt(squares / d + norm_eps), 128)
    mine[...] = turn(q[:, :128] * inv * wscale[...], cosine[...], sine[...]).astype(BF16)
    msg[:half, :] = q[:, 128:] * inv
    msg[half:, :] = jnp.concatenate(
        [
            squares[:, :128],
            squares[:, 128:],
            largest[:, :128],
            largest[:, 128:],
            jnp.zeros((4, 128), F32),
        ],
        axis=0,
    )


def last_q(d, info, shifts, xs, wq, wo, q, st, wscale, cosine, sine):
    half = q.shape[0]
    out_shape = (
        jax.ShapeDtypeStruct((half, HD), BF16),
        jax.ShapeDtypeStruct((half + 8, HD), F32),
    )
    return arrivals_call(
        lambda *refs: last_q_kernel(d, shifts, *refs),
        out_shape,
        info,
        xs,
        (wq, wo),
        (),
        [q, st, wscale, cosine, sine],
        10**9,
    )


def turn(v, cosine, sine):
    lane = lax.broadcasted_iota(jnp.int32, v.shape, 1)
    width = v.shape[1]
    swapped = jnp.where(
        lane % 2 == 0, -pltpu.roll(v, width - 1, 1), pltpu.roll(v, 1, 1)
    )
    return v * cosine + swapped * sine


def columns_of(row, width):
    return jnp.transpose(jnp.broadcast_to(row, (width, row.shape[1])))


def token_kernel(d, core, mine, msg, st, hidden, gain, wscale, cosine, sine, queries, payload, scale):
    half = mine.shape[0]
    c = core[0]
    own = pl.ds(pl.multiple_of(c * half, half), half)
    far = pl.ds(pl.multiple_of((1 - c) * half, half), half)
    queries[own, :] = mine[...]
    queries[far, :] = turn(msg[:half, :] * wscale[...], cosine[...], sine[...]).astype(BF16)
    wide = lambda r: jnp.concatenate(
        [msg[half + r : half + r + 1], msg[half + r + 1 : half + r + 2]], axis=1
    )
    for rows, squares, largest, place in (
        (own, st[0:1, :], st[1:2, :], c),
        (far, wide(0), wide(2), 1 - c),
    ):
        inverse = 1.0 / jnp.sqrt(squares / d + norm_eps)
        row_scale = largest * inverse + tiny_eps
        scale[pl.ds(2 * place, 1), :] = row_scale[:, :128]
        scale[pl.ds(2 * place + 1, 1), :] = row_scale[:, 128:]
        inv = columns_of(inverse, 128)
        rs = columns_of(row_scale, 128)
        normed = hidden[rows, :].astype(F32) * gain[...] * inv
        payload[rows, :] = (normed / rs).astype(BF16)


def head_kernel(order, kvr, keys, values, whole):
    half = kvr.shape[2]
    chips = kvr.shape[0] // 2
    n = KV_COLS_DEV
    for part in range(2):
        at = slice(part * half, (part + 1) * half)
        for i in range(chips):
            rows = kvr[2 * i + part].astype(F32)
            for which in range(2):
                for slot in range(2):
                    to = pl.ds(pl.multiple_of(order[2 * i + slot] * n, n), n)
                    lo = (2 * which + slot) * n
                    whole[which, to, :] = rows[lo : lo + n]
        for which, out in enumerate((keys, values)):
            out[at, :] = jnp.transpose(whole[which]).astype(BF16)


def call(kernel, out_shape, core, *args, flops=0, scratch=()):
    return pl.pallas_call(
        kernel,
        out_shape=out_shape,
        in_specs=[pl.BlockSpec(memory_space=pltpu.SMEM)]
        + [pl.BlockSpec(memory_space=pltpu.VMEM)] * len(args),
        scratch_shapes=list(scratch),
        compiler_params=pltpu.CompilerParams(vmem_limit_bytes=VMEM),
        cost_estimate=pl.CostEstimate(flops=flops or 10**8, bytes_accessed=10**6, transcendentals=0),
    )(core, *args)


def solution(mesh):
    tp = mesh.shape["tp"]
    side = math.isqrt(tp // 2)
    row = 2 * side

    def index(y, x, c):
        return (y % side) * row + (x % side) * 2 + c

    everyone = [(y, x, c) for y in range(side) for x in range(side) for c in range(2)]
    to_partner = [(index(y, x, c), index(y, x, 1 - c)) for y, x, c in everyone]
    heads = tp * KV_COLS_DEV // HD
    columns = side // 2

    def home(j):
        y, x = j // row, (j // 2) % side
        return index(j % heads, x - 1 + (y + x) % columns, y // columns)

    to_row = [(j, home(j)) for j in range(tp)]
    first_groups = [[index(y, x, 0) for x in range(side)] for y in range(side)]
    first_groups += [[index(y, x, 1) for y in range(side)] for x in range(side)]
    rows = [[y * row + i for i in range(row)] for y in range(side)]

    def second(v, s):
        pairs = [
            (index(y, x, c), index(y + s, x, c) if c == 0 else index(y, x + s, c))
            for y, x, c in everyone
        ]
        return lax.ppermute(v, "tp", pairs)

    def swap(v):
        return lax.ppermute(v, "tp", to_partner)

    def body(hidden, norm_gain, prefix, w_query, w_kv, w_scale):
        count, width = hidden.shape
        d = width * tp
        half = count // 2
        me = lax.axis_index("tp")
        core = me % 2
        x = (me // 2) % side
        y = me // row
        core1 = core[None].astype(jnp.int32)
        gain = norm_gain[None, :]

        def piece_at(xs, slot):
            base = y // 2
            h = jnp.where((xs - base + 1) % side < columns, 0, 1)
            source = base + columns * h
            o = (xs - source + 1) % side
            return 2 * ((o - source) % columns + columns * slot) + h

        blk = jax.ShapeDtypeStruct((half + STAT, width), BF16)
        keep, send = call(prep_kernel, (blk, blk), core1, hidden, gain)
        recv = swap(send)
        kvs = w_scale[HD:]
        hi = kvs.astype(BF16)
        mid = kvs - hi.astype(F32)
        mid, lo = mid.astype(BF16), (mid - mid.astype(BF16).astype(F32)).astype(BF16)
        scales = jnp.pad(jnp.stack([hi, mid, lo], axis=1), ((0, 0), (0, 125)))
        kv_mine = lax.ppermute(jnp.concatenate([w_kv, scales], axis=1), "tp", to_row)
        wq_other = swap(w_query)
        slots = call(
            combine_kernel,
            jax.ShapeDtypeStruct((side, half + STAT, 2 * width), BF16),
            core1,
            keep,
            recv,
        )
        gathered = lax.all_to_all(
            slots, "tp", split_axis=0, concat_axis=0, tiled=False, axis_index_groups=first_groups
        )
        positions = (prefix[0] + jnp.arange(count, dtype=jnp.int32)).astype(F32)
        pos_own = lax.dynamic_slice_in_dim(positions, core * half, half)
        pos_far = lax.dynamic_slice_in_dim(positions, (1 - core) * half, half)

        def freq(columns):
            pair = (columns % HD // 2).astype(F32)
            return jnp.power(F32(rope_base), -(2.0 * pair) / HD)

        fq = freq(jnp.arange(HD, dtype=jnp.int32))
        ang_own = pos_own[:, None] * fq[None, :]
        ang_far = pos_far[:, None] * fq[None, :]
        slots_of = jnp.arange(2 * KV_COLS_DEV, dtype=jnp.int32)
        fk = freq(piece_at(x, slots_of // KV_COLS_DEV) * KV_COLS_DEV + slots_of % KV_COLS_DEV)
        seats = jnp.arange(row, dtype=jnp.int32)
        order = piece_at(seats // 2, seats % 2).astype(jnp.int32)
        ang_k = fk[:, None] * pos_own[None, :]
        qscale = w_scale[None, :HD]
        tables = (
            jnp.cos(ang_own),
            jnp.sin(ang_own),
            jnp.cos(ang_far),
            jnp.sin(ang_far),
            jnp.cos(ang_k),
            jnp.sin(ang_k),
        )
        coord = jnp.where(core == 0, y, x)

        info = jnp.stack([core, coord]).astype(jnp.int32)
        wq = w_query.reshape(-1, 2 * width, HD)
        wo = wq_other.reshape(-1, 2 * width, HD)
        gathered, wo, tables, info, order, qscale = lax.optimization_barrier(
            (gathered, wo, tables, info, order, qscale)
        )
        cos_own, sin_own, cos_far, sin_far, cos_k, sin_k = tables

        n = side // 2
        low = gathered[:n, :half].reshape(n * half, -1)
        high = pl.pallas_call(
            high_kernel,
            out_shape=jax.ShapeDtypeStruct((n * half + STAT, gathered.shape[2]), BF16),
            compiler_params=pltpu.CompilerParams(vmem_limit_bytes=VMEM),
            cost_estimate=pl.CostEstimate(flops=10**8, bytes_accessed=10**6, transcendentals=0),
        )(gathered)

        def mm(acc, items):
            shifts = [(s, k) for s, k, _ in items]
            return matmul(half, info, shifts, [v for _, _, v in items], wq, wo, kv_all, acc)

        up, down = [second(low, 1)], [second(low, -1)]
        up.append(second(high, 1))
        down.append(second(high, -1))
        kv_other = swap(kv_mine)
        kv_all, kvscale = call(
            kv_weights_kernel,
            (
                jax.ShapeDtypeStruct((d // (2 * width), 4 * KV_COLS_DEV, 2 * width), BF16),
                jax.ShapeDtypeStruct((4 * KV_COLS_DEV, half), F32),
            ),
            info,
            kv_mine,
            kv_other,
        )
        acc = mm((), [(0, 0, low), (0, 1, high)])
        last_round = side // 2
        for r in range(1, last_round):
            for k in range(2):
                items = [(r, k, up[k]), (-r, k, down[k])]
                up[k], down[k], acc = lax.optimization_barrier((up[k], down[k], acc))
                if r + 1 < last_round:
                    up[k], down[k] = second(up[k], 1), second(down[k], -1)
                elif k == 0:
                    up[k] = second(up[k], 1)
                else:
                    down[k] = second(down[k], -1)
                acc = mm(acc, items)
        items = [(last_round, 0, up[0]), (-last_round, 1, down[1])]
        xs = [v for _, _, v in items]
        shifts = [(s, k) for s, k, _ in items]
        kvt, st = last_kv(
            d, row, info, shifts, xs, kv_all, acc[1], acc[2], kvscale, cos_k, sin_k
        )
        kvr = lax.all_to_all(
            kvt, "tp", split_axis=0, concat_axis=0, tiled=False, axis_index_groups=rows
        )
        mine, msg = last_q(d, info, shifts, xs, wq, wo, acc[0], st, qscale, cos_own, sin_own)
        far = swap(msg)
        out = jax.ShapeDtypeStruct((count, HD), BF16)
        queries, payload, scale = call(
            lambda *r: token_kernel(d, *r),
            (out, out, jax.ShapeDtypeStruct((count // HD, HD), F32)),
            info,
            mine,
            far,
            st,
            hidden,
            gain,
            qscale,
            cos_far,
            sin_far,
        )
        keys, values = call(
            head_kernel, (out, out), order, kvr, scratch=[pltpu.VMEM((2, HD, half), F32)]
        )
        return queries, keys, values, payload, scale.reshape(count)

    return jax.shard_map(
        body,
        mesh=mesh,
        in_specs=(P("grp", "tp"), P("tp"), P("grp"), P(None, "tp"), P("tp", None), P("tp")),
        out_specs=(P("grp", "tp"), P("grp", "tp"), P("grp", "tp"), P("grp", "tp"), P("grp")),
        check_vma=False,
    )
```

```python
import math

import jax
import jax.numpy as jnp
from jax import lax
from jax.experimental import pallas as pl
from jax.experimental.pallas import tpu as pltpu
from jax.sharding import PartitionSpec as P


HD = 128
KV_COLS_DEV = 8
norm_eps = 1e-05
tiny_eps = 1e-06
rope_base = 500000.0

VMEM = 24 * 2**20
RING_VMEM = 48 * 2**20

F32 = jnp.float32
BF16 = jnp.bfloat16
STAT = 16


def split2(v):
    hi = v.astype(BF16)
    return hi, (v - hi.astype(F32)).astype(BF16)


def prep_kernel(core, hidden, gain, keep, send):
    half = keep.shape[0] - STAT
    for out, which in ((keep, core[0]), (send, 1 - core[0])):
        h = hidden[pl.ds(pl.multiple_of(which * half, half), half), :].astype(F32)
        weighted = h * gain[...]
        out[:half, :] = weighted.astype(BF16)
        squares = jnp.sum(jnp.transpose(h * h), axis=0, keepdims=True)
        largest = jnp.max(jnp.transpose(jnp.abs(weighted)), axis=0, keepdims=True)
        rows = []
        for v in (squares, largest):
            for part in split2(v):
                part = part.astype(F32)
                rows += [part[:, :128], part[:, 128:]]
        rows.append(jnp.zeros((STAT - len(rows), 128), F32))
        out[half:, :] = jnp.concatenate(rows, axis=0).astype(BF16)


def combine_kernel(core, keep, recv, out):
    half = keep.shape[0] - STAT
    first = core[0] == 0
    mine, other = keep[:half, :], recv[:half, :]
    left = jnp.where(first, mine.astype(F32), other.astype(F32)).astype(BF16)
    right = jnp.where(first, other.astype(F32), mine.astype(F32)).astype(BF16)
    a, b = keep[half:, :].astype(F32), recv[half:, :].astype(F32)

    def wide(s, r):
        return jnp.concatenate([s[r : r + 1], s[r + 1 : r + 2]], axis=1)

    squares = (wide(a, 0) + wide(a, 2)) + (wide(b, 0) + wide(b, 2))
    largest = jnp.maximum(wide(a, 4) + wide(a, 6), wide(b, 4) + wide(b, 6))
    rows = [p.astype(F32) for v in (squares, largest) for p in split2(v)]
    rows.append(jnp.zeros((STAT - len(rows), rows[0].shape[1]), F32))
    stats = jnp.concatenate(rows, axis=0).astype(BF16)
    for s in range(out.shape[0]):
        out[s, :half, :128] = left
        out[s, :half, 128:] = right
        out[s, half:, :] = stats


def block_at(core, i, side):
    return jnp.where(core == 0, i, (i % side) * side + i // side)


def weights_kernel(info, wq, wo, w_all, w_buf, sems):
    n = w_buf.shape[0]
    hw = wq.shape[2]
    side = math.isqrt(n)

    def fetches(i):
        b = block_at(info[0], i, side)
        return (
            pltpu.make_async_copy(wq.at[b], w_buf.at[i, :, pl.ds(0, hw)], sems.at[0, i]),
            pltpu.make_async_copy(wo.at[b], w_buf.at[i, :, pl.ds(hw, hw)], sems.at[1, i]),
        )

    def store(i):
        return pltpu.make_async_copy(w_buf.at[i], w_all.at[i], sems.at[2, i])

    @pl.loop(0, n)
    def _(i):
        for c in fetches(i):
            c.start()

    @pl.loop(0, n)
    def _(i):
        for c in fetches(i):
            c.wait()
        store(i).start()

    @pl.loop(0, n)
    def _(i):
        store(i).wait()


def arrange_weights(info, wq, wo):
    n, kb, hw = wq.shape
    hbm = pl.BlockSpec(memory_space=pltpu.HBM)
    out = jax.ShapeDtypeStruct((n, kb, 2 * hw), BF16)
    return pl.pallas_call(
        weights_kernel,
        out_shape=out,
        in_specs=[pl.BlockSpec(memory_space=pltpu.SMEM), hbm, hbm],
        out_specs=hbm,
        scratch_shapes=[pltpu.VMEM(out.shape, out.dtype), pltpu.SemaphoreType.DMA((3, n))],
        compiler_params=pltpu.CompilerParams(vmem_limit_bytes=60 * 2**20),
        cost_estimate=pl.CostEstimate(flops=10**9, bytes_accessed=2 * 10**7, transcendentals=0),
    )(info, wq, wo)


def kv_weights_kernel(core, kv, ko, kv_all, kvscale):
    n, rows2, kb = kv_all.shape
    rows = rows2 // 2
    side = math.isqrt(n)
    for i in range(n):
        at = pl.ds(pl.multiple_of(block_at(core[0], i, side) * kb, kb), kb)
        kv_all[i, :rows, :] = kv[:, at]
        kv_all[i, rows:, :] = ko[:, at]
    width = kvscale.shape[1]

    def scales(ref):
        s = ref[:, n * kb : n * kb + 128].astype(F32)
        s = (s[:, 0:1] + s[:, 1:2]) + s[:, 2:3]
        return jnp.broadcast_to(s, (rows, width))

    m, o = scales(kv), scales(ko)
    first = core[0] == 0
    k = rows // 2
    for j, (lo, hi) in enumerate(((0, k), (k, 2 * k))):
        a, b = m[lo:hi], o[lo:hi]
        kvscale[2 * j * k : (2 * j + 1) * k, :] = jnp.where(first, a, b)
        kvscale[(2 * j + 1) * k : (2 * j + 2) * k, :] = jnp.where(first, b, a)


def high_kernel(gathered, high):
    n = gathered.shape[0] // 2
    half = gathered.shape[1] - STAT
    squares, largest = 0.0, 0.0
    for i in range(2 * n):
        s = gathered[i, half:, :].astype(F32)
        squares = squares + (s[0:1] + s[1:2])
        largest = jnp.maximum(largest, s[2:3] + s[3:4])
        if i >= n:
            high[(i - n) * half : (i - n + 1) * half, :] = gathered[i, :half, :]
    rows = [p.astype(F32) for v in (squares, largest) for p in split2(v)]
    rows.append(jnp.zeros((STAT - len(rows), rows[0].shape[1]), F32))
    high[n * half :, :] = jnp.concatenate(rows, axis=0).astype(BF16)


def kv_rows(xs, kvs, kv_in, st_in):
    half = kv_in.shape[1]
    total = kv_in[...]
    squares, largest = st_in[0:1, :], st_in[1:2, :]
    for x, w in zip(xs, kvs):
        n = w.shape[0]
        for i in range(n):
            total = total + lax.dot_general(
                w[i],
                x[i * half : (i + 1) * half, :],
                (((1,), (1,)), ((), ())),
                preferred_element_type=F32,
            )
        if x.shape[0] > n * half:
            s = x[n * half :, :].astype(F32)
            squares = squares + (s[0:1] + s[1:2])
            largest = jnp.maximum(largest, s[2:3] + s[3:4])
    return total, squares, largest


def q_sum(xs, ws, q_in):
    half = q_in.shape[0]
    total = q_in[...]
    for x, w in zip(xs, ws):
        for i in range(w.shape[0]):
            total = total + jnp.dot(
                x[i * half : (i + 1) * half, :],
                w[i],
                preferred_element_type=F32,
            )
    return total


def fetch(info, shifts, sems, xs, x_buf, *pairs):
    copies = []
    used = iter(range(sems.shape[0]))

    def add(src, dst):
        copies.append(pltpu.make_async_copy(src, dst, sems.at[next(used)]))

    for i, (x, (s, k)) in enumerate(zip(xs, shifts)):
        add(x, x_buf.at[i, pl.ds(0, x.shape[0])])
        for whole, buf in pairs:
            n, side = buf.shape[1], math.isqrt(whole.shape[0])
            place = lax.rem(info[1] + (side - s % side), side)
            add(whole.at[pl.ds(place * side + k * n, n)], buf.at[i])
    for c in copies:
        c.start()
    for c in copies:
        c.wait()
    return [x_buf.at[i, pl.ds(0, x.shape[0])] for i, x in enumerate(xs)]


def matmul_kernel(shifts, info, *refs):
    m = len(shifts)
    xs, w_all, kv_all = refs[:m], refs[m], refs[m + 1]
    q_out, kv_out, st_out, x_buf, w_buf, kv_buf, sems = refs[-7:]
    if len(refs) == m + 9:
        q_in, kv_in, st_in = q_out, kv_out, st_out
        for out in (q_out, kv_out, st_out):
            out[...] = jnp.zeros_like(out)
    else:
        q_in, kv_in, st_in = refs[m + 2 : m + 5]
    xs = fetch(info, shifts, sems, xs, x_buf, (w_all, w_buf), (kv_all, kv_buf))
    ws, kvs = [w_buf.at[i] for i in range(m)], [kv_buf.at[i] for i in range(m)]
    q_out[...] = q_sum(xs, ws, q_in)
    total, squares, largest = kv_rows(xs, kvs, kv_in, st_in)
    kv_out[...] = total
    st_out[0:1, :] = squares
    st_out[1:2, :] = largest


def arrivals_call(kernel, out_shape, info, xs, big, rest, flops, aliases=None):
    m = len(xs)
    n = xs[0].shape[0] // xs[0].shape[1]
    hbm = pl.BlockSpec(memory_space=pltpu.HBM)
    vmem = pl.BlockSpec(memory_space=pltpu.VMEM)
    smem = pl.BlockSpec(memory_space=pltpu.SMEM)
    scratch = [pltpu.VMEM((m, max(x.shape[0] for x in xs), xs[0].shape[1]), BF16)]
    scratch += [pltpu.VMEM((m, n) + w.shape[1:], BF16) for w in big]
    count = m * (1 + len(big))
    return pl.pallas_call(
        kernel,
        out_shape=out_shape,
        in_specs=[smem] + [hbm] * (m + len(big)) + [vmem] * len(rest),
        out_specs=tuple(vmem for _ in out_shape),
        scratch_shapes=scratch + [pltpu.SemaphoreType.DMA((count,))],
        input_output_aliases=aliases or {},
        compiler_params=pltpu.CompilerParams(vmem_limit_bytes=RING_VMEM),
        cost_estimate=pl.CostEstimate(flops=flops, bytes_accessed=10**6, transcendentals=0),
    )(info, *xs, *big, *rest)


def matmul(half, info, shifts, xs, w_all, kv_all, acc):
    m = len(xs)
    out_shape = (
        jax.ShapeDtypeStruct((half, w_all.shape[2]), F32),
        jax.ShapeDtypeStruct((kv_all.shape[1], half), F32),
        jax.ShapeDtypeStruct((8, half), F32),
    )
    return arrivals_call(
        lambda *refs: matmul_kernel(shifts, *refs),
        out_shape,
        info,
        xs,
        (w_all, kv_all),
        acc,
        2 * m * xs[0].shape[0] * xs[0].shape[1] * 288,
        {3 + m + i: i for i in range(len(acc))},
    )


def last_kv_kernel(d, shifts, info, *refs):
    m = len(shifts)
    xs, kv_all = refs[:m], refs[m]
    kv_in, st_in, kvscale, kcos, ksin, kvt, st_out, x_buf, kv_buf, sems = refs[m + 1 :]
    xs = fetch(info, shifts, sems, xs, x_buf, (kv_all, kv_buf))
    t, squares, largest = kv_rows(xs, [kv_buf.at[i] for i in range(m)], kv_in, st_in)
    st_out[0:1, :] = squares
    st_out[1:2, :] = largest
    t = t * (1.0 / jnp.sqrt(squares / d + norm_eps))
    first = info[0] == 0
    mk, mv, ok, ov = t[0:8], t[8:16], t[16:24], t[24:32]
    a = jnp.concatenate([jnp.where(first, mk, ok), jnp.where(first, ok, mk)], axis=0)
    b = jnp.concatenate([jnp.where(first, mv, ov), jnp.where(first, ov, mv)], axis=0)
    a = a * kvscale[:16, :]
    b = b * kvscale[16:, :]
    row = lax.broadcasted_iota(jnp.int32, a.shape, 0)
    swapped = jnp.where(row % 2 == 0, -pltpu.roll(a, a.shape[0] - 1, 0), pltpu.roll(a, 1, 0))
    a = a * kcos[...] + swapped * ksin[...]
    both = jnp.concatenate([a, b], axis=0).astype(BF16)
    for s in range(kvt.shape[0]):
        kvt[s] = both


def last_kv(d, copies, info, shifts, xs, kv_all, kv, st, kvscale, kcos, ksin):
    out_shape = (
        jax.ShapeDtypeStruct((copies,) + kv.shape, BF16),
        jax.ShapeDtypeStruct(st.shape, F32),
    )
    return arrivals_call(
        lambda *refs: last_kv_kernel(d, shifts, *refs),
        out_shape,
        info,
        xs,
        (kv_all,),
        [kv, st, kvscale, kcos, ksin],
        10**9,
    )


def last_q_kernel(d, shifts, info, *refs):
    m = len(shifts)
    xs, w_all = refs[:m], refs[m]
    q_in, st, wscale, cosine, sine, mine, msg, x_buf, w_buf, sems = refs[m + 1 :]
    xs = fetch(info, shifts, sems, xs, x_buf, (w_all, w_buf))
    q = q_sum(xs, [w_buf.at[i] for i in range(m)], q_in)
    half = q.shape[0]
    squares, largest = st[0:1, :], st[1:2, :]
    inv = columns_of(1.0 / jnp.sqrt(squares / d + norm_eps), 128)
    mine[...] = turn(q[:, :128] * inv * wscale[...], cosine[...], sine[...]).astype(BF16)
    msg[:half, :] = q[:, 128:] * inv
    msg[half:, :] = jnp.concatenate(
        [
            squares[:, :128],
            squares[:, 128:],
            largest[:, :128],
            largest[:, 128:],
            jnp.zeros((4, 128), F32),
        ],
        axis=0,
    )


def last_q(d, info, shifts, xs, w_all, q, st, wscale, cosine, sine):
    half = q.shape[0]
    out_shape = (
        jax.ShapeDtypeStruct((half, HD), BF16),
        jax.ShapeDtypeStruct((half + 8, HD), F32),
    )
    return arrivals_call(
        lambda *refs: last_q_kernel(d, shifts, *refs),
        out_shape,
        info,
        xs,
        (w_all,),
        [q, st, wscale, cosine, sine],
        10**9,
    )


def turn(v, cosine, sine):
    lane = lax.broadcasted_iota(jnp.int32, v.shape, 1)
    width = v.shape[1]
    swapped = jnp.where(
        lane % 2 == 0, -pltpu.roll(v, width - 1, 1), pltpu.roll(v, 1, 1)
    )
    return v * cosine + swapped * sine


def columns_of(row, width):
    return jnp.transpose(jnp.broadcast_to(row, (width, row.shape[1])))


def token_kernel(d, core, mine, msg, st, hidden, gain, wscale, cosine, sine, queries, payload, scale):
    half = mine.shape[0]
    c = core[0]
    own = pl.ds(pl.multiple_of(c * half, half), half)
    far = pl.ds(pl.multiple_of((1 - c) * half, half), half)
    queries[own, :] = mine[...]
    queries[far, :] = turn(msg[:half, :] * wscale[...], cosine[...], sine[...]).astype(BF16)
    wide = lambda r: jnp.concatenate(
        [msg[half + r : half + r + 1], msg[half + r + 1 : half + r + 2]], axis=1
    )
    for rows, squares, largest, place in (
        (own, st[0:1, :], st[1:2, :], c),
        (far, wide(0), wide(2), 1 - c),
    ):
        inverse = 1.0 / jnp.sqrt(squares / d + norm_eps)
        row_scale = largest * inverse + tiny_eps
        scale[pl.ds(2 * place, 1), :] = row_scale[:, :128]
        scale[pl.ds(2 * place + 1, 1), :] = row_scale[:, 128:]
        inv = columns_of(inverse, 128)
        rs = columns_of(row_scale, 128)
        normed = hidden[rows, :].astype(F32) * gain[...] * inv
        payload[rows, :] = (normed / rs).astype(BF16)


def head_kernel(order, kvr, keys, values, whole):
    half = kvr.shape[2]
    chips = kvr.shape[0] // 2
    n = KV_COLS_DEV
    for part in range(2):
        at = slice(part * half, (part + 1) * half)
        for i in range(chips):
            rows = kvr[2 * i + part].astype(F32)
            for which in range(2):
                for slot in range(2):
                    to = pl.ds(pl.multiple_of(order[2 * i + slot] * n, n), n)
                    lo = (2 * which + slot) * n
                    whole[which, to, :] = rows[lo : lo + n]
        for which, out in enumerate((keys, values)):
            out[at, :] = jnp.transpose(whole[which]).astype(BF16)


def call(kernel, out_shape, core, *args, flops=0, scratch=()):
    return pl.pallas_call(
        kernel,
        out_shape=out_shape,
        in_specs=[pl.BlockSpec(memory_space=pltpu.SMEM)]
        + [pl.BlockSpec(memory_space=pltpu.VMEM)] * len(args),
        scratch_shapes=list(scratch),
        compiler_params=pltpu.CompilerParams(vmem_limit_bytes=VMEM),
        cost_estimate=pl.CostEstimate(flops=flops or 10**8, bytes_accessed=10**6, transcendentals=0),
    )(core, *args)


def solution(mesh):
    tp = mesh.shape["tp"]
    side = math.isqrt(tp // 2)
    row = 2 * side

    def index(y, x, c):
        return (y % side) * row + (x % side) * 2 + c

    everyone = [(y, x, c) for y in range(side) for x in range(side) for c in range(2)]
    to_partner = [(index(y, x, c), index(y, x, 1 - c)) for y, x, c in everyone]
    heads = tp * KV_COLS_DEV // HD
    columns = side // 2

    def home(j):
        y, x = j // row, (j // 2) % side
        return index(j % heads, x - 1 + (y + x) % columns, y // columns)

    to_row = [(j, home(j)) for j in range(tp)]
    first_groups = [[index(y, x, 0) for x in range(side)] for y in range(side)]
    first_groups += [[index(y, x, 1) for y in range(side)] for x in range(side)]
    rows = [[y * row + i for i in range(row)] for y in range(side)]

    def second(v, s):
        pairs = [
            (index(y, x, c), index(y + s, x, c) if c == 0 else index(y, x + s, c))
            for y, x, c in everyone
        ]
        return lax.ppermute(v, "tp", pairs)

    def swap(v):
        return lax.ppermute(v, "tp", to_partner)

    def body(hidden, norm_gain, prefix, w_query, w_kv, w_scale):
        count, width = hidden.shape
        d = width * tp
        half = count // 2
        me = lax.axis_index("tp")
        core = me % 2
        x = (me // 2) % side
        y = me // row
        core1 = core[None].astype(jnp.int32)
        gain = norm_gain[None, :]

        def piece_at(xs, slot):
            base = y // 2
            h = jnp.where((xs - base + 1) % side < columns, 0, 1)
            source = base + columns * h
            o = (xs - source + 1) % side
            return 2 * ((o - source) % columns + columns * slot) + h

        blk = jax.ShapeDtypeStruct((half + STAT, width), BF16)
        keep, send = call(prep_kernel, (blk, blk), core1, hidden, gain)
        recv = swap(send)
        kvs = w_scale[HD:]
        hi = kvs.astype(BF16)
        mid = kvs - hi.astype(F32)
        mid, lo = mid.astype(BF16), (mid - mid.astype(BF16).astype(F32)).astype(BF16)
        scales = jnp.pad(jnp.stack([hi, mid, lo], axis=1), ((0, 0), (0, 125)))
        kv_mine = lax.ppermute(jnp.concatenate([w_kv, scales], axis=1), "tp", to_row)
        wq_other = swap(w_query)
        slots = call(
            combine_kernel,
            jax.ShapeDtypeStruct((side, half + STAT, 2 * width), BF16),
            core1,
            keep,
            recv,
        )
        gathered = lax.all_to_all(
            slots, "tp", split_axis=0, concat_axis=0, tiled=False, axis_index_groups=first_groups
        )
        positions = (prefix[0] + jnp.arange(count, dtype=jnp.int32)).astype(F32)
        pos_own = lax.dynamic_slice_in_dim(positions, core * half, half)
        pos_far = lax.dynamic_slice_in_dim(positions, (1 - core) * half, half)

        def freq(columns):
            pair = (columns % HD // 2).astype(F32)
            return jnp.power(F32(rope_base), -(2.0 * pair) / HD)

        fq = freq(jnp.arange(HD, dtype=jnp.int32))
        ang_own = pos_own[:, None] * fq[None, :]
        ang_far = pos_far[:, None] * fq[None, :]
        slots_of = jnp.arange(2 * KV_COLS_DEV, dtype=jnp.int32)
        fk = freq(piece_at(x, slots_of // KV_COLS_DEV) * KV_COLS_DEV + slots_of % KV_COLS_DEV)
        seats = jnp.arange(row, dtype=jnp.int32)
        order = piece_at(seats // 2, seats % 2).astype(jnp.int32)
        ang_k = fk[:, None] * pos_own[None, :]
        qscale = w_scale[None, :HD]
        tables = (
            jnp.cos(ang_own),
            jnp.sin(ang_own),
            jnp.cos(ang_far),
            jnp.sin(ang_far),
            jnp.cos(ang_k),
            jnp.sin(ang_k),
        )
        coord = jnp.where(core == 0, y, x)

        info = jnp.stack([core, coord]).astype(jnp.int32)
        w_all = arrange_weights(
            info, w_query.reshape(-1, 2 * width, HD), wq_other.reshape(-1, 2 * width, HD)
        )
        gathered, w_all, tables, info, order, qscale = lax.optimization_barrier(
            (gathered, w_all, tables, info, order, qscale)
        )
        cos_own, sin_own, cos_far, sin_far, cos_k, sin_k = tables

        n = side // 2
        low = gathered[:n, :half].reshape(n * half, -1)
        high = pl.pallas_call(
            high_kernel,
            out_shape=jax.ShapeDtypeStruct((n * half + STAT, gathered.shape[2]), BF16),
            compiler_params=pltpu.CompilerParams(vmem_limit_bytes=VMEM),
            cost_estimate=pl.CostEstimate(flops=10**8, bytes_accessed=10**6, transcendentals=0),
        )(gathered)

        def mm(acc, items):
            shifts = [(s, k) for s, k, _ in items]
            return matmul(half, info, shifts, [v for _, _, v in items], w_all, kv_all, acc)

        up, down = [second(low, 1)], [second(low, -1)]
        up.append(second(high, 1))
        down.append(second(high, -1))
        kv_other = swap(kv_mine)
        kv_all, kvscale = call(
            kv_weights_kernel,
            (
                jax.ShapeDtypeStruct((d // (2 * width), 4 * KV_COLS_DEV, 2 * width), BF16),
                jax.ShapeDtypeStruct((4 * KV_COLS_DEV, half), F32),
            ),
            info,
            kv_mine,
            kv_other,
        )
        acc = mm((), [(0, 0, low), (0, 1, high)])
        last_round = side // 2
        for r in range(1, last_round):
            for k in range(2):
                items = [(r, k, up[k]), (-r, k, down[k])]
                up[k], down[k], acc = lax.optimization_barrier((up[k], down[k], acc))
                if r + 1 < last_round:
                    up[k], down[k] = second(up[k], 1), second(down[k], -1)
                elif k == 0:
                    up[k] = second(up[k], 1)
                else:
                    down[k] = second(down[k], -1)
                acc = mm(acc, items)
        items = [(last_round, 0, up[0]), (-last_round, 1, down[1])]
        xs = [v for _, _, v in items]
        shifts = [(s, k) for s, k, _ in items]
        kvt, st = last_kv(
            d, row, info, shifts, xs, kv_all, acc[1], acc[2], kvscale, cos_k, sin_k
        )
        kvr = lax.all_to_all(
            kvt, "tp", split_axis=0, concat_axis=0, tiled=False, axis_index_groups=rows
        )
        mine, msg = last_q(d, info, shifts, xs, w_all, acc[0], st, qscale, cos_own, sin_own)
        far = swap(msg)
        out = jax.ShapeDtypeStruct((count, HD), BF16)
        queries, payload, scale = call(
            lambda *r: token_kernel(d, *r),
            (out, out, jax.ShapeDtypeStruct((count // HD, HD), F32)),
            info,
            mine,
            far,
            st,
            hidden,
            gain,
            qscale,
            cos_far,
            sin_far,
        )
        keys, values = call(
            head_kernel, (out, out), order, kvr, scratch=[pltpu.VMEM((2, HD, half), F32)]
        )
        return queries, keys, values, payload, scale.reshape(count)

    return jax.shard_map(
        body,
        mesh=mesh,
        in_specs=(P("grp", "tp"), P("tp"), P("grp"), P(None, "tp"), P("tp", None), P("tp")),
        out_specs=(P("grp", "tp"), P("grp", "tp"), P("grp", "tp"), P("grp", "tp"), P("grp")),
        check_vma=False,
    )
```

```python
import math

import jax
import jax.numpy as jnp
from jax import lax
from jax.experimental import pallas as pl
from jax.experimental.pallas import tpu as pltpu
from jax.sharding import PartitionSpec as P


HD = 128
KV_COLS_DEV = 8
norm_eps = 1e-05
tiny_eps = 1e-06
rope_base = 500000.0

VMEM = 24 * 2**20
RING_VMEM = 48 * 2**20

F32 = jnp.float32
BF16 = jnp.bfloat16
STAT = 16


def split2(v):
    hi = v.astype(BF16)
    return hi, (v - hi.astype(F32)).astype(BF16)


def prep_kernel(core, hidden, gain, keep, send):
    half = keep.shape[0] - STAT
    for out, which in ((keep, core[0]), (send, 1 - core[0])):
        h = hidden[pl.ds(pl.multiple_of(which * half, half), half), :].astype(F32)
        weighted = h * gain[...]
        out[:half, :] = weighted.astype(BF16)
        squares = jnp.sum(jnp.transpose(h * h), axis=0, keepdims=True)
        largest = jnp.max(jnp.transpose(jnp.abs(weighted)), axis=0, keepdims=True)
        rows = []
        for v in (squares, largest):
            for part in split2(v):
                part = part.astype(F32)
                rows += [part[:, :128], part[:, 128:]]
        rows.append(jnp.zeros((STAT - len(rows), 128), F32))
        out[half:, :] = jnp.concatenate(rows, axis=0).astype(BF16)


def combine_kernel(core, keep, recv, out):
    half = keep.shape[0] - STAT
    first = core[0] == 0
    mine, other = keep[:half, :], recv[:half, :]
    left = jnp.where(first, mine.astype(F32), other.astype(F32)).astype(BF16)
    right = jnp.where(first, other.astype(F32), mine.astype(F32)).astype(BF16)
    a, b = keep[half:, :].astype(F32), recv[half:, :].astype(F32)

    def wide(s, r):
        return jnp.concatenate([s[r : r + 1], s[r + 1 : r + 2]], axis=1)

    squares = (wide(a, 0) + wide(a, 2)) + (wide(b, 0) + wide(b, 2))
    largest = jnp.maximum(wide(a, 4) + wide(a, 6), wide(b, 4) + wide(b, 6))
    rows = [p.astype(F32) for v in (squares, largest) for p in split2(v)]
    rows.append(jnp.zeros((STAT - len(rows), rows[0].shape[1]), F32))
    stats = jnp.concatenate(rows, axis=0).astype(BF16)
    for s in range(out.shape[0]):
        out[s, :half, :128] = left
        out[s, :half, 128:] = right
        out[s, half:, :] = stats


def block_at(core, i, side):
    return jnp.where(core == 0, i, (i % side) * side + i // side)


def weights_kernel(info, wq, wo, w_all, w_buf, sems):
    n = w_buf.shape[0]
    hw = wq.shape[2]
    side = math.isqrt(n)

    def fetches(i):
        b = block_at(info[0], i, side)
        return (
            pltpu.make_async_copy(wq.at[b], w_buf.at[i, :, pl.ds(0, hw)], sems.at[0, i]),
            pltpu.make_async_copy(wo.at[b], w_buf.at[i, :, pl.ds(hw, hw)], sems.at[1, i]),
        )

    def store(i):
        return pltpu.make_async_copy(w_buf.at[i], w_all.at[i], sems.at[2, i])

    @pl.loop(0, n)
    def _(i):
        for c in fetches(i):
            c.start()

    @pl.loop(0, n)
    def _(i):
        for c in fetches(i):
            c.wait()
        store(i).start()

    @pl.loop(0, n)
    def _(i):
        store(i).wait()


def arrange_weights(info, wq, wo):
    n, kb, hw = wq.shape
    hbm = pl.BlockSpec(memory_space=pltpu.HBM)
    out = jax.ShapeDtypeStruct((n, kb, 2 * hw), BF16)
    return pl.pallas_call(
        weights_kernel,
        out_shape=out,
        in_specs=[pl.BlockSpec(memory_space=pltpu.SMEM), hbm, hbm],
        out_specs=hbm,
        scratch_shapes=[pltpu.VMEM(out.shape, out.dtype), pltpu.SemaphoreType.DMA((3, n))],
        compiler_params=pltpu.CompilerParams(vmem_limit_bytes=60 * 2**20),
        cost_estimate=pl.CostEstimate(flops=10**9, bytes_accessed=2 * 10**7, transcendentals=0),
    )(info, wq, wo)


def kv_weights_kernel(core, kv, ko, kv_all, kvscale):
    n, rows2, kb = kv_all.shape
    rows = rows2 // 2
    side = math.isqrt(n)
    for i in range(n):
        at = pl.ds(pl.multiple_of(block_at(core[0], i, side) * kb, kb), kb)
        kv_all[i, :rows, :] = kv[:, at]
        kv_all[i, rows:, :] = ko[:, at]
    width = kvscale.shape[1]

    def scales(ref):
        s = ref[:, n * kb : n * kb + 128].astype(F32)
        s = (s[:, 0:1] + s[:, 1:2]) + s[:, 2:3]
        return jnp.broadcast_to(s, (rows, width))

    m, o = scales(kv), scales(ko)
    first = core[0] == 0
    k = rows // 2
    for j, (lo, hi) in enumerate(((0, k), (k, 2 * k))):
        a, b = m[lo:hi], o[lo:hi]
        kvscale[2 * j * k : (2 * j + 1) * k, :] = jnp.where(first, a, b)
        kvscale[(2 * j + 1) * k : (2 * j + 2) * k, :] = jnp.where(first, b, a)


def high_kernel(gathered, high):
    n = gathered.shape[0] // 2
    half = gathered.shape[1] - STAT
    squares, largest = 0.0, 0.0
    for i in range(2 * n):
        s = gathered[i, half:, :].astype(F32)
        squares = squares + (s[0:1] + s[1:2])
        largest = jnp.maximum(largest, s[2:3] + s[3:4])
        if i >= n:
            high[(i - n) * half : (i - n + 1) * half, :] = gathered[i, :half, :]
    rows = [p.astype(F32) for v in (squares, largest) for p in split2(v)]
    rows.append(jnp.zeros((STAT - len(rows), rows[0].shape[1]), F32))
    high[n * half :, :] = jnp.concatenate(rows, axis=0).astype(BF16)


def kv_rows(xs, kvs, kv_in, st_in):
    half = kv_in.shape[1]
    total = kv_in[...]
    squares, largest = st_in[0:1, :], st_in[1:2, :]
    for x, w in zip(xs, kvs):
        n = len(w)
        for i in range(n):
            total = total + lax.dot_general(
                w[i],
                x[i * half : (i + 1) * half, :],
                (((1,), (1,)), ((), ())),
                preferred_element_type=F32,
            )
        if x.shape[0] > n * half:
            s = x[n * half :, :].astype(F32)
            squares = squares + (s[0:1] + s[1:2])
            largest = jnp.maximum(largest, s[2:3] + s[3:4])
    return total, squares, largest


def q_sum(xs, ws, q_in):
    half = q_in.shape[0]
    total = q_in[...]
    for x, w in zip(xs, ws):
        for i in range(len(w)):
            total = total + jnp.dot(
                x[i * half : (i + 1) * half, :],
                w[i],
                preferred_element_type=F32,
            )
    return total


def places_of(info, shifts, whole, n):
    side = math.isqrt(whole.shape[0])
    return [lax.rem(info[1] + (side - s % side), side) * side + k * n for s, k in shifts]


def blocks_from(info, shifts, whole, n):
    return [[whole[p + j] for j in range(n)] for p in places_of(info, shifts, whole, n)]


def fetch(info, shifts, w_all, w_buf, sems):
    n = w_buf.shape[1]
    copies = [
        pltpu.make_async_copy(w_all.at[pl.ds(p, n)], w_buf.at[i], sems.at[i])
        for i, p in enumerate(places_of(info, shifts, w_all, n))
    ]
    for c in copies:
        c.start()
    return copies


def arrived(copies, w_buf):
    for c in copies:
        c.wait()
    m, n = w_buf.shape[:2]
    return [[w_buf[i, j] for j in range(n)] for i in range(m)]


def matmul_kernel(shifts, info, *refs):
    m = len(shifts)
    xs, w_all, kv_all = refs[:m], refs[m], refs[m + 1]
    q_out, kv_out, st_out, w_buf, sems = refs[-5:]
    copies = fetch(info, shifts, w_all, w_buf, sems)
    if len(refs) == m + 7:
        q_in, kv_in, st_in = q_out, kv_out, st_out
        for out in (q_out, kv_out, st_out):
            out[...] = jnp.zeros_like(out)
    else:
        q_in, kv_in, st_in = refs[m + 2 : m + 5]
    n = xs[0].shape[0] // xs[0].shape[1]
    kvs = blocks_from(info, shifts, kv_all, n)
    total, squares, largest = kv_rows(xs, kvs, kv_in, st_in)
    kv_out[...] = total
    st_out[0:1, :] = squares
    st_out[1:2, :] = largest
    q_out[...] = q_sum(xs, arrived(copies, w_buf), q_in)


def arrivals_call(kernel, out_shape, info, xs, w_all, rest, flops, aliases=None):
    m = len(xs)
    n = xs[0].shape[0] // xs[0].shape[1]
    vmem = pl.BlockSpec(memory_space=pltpu.VMEM)
    smem = pl.BlockSpec(memory_space=pltpu.SMEM)
    w, scratch = [], []
    if w_all is not None:
        w = [w_all]
        scratch = [pltpu.VMEM((m, n) + w_all.shape[1:], BF16), pltpu.SemaphoreType.DMA((m,))]
    return pl.pallas_call(
        kernel,
        out_shape=out_shape,
        in_specs=[smem] + [vmem] * m + [pl.BlockSpec(memory_space=pltpu.HBM)] * len(w) + [vmem] * len(rest),
        out_specs=tuple(vmem for _ in out_shape),
        scratch_shapes=scratch,
        input_output_aliases=aliases or {},
        compiler_params=pltpu.CompilerParams(vmem_limit_bytes=RING_VMEM),
        cost_estimate=pl.CostEstimate(flops=flops, bytes_accessed=10**6, transcendentals=0),
    )(info, *xs, *w, *rest)


def matmul(half, info, shifts, xs, w_all, kv_all, acc):
    m = len(xs)
    out_shape = (
        jax.ShapeDtypeStruct((half, w_all.shape[2]), F32),
        jax.ShapeDtypeStruct((kv_all.shape[1], half), F32),
        jax.ShapeDtypeStruct((8, half), F32),
    )
    return arrivals_call(
        lambda *refs: matmul_kernel(shifts, *refs),
        out_shape,
        info,
        xs,
        w_all,
        [kv_all, *acc],
        2 * m * xs[0].shape[0] * xs[0].shape[1] * 288,
        {3 + m + i: i for i in range(len(acc))},
    )


def last_kv_kernel(d, shifts, info, *refs):
    m = len(shifts)
    xs, kv_all = refs[:m], refs[m]
    kv_in, st_in, kvscale, kcos, ksin, kvt, st_out = refs[m + 1 :]
    kvs = blocks_from(info, shifts, kv_all, xs[0].shape[0] // xs[0].shape[1])
    t, squares, largest = kv_rows(xs, kvs, kv_in, st_in)
    st_out[0:1, :] = squares
    st_out[1:2, :] = largest
    t = t * (1.0 / jnp.sqrt(squares / d + norm_eps))
    first = info[0] == 0
    mk, mv, ok, ov = t[0:8], t[8:16], t[16:24], t[24:32]
    a = jnp.concatenate([jnp.where(first, mk, ok), jnp.where(first, ok, mk)], axis=0)
    b = jnp.concatenate([jnp.where(first, mv, ov), jnp.where(first, ov, mv)], axis=0)
    a = a * kvscale[:16, :]
    b = b * kvscale[16:, :]
    row = lax.broadcasted_iota(jnp.int32, a.shape, 0)
    swapped = jnp.where(row % 2 == 0, -pltpu.roll(a, a.shape[0] - 1, 0), pltpu.roll(a, 1, 0))
    a = a * kcos[...] + swapped * ksin[...]
    both = jnp.concatenate([a, b], axis=0).astype(BF16)
    for s in range(kvt.shape[0]):
        kvt[s] = both


def last_kv(d, copies, info, shifts, xs, kv_all, kv, st, kvscale, kcos, ksin):
    out_shape = (
        jax.ShapeDtypeStruct((copies,) + kv.shape, BF16),
        jax.ShapeDtypeStruct(st.shape, F32),
    )
    return arrivals_call(
        lambda *refs: last_kv_kernel(d, shifts, *refs),
        out_shape,
        info,
        xs,
        None,
        [kv_all, kv, st, kvscale, kcos, ksin],
        10**9,
    )


def last_q_kernel(d, shifts, info, *refs):
    m = len(shifts)
    xs, w_all = refs[:m], refs[m]
    q_in, st, wscale, cosine, sine, mine, msg, w_buf, sems = refs[m + 1 :]
    q = q_sum(xs, arrived(fetch(info, shifts, w_all, w_buf, sems), w_buf), q_in)
    half = q.shape[0]
    squares, largest = st[0:1, :], st[1:2, :]
    inv = columns_of(1.0 / jnp.sqrt(squares / d + norm_eps), 128)
    mine[...] = turn(q[:, :128] * inv * wscale[...], cosine[...], sine[...]).astype(BF16)
    msg[:half, :] = q[:, 128:] * inv
    msg[half:, :] = jnp.concatenate(
        [
            squares[:, :128],
            squares[:, 128:],
            largest[:, :128],
            largest[:, 128:],
            jnp.zeros((4, 128), F32),
        ],
        axis=0,
    )


def last_q(d, info, shifts, xs, w_all, q, st, wscale, cosine, sine):
    half = q.shape[0]
    out_shape = (
        jax.ShapeDtypeStruct((half, HD), BF16),
        jax.ShapeDtypeStruct((half + 8, HD), F32),
    )
    return arrivals_call(
        lambda *refs: last_q_kernel(d, shifts, *refs),
        out_shape,
        info,
        xs,
        w_all,
        [q, st, wscale, cosine, sine],
        10**9,
    )


def turn(v, cosine, sine):
    lane = lax.broadcasted_iota(jnp.int32, v.shape, 1)
    width = v.shape[1]
    swapped = jnp.where(
        lane % 2 == 0, -pltpu.roll(v, width - 1, 1), pltpu.roll(v, 1, 1)
    )
    return v * cosine + swapped * sine


def columns_of(row, width):
    return jnp.transpose(jnp.broadcast_to(row, (width, row.shape[1])))


def token_kernel(d, core, mine, msg, st, hidden, gain, wscale, cosine, sine, queries, payload, scale):
    half = mine.shape[0]
    c = core[0]
    own = pl.ds(pl.multiple_of(c * half, half), half)
    far = pl.ds(pl.multiple_of((1 - c) * half, half), half)
    queries[own, :] = mine[...]
    queries[far, :] = turn(msg[:half, :] * wscale[...], cosine[...], sine[...]).astype(BF16)
    wide = lambda r: jnp.concatenate(
        [msg[half + r : half + r + 1], msg[half + r + 1 : half + r + 2]], axis=1
    )
    for rows, squares, largest, place in (
        (own, st[0:1, :], st[1:2, :], c),
        (far, wide(0), wide(2), 1 - c),
    ):
        inverse = 1.0 / jnp.sqrt(squares / d + norm_eps)
        row_scale = largest * inverse + tiny_eps
        scale[pl.ds(2 * place, 1), :] = row_scale[:, :128]
        scale[pl.ds(2 * place + 1, 1), :] = row_scale[:, 128:]
        inv = columns_of(inverse, 128)
        rs = columns_of(row_scale, 128)
        normed = hidden[rows, :].astype(F32) * gain[...] * inv
        payload[rows, :] = (normed / rs).astype(BF16)


def head_kernel(order, kvr, keys, values, whole):
    half = kvr.shape[2]
    chips = kvr.shape[0] // 2
    n = KV_COLS_DEV
    for part in range(2):
        at = slice(part * half, (part + 1) * half)
        for i in range(chips):
            rows = kvr[2 * i + part].astype(F32)
            for which in range(2):
                for slot in range(2):
                    to = pl.ds(pl.multiple_of(order[2 * i + slot] * n, n), n)
                    lo = (2 * which + slot) * n
                    whole[which, to, :] = rows[lo : lo + n]
        for which, out in enumerate((keys, values)):
            out[at, :] = jnp.transpose(whole[which]).astype(BF16)


def call(kernel, out_shape, core, *args, flops=0, scratch=()):
    return pl.pallas_call(
        kernel,
        out_shape=out_shape,
        in_specs=[pl.BlockSpec(memory_space=pltpu.SMEM)]
        + [pl.BlockSpec(memory_space=pltpu.VMEM)] * len(args),
        scratch_shapes=list(scratch),
        compiler_params=pltpu.CompilerParams(vmem_limit_bytes=VMEM),
        cost_estimate=pl.CostEstimate(flops=flops or 10**8, bytes_accessed=10**6, transcendentals=0),
    )(core, *args)


def solution(mesh):
    tp = mesh.shape["tp"]
    side = math.isqrt(tp // 2)
    row = 2 * side

    def index(y, x, c):
        return (y % side) * row + (x % side) * 2 + c

    everyone = [(y, x, c) for y in range(side) for x in range(side) for c in range(2)]
    to_partner = [(index(y, x, c), index(y, x, 1 - c)) for y, x, c in everyone]
    heads = tp * KV_COLS_DEV // HD
    columns = side // 2

    def home(j):
        y, x = j // row, (j // 2) % side
        return index(j % heads, x - 1 + (y + x) % columns, y // columns)

    to_row = [(j, home(j)) for j in range(tp)]
    first_groups = [[index(y, x, 0) for x in range(side)] for y in range(side)]
    first_groups += [[index(y, x, 1) for y in range(side)] for x in range(side)]
    rows = [[y * row + i for i in range(row)] for y in range(side)]

    def second(v, s):
        pairs = [
            (index(y, x, c), index(y + s, x, c) if c == 0 else index(y, x + s, c))
            for y, x, c in everyone
        ]
        return lax.ppermute(v, "tp", pairs)

    def swap(v):
        return lax.ppermute(v, "tp", to_partner)

    def body(hidden, norm_gain, prefix, w_query, w_kv, w_scale):
        count, width = hidden.shape
        d = width * tp
        half = count // 2
        me = lax.axis_index("tp")
        core = me % 2
        x = (me // 2) % side
        y = me // row
        core1 = core[None].astype(jnp.int32)
        gain = norm_gain[None, :]

        def piece_at(xs, slot):
            base = y // 2
            h = jnp.where((xs - base + 1) % side < columns, 0, 1)
            source = base + columns * h
            o = (xs - source + 1) % side
            return 2 * ((o - source) % columns + columns * slot) + h

        blk = jax.ShapeDtypeStruct((half + STAT, width), BF16)
        keep, send = call(prep_kernel, (blk, blk), core1, hidden, gain)
        recv = swap(send)
        kvs = w_scale[HD:]
        hi = kvs.astype(BF16)
        mid = kvs - hi.astype(F32)
        mid, lo = mid.astype(BF16), (mid - mid.astype(BF16).astype(F32)).astype(BF16)
        scales = jnp.pad(jnp.stack([hi, mid, lo], axis=1), ((0, 0), (0, 125)))
        kv_mine = lax.ppermute(jnp.concatenate([w_kv, scales], axis=1), "tp", to_row)
        wq_other = swap(w_query)
        slots = call(
            combine_kernel,
            jax.ShapeDtypeStruct((side, half + STAT, 2 * width), BF16),
            core1,
            keep,
            recv,
        )
        gathered = lax.all_to_all(
            slots, "tp", split_axis=0, concat_axis=0, tiled=False, axis_index_groups=first_groups
        )
        positions = (prefix[0] + jnp.arange(count, dtype=jnp.int32)).astype(F32)
        pos_own = lax.dynamic_slice_in_dim(positions, core * half, half)
        pos_far = lax.dynamic_slice_in_dim(positions, (1 - core) * half, half)

        def freq(columns):
            pair = (columns % HD // 2).astype(F32)
            return jnp.power(F32(rope_base), -(2.0 * pair) / HD)

        fq = freq(jnp.arange(HD, dtype=jnp.int32))
        ang_own = pos_own[:, None] * fq[None, :]
        ang_far = pos_far[:, None] * fq[None, :]
        slots_of = jnp.arange(2 * KV_COLS_DEV, dtype=jnp.int32)
        fk = freq(piece_at(x, slots_of // KV_COLS_DEV) * KV_COLS_DEV + slots_of % KV_COLS_DEV)
        seats = jnp.arange(row, dtype=jnp.int32)
        order = piece_at(seats // 2, seats % 2).astype(jnp.int32)
        ang_k = fk[:, None] * pos_own[None, :]
        qscale = w_scale[None, :HD]
        tables = (
            jnp.cos(ang_own),
            jnp.sin(ang_own),
            jnp.cos(ang_far),
            jnp.sin(ang_far),
            jnp.cos(ang_k),
            jnp.sin(ang_k),
        )
        coord = jnp.where(core == 0, y, x)

        info = jnp.stack([core, coord]).astype(jnp.int32)
        w_all = arrange_weights(
            info, w_query.reshape(-1, 2 * width, HD), wq_other.reshape(-1, 2 * width, HD)
        )
        gathered, w_all, tables, info, order, qscale = lax.optimization_barrier(
            (gathered, w_all, tables, info, order, qscale)
        )
        cos_own, sin_own, cos_far, sin_far, cos_k, sin_k = tables

        n = side // 2
        low = gathered[:n, :half].reshape(n * half, -1)
        high = pl.pallas_call(
            high_kernel,
            out_shape=jax.ShapeDtypeStruct((n * half + STAT, gathered.shape[2]), BF16),
            compiler_params=pltpu.CompilerParams(vmem_limit_bytes=VMEM),
            cost_estimate=pl.CostEstimate(flops=10**8, bytes_accessed=10**6, transcendentals=0),
        )(gathered)

        def mm(acc, items):
            shifts = [(s, k) for s, k, _ in items]
            return matmul(half, info, shifts, [v for _, _, v in items], w_all, kv_all, acc)

        up, down = [second(low, 1)], [second(low, -1)]
        up.append(second(high, 1))
        down.append(second(high, -1))
        kv_other = swap(kv_mine)
        kv_all, kvscale = call(
            kv_weights_kernel,
            (
                jax.ShapeDtypeStruct((d // (2 * width), 4 * KV_COLS_DEV, 2 * width), BF16),
                jax.ShapeDtypeStruct((4 * KV_COLS_DEV, half), F32),
            ),
            info,
            kv_mine,
            kv_other,
        )
        acc = mm((), [(0, 0, low), (0, 1, high)])
        last_round = side // 2
        for r in range(1, last_round):
            for k in range(2):
                items = [(r, k, up[k]), (-r, k, down[k])]
                up[k], down[k], acc = lax.optimization_barrier((up[k], down[k], acc))
                if r + 1 < last_round:
                    up[k], down[k] = second(up[k], 1), second(down[k], -1)
                elif k == 0:
                    up[k] = second(up[k], 1)
                else:
                    down[k] = second(down[k], -1)
                acc = mm(acc, items)
        items = [(last_round, 0, up[0]), (-last_round, 1, down[1])]
        xs = [v for _, _, v in items]
        shifts = [(s, k) for s, k, _ in items]
        kvt, st = last_kv(
            d, row, info, shifts, xs, kv_all, acc[1], acc[2], kvscale, cos_k, sin_k
        )
        kvr = lax.all_to_all(
            kvt, "tp", split_axis=0, concat_axis=0, tiled=False, axis_index_groups=rows
        )
        mine, msg = last_q(d, info, shifts, xs, w_all, acc[0], st, qscale, cos_own, sin_own)
        far = swap(msg)
        out = jax.ShapeDtypeStruct((count, HD), BF16)
        queries, payload, scale = call(
            lambda *r: token_kernel(d, *r),
            (out, out, jax.ShapeDtypeStruct((count // HD, HD), F32)),
            info,
            mine,
            far,
            st,
            hidden,
            gain,
            qscale,
            cos_far,
            sin_far,
        )
        keys, values = call(
            head_kernel, (out, out), order, kvr, scratch=[pltpu.VMEM((2, HD, half), F32)]
        )
        return queries, keys, values, payload, scale.reshape(count)

    return jax.shard_map(
        body,
        mesh=mesh,
        in_specs=(P("grp", "tp"), P("tp"), P("grp"), P(None, "tp"), P("tp", None), P("tp")),
        out_specs=(P("grp", "tp"), P("grp", "tp"), P("grp", "tp"), P("grp", "tp"), P("grp")),
        check_vma=False,
    )
```

```python
import math

import jax
import jax.numpy as jnp
from jax import lax
from jax.experimental import pallas as pl
from jax.experimental.pallas import tpu as pltpu
from jax.sharding import PartitionSpec as P


HD = 128
KV_COLS_DEV = 8
norm_eps = 1e-05
tiny_eps = 1e-06
rope_base = 500000.0

VMEM = 24 * 2**20
RING_VMEM = 48 * 2**20

F32 = jnp.float32
BF16 = jnp.bfloat16
STAT = 16


def split2(v):
    hi = v.astype(BF16)
    return hi, (v - hi.astype(F32)).astype(BF16)


def prep_kernel(core, hidden, gain, keep, send):
    half = keep.shape[0] - STAT
    for out, which in ((keep, core[0]), (send, 1 - core[0])):
        h = hidden[pl.ds(pl.multiple_of(which * half, half), half), :].astype(F32)
        weighted = h * gain[...]
        out[:half, :] = weighted.astype(BF16)
        squares = jnp.sum(jnp.transpose(h * h), axis=0, keepdims=True)
        largest = jnp.max(jnp.transpose(jnp.abs(weighted)), axis=0, keepdims=True)
        rows = []
        for v in (squares, largest):
            for part in split2(v):
                part = part.astype(F32)
                rows += [part[:, :128], part[:, 128:]]
        rows.append(jnp.zeros((STAT - len(rows), 128), F32))
        out[half:, :] = jnp.concatenate(rows, axis=0).astype(BF16)


def combine_kernel(core, keep, recv, out):
    half = keep.shape[0] - STAT
    first = core[0] == 0
    mine, other = keep[:half, :], recv[:half, :]
    left = jnp.where(first, mine.astype(F32), other.astype(F32)).astype(BF16)
    right = jnp.where(first, other.astype(F32), mine.astype(F32)).astype(BF16)
    a, b = keep[half:, :].astype(F32), recv[half:, :].astype(F32)

    def wide(s, r):
        return jnp.concatenate([s[r : r + 1], s[r + 1 : r + 2]], axis=1)

    squares = (wide(a, 0) + wide(a, 2)) + (wide(b, 0) + wide(b, 2))
    largest = jnp.maximum(wide(a, 4) + wide(a, 6), wide(b, 4) + wide(b, 6))
    rows = [p.astype(F32) for v in (squares, largest) for p in split2(v)]
    rows.append(jnp.zeros((STAT - len(rows), rows[0].shape[1]), F32))
    stats = jnp.concatenate(rows, axis=0).astype(BF16)
    for s in range(out.shape[0]):
        out[s, :half, :128] = left
        out[s, :half, 128:] = right
        out[s, half:, :] = stats


def block_at(core, i, side):
    return jnp.where(core == 0, i, (i % side) * side + i // side)


def weights_kernel(info, wq, wo, w_all, w_buf, sems):
    n = w_buf.shape[0]
    hw = wq.shape[2]
    side = math.isqrt(n)

    def fetches(i):
        b = block_at(info[0], i, side)
        return (
            pltpu.make_async_copy(wq.at[b], w_buf.at[i, :, pl.ds(0, hw)], sems.at[0, i]),
            pltpu.make_async_copy(wo.at[b], w_buf.at[i, :, pl.ds(hw, hw)], sems.at[1, i]),
        )

    def store(i):
        return pltpu.make_async_copy(w_buf.at[i], w_all.at[i], sems.at[2, i])

    @pl.loop(0, n)
    def _(i):
        for c in fetches(i):
            c.start()

    @pl.loop(0, n)
    def _(i):
        for c in fetches(i):
            c.wait()
        store(i).start()

    @pl.loop(0, n)
    def _(i):
        store(i).wait()


def arrange_weights(info, wq, wo):
    n, kb, hw = wq.shape
    hbm = pl.BlockSpec(memory_space=pltpu.HBM)
    out = jax.ShapeDtypeStruct((n, kb, 2 * hw), BF16)
    return pl.pallas_call(
        weights_kernel,
        out_shape=out,
        in_specs=[pl.BlockSpec(memory_space=pltpu.SMEM), hbm, hbm],
        out_specs=hbm,
        scratch_shapes=[pltpu.VMEM(out.shape, out.dtype), pltpu.SemaphoreType.DMA((3, n))],
        compiler_params=pltpu.CompilerParams(vmem_limit_bytes=60 * 2**20),
        cost_estimate=pl.CostEstimate(flops=10**9, bytes_accessed=2 * 10**7, transcendentals=0),
    )(info, wq, wo)


def kv_weights_kernel(core, kv, ko, kv_all, kvscale):
    n, rows2, kb = kv_all.shape
    rows = rows2 // 2
    side = math.isqrt(n)
    for i in range(n):
        at = pl.ds(pl.multiple_of(block_at(core[0], i, side) * kb, kb), kb)
        kv_all[i, :rows, :] = kv[:, at]
        kv_all[i, rows:, :] = ko[:, at]
    width = kvscale.shape[1]

    def scales(ref):
        s = ref[:, n * kb : n * kb + 128].astype(F32)
        s = (s[:, 0:1] + s[:, 1:2]) + s[:, 2:3]
        return jnp.broadcast_to(s, (rows, width))

    m, o = scales(kv), scales(ko)
    first = core[0] == 0
    k = rows // 2
    for j, (lo, hi) in enumerate(((0, k), (k, 2 * k))):
        a, b = m[lo:hi], o[lo:hi]
        kvscale[2 * j * k : (2 * j + 1) * k, :] = jnp.where(first, a, b)
        kvscale[(2 * j + 1) * k : (2 * j + 2) * k, :] = jnp.where(first, b, a)


def high_kernel(gathered, high):
    n = gathered.shape[0] // 2
    half = gathered.shape[1] - STAT
    squares, largest = 0.0, 0.0
    for i in range(2 * n):
        s = gathered[i, half:, :].astype(F32)
        squares = squares + (s[0:1] + s[1:2])
        largest = jnp.maximum(largest, s[2:3] + s[3:4])
        if i >= n:
            high[(i - n) * half : (i - n + 1) * half, :] = gathered[i, :half, :]
    rows = [p.astype(F32) for v in (squares, largest) for p in split2(v)]
    rows.append(jnp.zeros((STAT - len(rows), rows[0].shape[1]), F32))
    high[n * half :, :] = jnp.concatenate(rows, axis=0).astype(BF16)


def kv_rows(xs, kvs, kv_in, st_in):
    half = kv_in.shape[1]
    total = kv_in[...]
    squares, largest = st_in[0:1, :], st_in[1:2, :]
    for x, w in zip(xs, kvs):
        n = len(w)
        for i in range(n):
            total = total + lax.dot_general(
                w[i],
                x[i * half : (i + 1) * half, :],
                (((1,), (1,)), ((), ())),
                preferred_element_type=F32,
            )
        if x.shape[0] > n * half:
            s = x[n * half :, :].astype(F32)
            squares = squares + (s[0:1] + s[1:2])
            largest = jnp.maximum(largest, s[2:3] + s[3:4])
    return total, squares, largest


def q_sum(xs, ws, q_in):
    half = q_in.shape[0]
    total = q_in[...]
    for x, w in zip(xs, ws):
        for i in range(len(w)):
            total = total + jnp.dot(
                x[i * half : (i + 1) * half, :],
                w[i],
                preferred_element_type=F32,
            )
    return total


def places_of(info, shifts, whole, n):
    side = math.isqrt(whole.shape[0])
    return [lax.rem(info[1] + (side - s % side), side) * side + k * n for s, k in shifts]


def blocks_from(info, shifts, whole, n):
    return [[whole[p + j] for j in range(n)] for p in places_of(info, shifts, whole, n)]


def fetch(info, shifts, w_all, w_buf, sems):
    n = w_buf.shape[1]
    copies = [
        pltpu.make_async_copy(w_all.at[pl.ds(p, n)], w_buf.at[i], sems.at[i])
        for i, p in enumerate(places_of(info, shifts, w_all, n))
    ]
    for c in copies:
        c.start()
    return copies


def ahead_kernel(shifts, info, w_all, w_next, sems):
    for c in fetch(info, shifts, w_all, w_next, sems):
        c.wait()


def first_weights(info, shifts, w_all, n):
    m = len(shifts)
    hbm = pl.BlockSpec(memory_space=pltpu.HBM)
    return pl.pallas_call(
        lambda *refs: ahead_kernel(shifts, *refs),
        out_shape=jax.ShapeDtypeStruct((m, n) + w_all.shape[1:], BF16),
        in_specs=[pl.BlockSpec(memory_space=pltpu.SMEM), hbm],
        out_specs=pl.BlockSpec(memory_space=pltpu.VMEM),
        scratch_shapes=[pltpu.SemaphoreType.DMA((m,))],
        compiler_params=pltpu.CompilerParams(vmem_limit_bytes=RING_VMEM),
        cost_estimate=pl.CostEstimate(flops=10**8, bytes_accessed=10**6, transcendentals=0),
    )(info, w_all)


def matmul_kernel(shifts, next_shifts, info, *refs):
    m = len(shifts)
    xs, w_now, w_all, kv_all = refs[:m], *refs[m : m + 3]
    q_out, kv_out, st_out, w_next, sems = refs[-5:]
    copies = fetch(info, next_shifts, w_all, w_next, sems)
    if len(refs) == m + 8:
        q_in, kv_in, st_in = q_out, kv_out, st_out
        for out in (q_out, kv_out, st_out):
            out[...] = jnp.zeros_like(out)
    else:
        q_in, kv_in, st_in = refs[m + 3 : m + 6]
    n = w_now.shape[1]
    kvs = blocks_from(info, shifts, kv_all, n)
    total, squares, largest = kv_rows(xs, kvs, kv_in, st_in)
    kv_out[...] = total
    st_out[0:1, :] = squares
    st_out[1:2, :] = largest
    q_out[...] = q_sum(xs, [[w_now[i, j] for j in range(n)] for i in range(m)], q_in)
    for c in copies:
        c.wait()


def arrivals_call(kernel, out_shape, info, xs, hbm_args, rest, flops, aliases=None, scratch=()):
    vmem = pl.BlockSpec(memory_space=pltpu.VMEM)
    smem = pl.BlockSpec(memory_space=pltpu.SMEM)
    hbm = pl.BlockSpec(memory_space=pltpu.HBM)
    return pl.pallas_call(
        kernel,
        out_shape=out_shape,
        in_specs=[smem] + [vmem] * len(xs) + [hbm] * len(hbm_args) + [vmem] * len(rest),
        out_specs=tuple(vmem for _ in out_shape),
        scratch_shapes=list(scratch),
        input_output_aliases=aliases or {},
        compiler_params=pltpu.CompilerParams(vmem_limit_bytes=RING_VMEM),
        cost_estimate=pl.CostEstimate(flops=flops, bytes_accessed=10**6, transcendentals=0),
    )(info, *xs, *hbm_args, *rest)


def matmul(half, info, shifts, next_shifts, xs, w_now, w_all, kv_all, acc):
    m = len(xs)
    out_shape = (
        jax.ShapeDtypeStruct((half, w_all.shape[2]), F32),
        jax.ShapeDtypeStruct((kv_all.shape[1], half), F32),
        jax.ShapeDtypeStruct((8, half), F32),
        jax.ShapeDtypeStruct(w_now.shape, w_now.dtype),
    )
    return arrivals_call(
        lambda *refs: matmul_kernel(shifts, next_shifts, *refs),
        out_shape,
        info,
        [*xs, w_now],
        [w_all],
        [kv_all, *acc],
        2 * m * xs[0].shape[0] * xs[0].shape[1] * 288,
        {4 + m + i: i for i in range(len(acc))},
        [pltpu.SemaphoreType.DMA((m,))],
    )


def last_kv_kernel(d, shifts, info, *refs):
    m = len(shifts)
    xs, kv_all = refs[:m], refs[m]
    kv_in, st_in, kvscale, kcos, ksin, kvt, st_out = refs[m + 1 :]
    kvs = blocks_from(info, shifts, kv_all, xs[0].shape[0] // xs[0].shape[1])
    t, squares, largest = kv_rows(xs, kvs, kv_in, st_in)
    st_out[0:1, :] = squares
    st_out[1:2, :] = largest
    t = t * (1.0 / jnp.sqrt(squares / d + norm_eps))
    first = info[0] == 0
    mk, mv, ok, ov = t[0:8], t[8:16], t[16:24], t[24:32]
    a = jnp.concatenate([jnp.where(first, mk, ok), jnp.where(first, ok, mk)], axis=0)
    b = jnp.concatenate([jnp.where(first, mv, ov), jnp.where(first, ov, mv)], axis=0)
    a = a * kvscale[:16, :]
    b = b * kvscale[16:, :]
    row = lax.broadcasted_iota(jnp.int32, a.shape, 0)
    swapped = jnp.where(row % 2 == 0, -pltpu.roll(a, a.shape[0] - 1, 0), pltpu.roll(a, 1, 0))
    a = a * kcos[...] + swapped * ksin[...]
    both = jnp.concatenate([a, b], axis=0).astype(BF16)
    for s in range(kvt.shape[0]):
        kvt[s] = both


def last_kv(d, copies, info, shifts, xs, kv_all, kv, st, kvscale, kcos, ksin):
    out_shape = (
        jax.ShapeDtypeStruct((copies,) + kv.shape, BF16),
        jax.ShapeDtypeStruct(st.shape, F32),
    )
    return arrivals_call(
        lambda *refs: last_kv_kernel(d, shifts, *refs),
        out_shape,
        info,
        xs,
        [],
        [kv_all, kv, st, kvscale, kcos, ksin],
        10**9,
    )


def last_q_kernel(d, shifts, info, *refs):
    m = len(shifts)
    xs, w_now = refs[:m], refs[m]
    q_in, st, wscale, cosine, sine, mine, msg = refs[m + 1 :]
    n = w_now.shape[1]
    q = q_sum(xs, [[w_now[i, j] for j in range(n)] for i in range(m)], q_in)
    half = q.shape[0]
    squares, largest = st[0:1, :], st[1:2, :]
    inv = columns_of(1.0 / jnp.sqrt(squares / d + norm_eps), 128)
    mine[...] = turn(q[:, :128] * inv * wscale[...], cosine[...], sine[...]).astype(BF16)
    msg[:half, :] = q[:, 128:] * inv
    msg[half:, :] = jnp.concatenate(
        [
            squares[:, :128],
            squares[:, 128:],
            largest[:, :128],
            largest[:, 128:],
            jnp.zeros((4, 128), F32),
        ],
        axis=0,
    )


def last_q(d, info, shifts, xs, w_now, q, st, wscale, cosine, sine):
    half = q.shape[0]
    out_shape = (
        jax.ShapeDtypeStruct((half, HD), BF16),
        jax.ShapeDtypeStruct((half + 8, HD), F32),
    )
    return arrivals_call(
        lambda *refs: last_q_kernel(d, shifts, *refs),
        out_shape,
        info,
        [*xs, w_now],
        [],
        [q, st, wscale, cosine, sine],
        10**9,
    )


def turn(v, cosine, sine):
    lane = lax.broadcasted_iota(jnp.int32, v.shape, 1)
    width = v.shape[1]
    swapped = jnp.where(
        lane % 2 == 0, -pltpu.roll(v, width - 1, 1), pltpu.roll(v, 1, 1)
    )
    return v * cosine + swapped * sine


def columns_of(row, width):
    return jnp.transpose(jnp.broadcast_to(row, (width, row.shape[1])))


def token_kernel(d, core, mine, msg, st, hidden, gain, wscale, cosine, sine, queries, payload, scale):
    half = mine.shape[0]
    c = core[0]
    own = pl.ds(pl.multiple_of(c * half, half), half)
    far = pl.ds(pl.multiple_of((1 - c) * half, half), half)
    queries[own, :] = mine[...]
    queries[far, :] = turn(msg[:half, :] * wscale[...], cosine[...], sine[...]).astype(BF16)
    wide = lambda r: jnp.concatenate(
        [msg[half + r : half + r + 1], msg[half + r + 1 : half + r + 2]], axis=1
    )
    for rows, squares, largest, place in (
        (own, st[0:1, :], st[1:2, :], c),
        (far, wide(0), wide(2), 1 - c),
    ):
        inverse = 1.0 / jnp.sqrt(squares / d + norm_eps)
        row_scale = largest * inverse + tiny_eps
        scale[pl.ds(2 * place, 1), :] = row_scale[:, :128]
        scale[pl.ds(2 * place + 1, 1), :] = row_scale[:, 128:]
        inv = columns_of(inverse, 128)
        rs = columns_of(row_scale, 128)
        normed = hidden[rows, :].astype(F32) * gain[...] * inv
        payload[rows, :] = (normed / rs).astype(BF16)


def head_kernel(order, kvr, keys, values, whole):
    half = kvr.shape[2]
    chips = kvr.shape[0] // 2
    n = KV_COLS_DEV
    for part in range(2):
        at = slice(part * half, (part + 1) * half)
        for i in range(chips):
            rows = kvr[2 * i + part].astype(F32)
            for which in range(2):
                for slot in range(2):
                    to = pl.ds(pl.multiple_of(order[2 * i + slot] * n, n), n)
                    lo = (2 * which + slot) * n
                    whole[which, to, :] = rows[lo : lo + n]
        for which, out in enumerate((keys, values)):
            out[at, :] = jnp.transpose(whole[which]).astype(BF16)


def call(kernel, out_shape, core, *args, flops=0, scratch=()):
    return pl.pallas_call(
        kernel,
        out_shape=out_shape,
        in_specs=[pl.BlockSpec(memory_space=pltpu.SMEM)]
        + [pl.BlockSpec(memory_space=pltpu.VMEM)] * len(args),
        scratch_shapes=list(scratch),
        compiler_params=pltpu.CompilerParams(vmem_limit_bytes=VMEM),
        cost_estimate=pl.CostEstimate(flops=flops or 10**8, bytes_accessed=10**6, transcendentals=0),
    )(core, *args)


def solution(mesh):
    tp = mesh.shape["tp"]
    side = math.isqrt(tp // 2)
    row = 2 * side

    def index(y, x, c):
        return (y % side) * row + (x % side) * 2 + c

    everyone = [(y, x, c) for y in range(side) for x in range(side) for c in range(2)]
    to_partner = [(index(y, x, c), index(y, x, 1 - c)) for y, x, c in everyone]
    heads = tp * KV_COLS_DEV // HD
    columns = side // 2

    def home(j):
        y, x = j // row, (j // 2) % side
        return index(j % heads, x - 1 + (y + x) % columns, y // columns)

    to_row = [(j, home(j)) for j in range(tp)]
    first_groups = [[index(y, x, 0) for x in range(side)] for y in range(side)]
    first_groups += [[index(y, x, 1) for y in range(side)] for x in range(side)]
    rows = [[y * row + i for i in range(row)] for y in range(side)]

    def second(v, s):
        pairs = [
            (index(y, x, c), index(y + s, x, c) if c == 0 else index(y, x + s, c))
            for y, x, c in everyone
        ]
        return lax.ppermute(v, "tp", pairs)

    def swap(v):
        return lax.ppermute(v, "tp", to_partner)

    def body(hidden, norm_gain, prefix, w_query, w_kv, w_scale):
        count, width = hidden.shape
        d = width * tp
        half = count // 2
        me = lax.axis_index("tp")
        core = me % 2
        x = (me // 2) % side
        y = me // row
        core1 = core[None].astype(jnp.int32)
        gain = norm_gain[None, :]

        def piece_at(xs, slot):
            base = y // 2
            h = jnp.where((xs - base + 1) % side < columns, 0, 1)
            source = base + columns * h
            o = (xs - source + 1) % side
            return 2 * ((o - source) % columns + columns * slot) + h

        blk = jax.ShapeDtypeStruct((half + STAT, width), BF16)
        keep, send = call(prep_kernel, (blk, blk), core1, hidden, gain)
        recv = swap(send)
        kvs = w_scale[HD:]
        hi = kvs.astype(BF16)
        mid = kvs - hi.astype(F32)
        mid, lo = mid.astype(BF16), (mid - mid.astype(BF16).astype(F32)).astype(BF16)
        scales = jnp.pad(jnp.stack([hi, mid, lo], axis=1), ((0, 0), (0, 125)))
        kv_mine = lax.ppermute(jnp.concatenate([w_kv, scales], axis=1), "tp", to_row)
        wq_other = swap(w_query)
        slots = call(
            combine_kernel,
            jax.ShapeDtypeStruct((side, half + STAT, 2 * width), BF16),
            core1,
            keep,
            recv,
        )
        gathered = lax.all_to_all(
            slots, "tp", split_axis=0, concat_axis=0, tiled=False, axis_index_groups=first_groups
        )
        positions = (prefix[0] + jnp.arange(count, dtype=jnp.int32)).astype(F32)
        pos_own = lax.dynamic_slice_in_dim(positions, core * half, half)
        pos_far = lax.dynamic_slice_in_dim(positions, (1 - core) * half, half)

        def freq(columns):
            pair = (columns % HD // 2).astype(F32)
            return jnp.power(F32(rope_base), -(2.0 * pair) / HD)

        fq = freq(jnp.arange(HD, dtype=jnp.int32))
        ang_own = pos_own[:, None] * fq[None, :]
        ang_far = pos_far[:, None] * fq[None, :]
        slots_of = jnp.arange(2 * KV_COLS_DEV, dtype=jnp.int32)
        fk = freq(piece_at(x, slots_of // KV_COLS_DEV) * KV_COLS_DEV + slots_of % KV_COLS_DEV)
        seats = jnp.arange(row, dtype=jnp.int32)
        order = piece_at(seats // 2, seats % 2).astype(jnp.int32)
        ang_k = fk[:, None] * pos_own[None, :]
        qscale = w_scale[None, :HD]
        tables = (
            jnp.cos(ang_own),
            jnp.sin(ang_own),
            jnp.cos(ang_far),
            jnp.sin(ang_far),
            jnp.cos(ang_k),
            jnp.sin(ang_k),
        )
        coord = jnp.where(core == 0, y, x)

        info = jnp.stack([core, coord]).astype(jnp.int32)
        w_all = arrange_weights(
            info, w_query.reshape(-1, 2 * width, HD), wq_other.reshape(-1, 2 * width, HD)
        )
        n = side // 2
        w_now = first_weights(info, [(0, 0), (0, 1)], w_all, n)
        gathered, w_all, w_now, tables, info, order, qscale = lax.optimization_barrier(
            (gathered, w_all, w_now, tables, info, order, qscale)
        )
        cos_own, sin_own, cos_far, sin_far, cos_k, sin_k = tables

        n = side // 2
        low = gathered[:n, :half].reshape(n * half, -1)
        high = pl.pallas_call(
            high_kernel,
            out_shape=jax.ShapeDtypeStruct((n * half + STAT, gathered.shape[2]), BF16),
            compiler_params=pltpu.CompilerParams(vmem_limit_bytes=VMEM),
            cost_estimate=pl.CostEstimate(flops=10**8, bytes_accessed=10**6, transcendentals=0),
        )(gathered)

        last_round = side // 2
        plan = [[(0, 0), (0, 1)]]
        plan += [[(r, k), (-r, k)] for r in range(1, last_round) for k in range(2)]
        plan += [[(last_round, 0), (-last_round, 1)]]

        def mm(at, acc, w_now, xs):
            *acc, w_next = matmul(
                half, info, plan[at], plan[at + 1], xs, w_now, w_all, kv_all, acc
            )
            return acc, w_next

        up, down = [second(low, 1)], [second(low, -1)]
        up.append(second(high, 1))
        down.append(second(high, -1))
        kv_other = swap(kv_mine)
        kv_all, kvscale = call(
            kv_weights_kernel,
            (
                jax.ShapeDtypeStruct((d // (2 * width), 4 * KV_COLS_DEV, 2 * width), BF16),
                jax.ShapeDtypeStruct((4 * KV_COLS_DEV, half), F32),
            ),
            info,
            kv_mine,
            kv_other,
        )
        acc, w_now = mm(0, (), w_now, [low, high])
        at = 1
        for r in range(1, last_round):
            for k in range(2):
                xs = [up[k], down[k]]
                up[k], down[k], acc = lax.optimization_barrier((up[k], down[k], acc))
                if r + 1 < last_round:
                    up[k], down[k] = second(up[k], 1), second(down[k], -1)
                elif k == 0:
                    up[k] = second(up[k], 1)
                else:
                    down[k] = second(down[k], -1)
                acc, w_now = mm(at, acc, w_now, xs)
                at += 1
        xs = [up[0], down[1]]
        shifts = plan[-1]
        kvt, st = last_kv(
            d, row, info, shifts, xs, kv_all, acc[1], acc[2], kvscale, cos_k, sin_k
        )
        kvr = lax.all_to_all(
            kvt, "tp", split_axis=0, concat_axis=0, tiled=False, axis_index_groups=rows
        )
        mine, msg = last_q(d, info, shifts, xs, w_now, acc[0], st, qscale, cos_own, sin_own)
        far = swap(msg)
        out = jax.ShapeDtypeStruct((count, HD), BF16)
        queries, payload, scale = call(
            lambda *r: token_kernel(d, *r),
            (out, out, jax.ShapeDtypeStruct((count // HD, HD), F32)),
            info,
            mine,
            far,
            st,
            hidden,
            gain,
            qscale,
            cos_far,
            sin_far,
        )
        keys, values = call(
            head_kernel, (out, out), order, kvr, scratch=[pltpu.VMEM((2, HD, half), F32)]
        )
        return queries, keys, values, payload, scale.reshape(count)

    return jax.shard_map(
        body,
        mesh=mesh,
        in_specs=(P("grp", "tp"), P("tp"), P("grp"), P(None, "tp"), P("tp", None), P("tp")),
        out_specs=(P("grp", "tp"), P("grp", "tp"), P("grp", "tp"), P("grp", "tp"), P("grp")),
        check_vma=False,
    )
```

```python
import math

import jax
import jax.numpy as jnp
from jax import lax
from jax.experimental import pallas as pl
from jax.experimental.pallas import tpu as pltpu
from jax.sharding import PartitionSpec as P


HD = 128
KV_COLS_DEV = 8
norm_eps = 1e-05
tiny_eps = 1e-06
rope_base = 500000.0

VMEM = 24 * 2**20
RING_VMEM = 48 * 2**20

F32 = jnp.float32
BF16 = jnp.bfloat16
STAT = 16


def split2(v):
    hi = v.astype(BF16)
    return hi, (v - hi.astype(F32)).astype(BF16)


def prep_kernel(core, hidden, gain, keep, send):
    half = keep.shape[0] - STAT
    for out, which in ((keep, core[0]), (send, 1 - core[0])):
        h = hidden[pl.ds(pl.multiple_of(which * half, half), half), :].astype(F32)
        weighted = h * gain[...]
        out[:half, :] = weighted.astype(BF16)
        squares = jnp.sum(jnp.transpose(h * h), axis=0, keepdims=True)
        largest = jnp.max(jnp.transpose(jnp.abs(weighted)), axis=0, keepdims=True)
        rows = []
        for v in (squares, largest):
            for part in split2(v):
                part = part.astype(F32)
                rows += [part[:, :128], part[:, 128:]]
        rows.append(jnp.zeros((STAT - len(rows), 128), F32))
        out[half:, :] = jnp.concatenate(rows, axis=0).astype(BF16)


def combine_kernel(core, keep, recv, out):
    half = keep.shape[0] - STAT
    first = core[0] == 0
    mine, other = keep[:half, :], recv[:half, :]
    left = jnp.where(first, mine.astype(F32), other.astype(F32)).astype(BF16)
    right = jnp.where(first, other.astype(F32), mine.astype(F32)).astype(BF16)
    a, b = keep[half:, :].astype(F32), recv[half:, :].astype(F32)

    def wide(s, r):
        return jnp.concatenate([s[r : r + 1], s[r + 1 : r + 2]], axis=1)

    squares = (wide(a, 0) + wide(a, 2)) + (wide(b, 0) + wide(b, 2))
    largest = jnp.maximum(wide(a, 4) + wide(a, 6), wide(b, 4) + wide(b, 6))
    rows = [p.astype(F32) for v in (squares, largest) for p in split2(v)]
    rows.append(jnp.zeros((STAT - len(rows), rows[0].shape[1]), F32))
    stats = jnp.concatenate(rows, axis=0).astype(BF16)
    for s in range(out.shape[0]):
        out[s, :half, :128] = left
        out[s, :half, 128:] = right
        out[s, half:, :] = stats


def block_at(core, i, side):
    return jnp.where(core == 0, i, (i % side) * side + i // side)


def weights_kernel(info, wq, wo, w_all, w_buf, sems):
    n = w_buf.shape[0]
    hw = wq.shape[2]
    side = math.isqrt(n)

    def fetches(i):
        b = block_at(info[0], i, side)
        return (
            pltpu.make_async_copy(wq.at[b], w_buf.at[i, :, pl.ds(0, hw)], sems.at[0, i]),
            pltpu.make_async_copy(wo.at[b], w_buf.at[i, :, pl.ds(hw, hw)], sems.at[1, i]),
        )

    def store(i):
        return pltpu.make_async_copy(w_buf.at[i], w_all.at[i], sems.at[2, i])

    @pl.loop(0, n)
    def _(i):
        for c in fetches(i):
            c.start()

    @pl.loop(0, n)
    def _(i):
        for c in fetches(i):
            c.wait()
        store(i).start()

    @pl.loop(0, n)
    def _(i):
        store(i).wait()


def arrange_weights(info, wq, wo):
    n, kb, hw = wq.shape
    hbm = pl.BlockSpec(memory_space=pltpu.HBM)
    out = jax.ShapeDtypeStruct((n, kb, 2 * hw), BF16)
    return pl.pallas_call(
        weights_kernel,
        out_shape=out,
        in_specs=[pl.BlockSpec(memory_space=pltpu.SMEM), hbm, hbm],
        out_specs=hbm,
        scratch_shapes=[pltpu.VMEM(out.shape, out.dtype), pltpu.SemaphoreType.DMA((3, n))],
        compiler_params=pltpu.CompilerParams(vmem_limit_bytes=60 * 2**20),
        cost_estimate=pl.CostEstimate(flops=10**9, bytes_accessed=2 * 10**7, transcendentals=0),
    )(info, wq, wo)


def kv_weights_kernel(core, kv, ko, kv_all):
    n, rows2, kb = kv_all.shape
    rows = rows2 // 2
    side = math.isqrt(n)
    for i in range(n):
        at = pl.ds(pl.multiple_of(block_at(core[0], i, side) * kb, kb), kb)
        kv_all[i, :rows, :] = kv[:, at]
        kv_all[i, rows:, :] = ko[:, at]


def kv_scale_kernel(core, kvs, kos, kvscale):
    rows = kvs.shape[1]
    width = kvscale.shape[1]

    def scales(ref):
        shape = (rows, rows)
        diagonal = lax.broadcasted_iota(jnp.int32, shape, 0) == lax.broadcasted_iota(
            jnp.int32, shape, 1
        )
        column = jnp.sum(
            jnp.where(diagonal, jnp.broadcast_to(ref[...], shape), 0.0), axis=1, keepdims=True
        )
        return jnp.broadcast_to(column, (rows, width))

    m, o = scales(kvs), scales(kos)
    first = core[0] == 0
    k = rows // 2
    for j, (lo, hi) in enumerate(((0, k), (k, 2 * k))):
        a, b = m[lo:hi], o[lo:hi]
        kvscale[2 * j * k : (2 * j + 1) * k, :] = jnp.where(first, a, b)
        kvscale[(2 * j + 1) * k : (2 * j + 2) * k, :] = jnp.where(first, b, a)


def high_kernel(gathered, high):
    n = gathered.shape[0] // 2
    half = gathered.shape[1] - STAT
    squares, largest = 0.0, 0.0
    for i in range(2 * n):
        s = gathered[i, half:, :].astype(F32)
        squares = squares + (s[0:1] + s[1:2])
        largest = jnp.maximum(largest, s[2:3] + s[3:4])
        if i >= n:
            high[(i - n) * half : (i - n + 1) * half, :] = gathered[i, :half, :]
    rows = [p.astype(F32) for v in (squares, largest) for p in split2(v)]
    rows.append(jnp.zeros((STAT - len(rows), rows[0].shape[1]), F32))
    high[n * half :, :] = jnp.concatenate(rows, axis=0).astype(BF16)


def kv_rows(xs, kvs, kv_in, st_in):
    half = kv_in.shape[1]
    total = kv_in[...]
    squares, largest = st_in[0:1, :], st_in[1:2, :]
    for x, w in zip(xs, kvs):
        n = len(w)
        for i in range(n):
            total = total + lax.dot_general(
                w[i],
                x[i * half : (i + 1) * half, :],
                (((1,), (1,)), ((), ())),
                preferred_element_type=F32,
            )
        if x.shape[0] > n * half:
            s = x[n * half :, :].astype(F32)
            squares = squares + (s[0:1] + s[1:2])
            largest = jnp.maximum(largest, s[2:3] + s[3:4])
    return total, squares, largest


def q_sum(xs, ws, q_in):
    half = q_in.shape[0]
    total = q_in[...]
    for x, w in zip(xs, ws):
        for i in range(len(w)):
            total = total + jnp.dot(
                x[i * half : (i + 1) * half, :],
                w[i],
                preferred_element_type=F32,
            )
    return total


def places_of(info, shifts, whole, n):
    side = math.isqrt(whole.shape[0])
    return [lax.rem(info[1] + (side - s % side), side) * side + k * n for s, k in shifts]


def blocks_from(info, shifts, whole, n):
    return [[whole[p + j] for j in range(n)] for p in places_of(info, shifts, whole, n)]


def fetch(info, shifts, w_all, w_buf, sems):
    n = w_buf.shape[1]
    copies = [
        pltpu.make_async_copy(w_all.at[pl.ds(p, n)], w_buf.at[i], sems.at[i])
        for i, p in enumerate(places_of(info, shifts, w_all, n))
    ]
    for c in copies:
        c.start()
    return copies


def ahead_kernel(shifts, info, w_all, w_next, sems):
    for c in fetch(info, shifts, w_all, w_next, sems):
        c.wait()


def first_weights(info, shifts, w_all, n):
    m = len(shifts)
    hbm = pl.BlockSpec(memory_space=pltpu.HBM)
    return pl.pallas_call(
        lambda *refs: ahead_kernel(shifts, *refs),
        out_shape=jax.ShapeDtypeStruct((m, n) + w_all.shape[1:], BF16),
        in_specs=[pl.BlockSpec(memory_space=pltpu.SMEM), hbm],
        out_specs=pl.BlockSpec(memory_space=pltpu.VMEM),
        scratch_shapes=[pltpu.SemaphoreType.DMA((m,))],
        compiler_params=pltpu.CompilerParams(vmem_limit_bytes=RING_VMEM),
        cost_estimate=pl.CostEstimate(flops=10**8, bytes_accessed=10**6, transcendentals=0),
    )(info, w_all)


def matmul_kernel(shifts, next_shifts, info, *refs):
    m = len(shifts)
    xs, w_now, w_all, kv_all = refs[:m], *refs[m : m + 3]
    q_out, kv_out, st_out, w_next, sems = refs[-5:]
    copies = fetch(info, next_shifts, w_all, w_next, sems)
    if len(refs) == m + 8:
        q_in, kv_in, st_in = q_out, kv_out, st_out
        for out in (q_out, kv_out, st_out):
            out[...] = jnp.zeros_like(out)
    else:
        q_in, kv_in, st_in = refs[m + 3 : m + 6]
    n = w_now.shape[1]
    kvs = blocks_from(info, shifts, kv_all, n)
    total, squares, largest = kv_rows(xs, kvs, kv_in, st_in)
    kv_out[...] = total
    st_out[0:1, :] = squares
    st_out[1:2, :] = largest
    q_out[...] = q_sum(xs, [[w_now[i, j] for j in range(n)] for i in range(m)], q_in)
    for c in copies:
        c.wait()


def arrivals_call(kernel, out_shape, info, xs, hbm_args, rest, flops, aliases=None, scratch=()):
    vmem = pl.BlockSpec(memory_space=pltpu.VMEM)
    smem = pl.BlockSpec(memory_space=pltpu.SMEM)
    hbm = pl.BlockSpec(memory_space=pltpu.HBM)
    return pl.pallas_call(
        kernel,
        out_shape=out_shape,
        in_specs=[smem] + [vmem] * len(xs) + [hbm] * len(hbm_args) + [vmem] * len(rest),
        out_specs=tuple(vmem for _ in out_shape),
        scratch_shapes=list(scratch),
        input_output_aliases=aliases or {},
        compiler_params=pltpu.CompilerParams(vmem_limit_bytes=RING_VMEM),
        cost_estimate=pl.CostEstimate(flops=flops, bytes_accessed=10**6, transcendentals=0),
    )(info, *xs, *hbm_args, *rest)


def matmul(half, info, shifts, next_shifts, xs, w_now, w_all, kv_all, acc):
    m = len(xs)
    out_shape = (
        jax.ShapeDtypeStruct((half, w_all.shape[2]), F32),
        jax.ShapeDtypeStruct((kv_all.shape[1], half), F32),
        jax.ShapeDtypeStruct((8, half), F32),
        jax.ShapeDtypeStruct(w_now.shape, w_now.dtype),
    )
    return arrivals_call(
        lambda *refs: matmul_kernel(shifts, next_shifts, *refs),
        out_shape,
        info,
        [*xs, w_now],
        [w_all],
        [kv_all, *acc],
        2 * m * xs[0].shape[0] * xs[0].shape[1] * 288,
        {4 + m + i: i for i in range(len(acc))},
        [pltpu.SemaphoreType.DMA((m,))],
    )


def last_kv_kernel(d, shifts, info, *refs):
    m = len(shifts)
    xs, kv_all = refs[:m], refs[m]
    kv_in, st_in, kvscale, kcos, ksin, kvt, st_out = refs[m + 1 :]
    kvs = blocks_from(info, shifts, kv_all, xs[0].shape[0] // xs[0].shape[1])
    t, squares, largest = kv_rows(xs, kvs, kv_in, st_in)
    st_out[0:1, :] = squares
    st_out[1:2, :] = largest
    t = t * (1.0 / jnp.sqrt(squares / d + norm_eps))
    first = info[0] == 0
    mk, mv, ok, ov = t[0:8], t[8:16], t[16:24], t[24:32]
    a = jnp.concatenate([jnp.where(first, mk, ok), jnp.where(first, ok, mk)], axis=0)
    b = jnp.concatenate([jnp.where(first, mv, ov), jnp.where(first, ov, mv)], axis=0)
    a = a * kvscale[:16, :]
    b = b * kvscale[16:, :]
    row = lax.broadcasted_iota(jnp.int32, a.shape, 0)
    swapped = jnp.where(row % 2 == 0, -pltpu.roll(a, a.shape[0] - 1, 0), pltpu.roll(a, 1, 0))
    a = a * kcos[...] + swapped * ksin[...]
    both = jnp.concatenate([a, b], axis=0).astype(BF16)
    for s in range(kvt.shape[0]):
        kvt[s] = both


def last_kv(d, copies, info, shifts, xs, kv_all, kv, st, kvscale, kcos, ksin):
    out_shape = (
        jax.ShapeDtypeStruct((copies,) + kv.shape, BF16),
        jax.ShapeDtypeStruct(st.shape, F32),
    )
    return arrivals_call(
        lambda *refs: last_kv_kernel(d, shifts, *refs),
        out_shape,
        info,
        xs,
        [],
        [kv_all, kv, st, kvscale, kcos, ksin],
        10**9,
    )


def last_q_kernel(d, shifts, info, *refs):
    m = len(shifts)
    xs, w_now = refs[:m], refs[m]
    q_in, st, wscale, cosine, sine, mine, msg = refs[m + 1 :]
    n = w_now.shape[1]
    q = q_sum(xs, [[w_now[i, j] for j in range(n)] for i in range(m)], q_in)
    half = q.shape[0]
    squares, largest = st[0:1, :], st[1:2, :]
    inv = columns_of(1.0 / jnp.sqrt(squares / d + norm_eps), 128)
    mine[...] = turn(q[:, :128] * inv * wscale[...], cosine[...], sine[...]).astype(BF16)
    msg[:half, :] = q[:, 128:] * inv
    msg[half:, :] = jnp.concatenate(
        [
            squares[:, :128],
            squares[:, 128:],
            largest[:, :128],
            largest[:, 128:],
            jnp.zeros((4, 128), F32),
        ],
        axis=0,
    )


def last_q(d, info, shifts, xs, w_now, q, st, wscale, cosine, sine):
    half = q.shape[0]
    out_shape = (
        jax.ShapeDtypeStruct((half, HD), BF16),
        jax.ShapeDtypeStruct((half + 8, HD), F32),
    )
    return arrivals_call(
        lambda *refs: last_q_kernel(d, shifts, *refs),
        out_shape,
        info,
        [*xs, w_now],
        [],
        [q, st, wscale, cosine, sine],
        10**9,
    )


def turn(v, cosine, sine):
    lane = lax.broadcasted_iota(jnp.int32, v.shape, 1)
    width = v.shape[1]
    swapped = jnp.where(
        lane % 2 == 0, -pltpu.roll(v, width - 1, 1), pltpu.roll(v, 1, 1)
    )
    return v * cosine + swapped * sine


def columns_of(row, width):
    return jnp.transpose(jnp.broadcast_to(row, (width, row.shape[1])))


def token_kernel(d, core, mine, msg, st, hidden, gain, wscale, cosine, sine, queries, payload, scale):
    half = mine.shape[0]
    c = core[0]
    own = pl.ds(pl.multiple_of(c * half, half), half)
    far = pl.ds(pl.multiple_of((1 - c) * half, half), half)
    queries[own, :] = mine[...]
    queries[far, :] = turn(msg[:half, :] * wscale[...], cosine[...], sine[...]).astype(BF16)
    wide = lambda r: jnp.concatenate(
        [msg[half + r : half + r + 1], msg[half + r + 1 : half + r + 2]], axis=1
    )
    for rows, squares, largest, place in (
        (own, st[0:1, :], st[1:2, :], c),
        (far, wide(0), wide(2), 1 - c),
    ):
        inverse = 1.0 / jnp.sqrt(squares / d + norm_eps)
        row_scale = largest * inverse + tiny_eps
        scale[pl.ds(2 * place, 1), :] = row_scale[:, :128]
        scale[pl.ds(2 * place + 1, 1), :] = row_scale[:, 128:]
        inv = columns_of(inverse, 128)
        rs = columns_of(row_scale, 128)
        normed = hidden[rows, :].astype(F32) * gain[...] * inv
        payload[rows, :] = (normed / rs).astype(BF16)


def head_kernel(order, kvr, keys, values, whole):
    half = kvr.shape[2]
    chips = kvr.shape[0] // 2
    n = KV_COLS_DEV
    for part in range(2):
        at = slice(part * half, (part + 1) * half)
        for i in range(chips):
            rows = kvr[2 * i + part].astype(F32)
            for which in range(2):
                for slot in range(2):
                    to = pl.ds(pl.multiple_of(order[2 * i + slot] * n, n), n)
                    lo = (2 * which + slot) * n
                    whole[which, to, :] = rows[lo : lo + n]
        for which, out in enumerate((keys, values)):
            out[at, :] = jnp.transpose(whole[which]).astype(BF16)


def call(kernel, out_shape, core, *args, flops=0, scratch=()):
    return pl.pallas_call(
        kernel,
        out_shape=out_shape,
        in_specs=[pl.BlockSpec(memory_space=pltpu.SMEM)]
        + [pl.BlockSpec(memory_space=pltpu.VMEM)] * len(args),
        scratch_shapes=list(scratch),
        compiler_params=pltpu.CompilerParams(vmem_limit_bytes=VMEM),
        cost_estimate=pl.CostEstimate(flops=flops or 10**8, bytes_accessed=10**6, transcendentals=0),
    )(core, *args)


def solution(mesh):
    tp = mesh.shape["tp"]
    side = math.isqrt(tp // 2)
    row = 2 * side

    def index(y, x, c):
        return (y % side) * row + (x % side) * 2 + c

    everyone = [(y, x, c) for y in range(side) for x in range(side) for c in range(2)]
    to_partner = [(index(y, x, c), index(y, x, 1 - c)) for y, x, c in everyone]
    heads = tp * KV_COLS_DEV // HD
    columns = side // 2

    def home(j):
        y, x = j // row, (j // 2) % side
        return index(j % heads, x - 1 + (y + x) % columns, y // columns)

    to_row = [(j, home(j)) for j in range(tp)]
    first_groups = [[index(y, x, 0) for x in range(side)] for y in range(side)]
    first_groups += [[index(y, x, 1) for y in range(side)] for x in range(side)]
    rows = [[y * row + i for i in range(row)] for y in range(side)]

    def second(v, s):
        pairs = [
            (index(y, x, c), index(y + s, x, c) if c == 0 else index(y, x + s, c))
            for y, x, c in everyone
        ]
        return lax.ppermute(v, "tp", pairs)

    def swap(v):
        return lax.ppermute(v, "tp", to_partner)

    def body(hidden, norm_gain, prefix, w_query, w_kv, w_scale):
        count, width = hidden.shape
        d = width * tp
        half = count // 2
        me = lax.axis_index("tp")
        core = me % 2
        x = (me // 2) % side
        y = me // row
        core1 = core[None].astype(jnp.int32)
        gain = norm_gain[None, :]

        def piece_at(xs, slot):
            base = y // 2
            h = jnp.where((xs - base + 1) % side < columns, 0, 1)
            source = base + columns * h
            o = (xs - source + 1) % side
            return 2 * ((o - source) % columns + columns * slot) + h

        blk = jax.ShapeDtypeStruct((half + STAT, width), BF16)
        keep, send = call(prep_kernel, (blk, blk), core1, hidden, gain)
        recv = swap(send)
        kv_mine = lax.ppermute(w_kv, "tp", to_row)
        kvs_mine = lax.ppermute(w_scale[None, HD:], "tp", to_row)
        wq_other = swap(w_query)
        slots = call(
            combine_kernel,
            jax.ShapeDtypeStruct((side, half + STAT, 2 * width), BF16),
            core1,
            keep,
            recv,
        )
        gathered = lax.all_to_all(
            slots, "tp", split_axis=0, concat_axis=0, tiled=False, axis_index_groups=first_groups
        )
        positions = (prefix[0] + jnp.arange(count, dtype=jnp.int32)).astype(F32)
        pos_own = lax.dynamic_slice_in_dim(positions, core * half, half)
        pos_far = lax.dynamic_slice_in_dim(positions, (1 - core) * half, half)

        def freq(columns):
            pair = (columns % HD // 2).astype(F32)
            return jnp.power(F32(rope_base), -(2.0 * pair) / HD)

        fq = freq(jnp.arange(HD, dtype=jnp.int32))
        ang_own = pos_own[:, None] * fq[None, :]
        ang_far = pos_far[:, None] * fq[None, :]
        slots_of = jnp.arange(2 * KV_COLS_DEV, dtype=jnp.int32)
        fk = freq(piece_at(x, slots_of // KV_COLS_DEV) * KV_COLS_DEV + slots_of % KV_COLS_DEV)
        seats = jnp.arange(row, dtype=jnp.int32)
        order = piece_at(seats // 2, seats % 2).astype(jnp.int32)
        ang_k = fk[:, None] * pos_own[None, :]
        qscale = w_scale[None, :HD]
        tables = (
            jnp.cos(ang_own),
            jnp.sin(ang_own),
            jnp.cos(ang_far),
            jnp.sin(ang_far),
            jnp.cos(ang_k),
            jnp.sin(ang_k),
        )
        coord = jnp.where(core == 0, y, x)

        info = jnp.stack([core, coord]).astype(jnp.int32)
        w_all = arrange_weights(
            info, w_query.reshape(-1, 2 * width, HD), wq_other.reshape(-1, 2 * width, HD)
        )
        n = side // 2
        w_now = first_weights(info, [(0, 0), (0, 1)], w_all, n)
        gathered, w_all, w_now, tables, info, order, qscale = lax.optimization_barrier(
            (gathered, w_all, w_now, tables, info, order, qscale)
        )
        cos_own, sin_own, cos_far, sin_far, cos_k, sin_k = tables

        n = side // 2
        low = gathered[:n, :half].reshape(n * half, -1)
        high = pl.pallas_call(
            high_kernel,
            out_shape=jax.ShapeDtypeStruct((n * half + STAT, gathered.shape[2]), BF16),
            compiler_params=pltpu.CompilerParams(vmem_limit_bytes=VMEM),
            cost_estimate=pl.CostEstimate(flops=10**8, bytes_accessed=10**6, transcendentals=0),
        )(gathered)

        last_round = side // 2
        plan = [[(0, 0), (0, 1)]]
        plan += [[(r, k), (-r, k)] for r in range(1, last_round) for k in range(2)]
        plan += [[(last_round, 0), (-last_round, 1)]]

        def mm(at, acc, w_now, xs):
            *acc, w_next = matmul(
                half, info, plan[at], plan[at + 1], xs, w_now, w_all, kv_all, acc
            )
            return acc, w_next

        up, down = [second(low, 1)], [second(low, -1)]
        up.append(second(high, 1))
        down.append(second(high, -1))
        kv_other = swap(kv_mine)
        kv_all = call(
            kv_weights_kernel,
            jax.ShapeDtypeStruct((d // (2 * width), 4 * KV_COLS_DEV, 2 * width), BF16),
            info,
            kv_mine,
            kv_other,
        )
        acc, w_now = mm(0, (), w_now, [low, high])
        at = 1
        for r in range(1, last_round):
            for k in range(2):
                xs = [up[k], down[k]]
                if at > 1:
                    up[k], down[k], acc = lax.optimization_barrier((up[k], down[k], acc))
                if r + 1 < last_round:
                    up[k], down[k] = second(up[k], 1), second(down[k], -1)
                elif k == 0:
                    up[k] = second(up[k], 1)
                else:
                    down[k] = second(down[k], -1)
                acc, w_now = mm(at, acc, w_now, xs)
                at += 1
        xs = [up[0], down[1]]
        shifts = plan[-1]
        kvs_other = swap(kvs_mine)
        kvscale = call(
            kv_scale_kernel,
            jax.ShapeDtypeStruct((4 * KV_COLS_DEV, half), F32),
            info,
            kvs_mine,
            kvs_other,
        )
        kvt, st = last_kv(
            d, row, info, shifts, xs, kv_all, acc[1], acc[2], kvscale, cos_k, sin_k
        )
        kvr = lax.all_to_all(
            kvt, "tp", split_axis=0, concat_axis=0, tiled=False, axis_index_groups=rows
        )
        mine, msg = last_q(d, info, shifts, xs, w_now, acc[0], st, qscale, cos_own, sin_own)
        far = swap(msg)
        out = jax.ShapeDtypeStruct((count, HD), BF16)
        queries, payload, scale = call(
            lambda *r: token_kernel(d, *r),
            (out, out, jax.ShapeDtypeStruct((count // HD, HD), F32)),
            info,
            mine,
            far,
            st,
            hidden,
            gain,
            qscale,
            cos_far,
            sin_far,
        )
        keys, values = call(
            head_kernel, (out, out), order, kvr, scratch=[pltpu.VMEM((2, HD, half), F32)]
        )
        return queries, keys, values, payload, scale.reshape(count)

    return jax.shard_map(
        body,
        mesh=mesh,
        in_specs=(P("grp", "tp"), P("tp"), P("grp"), P(None, "tp"), P("tp", None), P("tp")),
        out_specs=(P("grp", "tp"), P("grp", "tp"), P("grp", "tp"), P("grp", "tp"), P("grp")),
        check_vma=False,
    )
```

```python
import math

import jax
import jax.numpy as jnp
from jax import lax
from jax.experimental import pallas as pl
from jax.experimental.pallas import tpu as pltpu
from jax.sharding import PartitionSpec as P


HD = 128
KV_COLS_DEV = 8
norm_eps = 1e-05
tiny_eps = 1e-06
rope_base = 500000.0

VMEM = 24 * 2**20
RING_VMEM = 48 * 2**20

F32 = jnp.float32
BF16 = jnp.bfloat16
STAT = 16


def split2(v):
    hi = v.astype(BF16)
    return hi, (v - hi.astype(F32)).astype(BF16)


def prep_kernel(core, hidden, gain, keep, send):
    half = keep.shape[0] - STAT
    for out, which in ((keep, core[0]), (send, 1 - core[0])):
        h = hidden[pl.ds(pl.multiple_of(which * half, half), half), :].astype(F32)
        weighted = h * gain[...]
        out[:half, :] = weighted.astype(BF16)
        squares = jnp.sum(jnp.transpose(h * h), axis=0, keepdims=True)
        largest = jnp.max(jnp.transpose(jnp.abs(weighted)), axis=0, keepdims=True)
        rows = []
        for v in (squares, largest):
            for part in split2(v):
                part = part.astype(F32)
                rows += [part[:, :128], part[:, 128:]]
        rows.append(jnp.zeros((STAT - len(rows), 128), F32))
        out[half:, :] = jnp.concatenate(rows, axis=0).astype(BF16)


def combine_kernel(core, keep, recv, out):
    half = keep.shape[0] - STAT
    first = core[0] == 0
    mine, other = keep[:half, :], recv[:half, :]
    left = jnp.where(first, mine.astype(F32), other.astype(F32)).astype(BF16)
    right = jnp.where(first, other.astype(F32), mine.astype(F32)).astype(BF16)
    a, b = keep[half:, :].astype(F32), recv[half:, :].astype(F32)

    def wide(s, r):
        return jnp.concatenate([s[r : r + 1], s[r + 1 : r + 2]], axis=1)

    squares = (wide(a, 0) + wide(a, 2)) + (wide(b, 0) + wide(b, 2))
    largest = jnp.maximum(wide(a, 4) + wide(a, 6), wide(b, 4) + wide(b, 6))
    rows = [p.astype(F32) for v in (squares, largest) for p in split2(v)]
    rows.append(jnp.zeros((STAT - len(rows), rows[0].shape[1]), F32))
    stats = jnp.concatenate(rows, axis=0).astype(BF16)
    for s in range(out.shape[0]):
        out[s, :half, :128] = left
        out[s, :half, 128:] = right
        out[s, half:, :] = stats


def block_at(core, i, side):
    return jnp.where(core == 0, i, (i % side) * side + i // side)


def weights_kernel(info, wq, wo, w_all, w_buf, sems):
    n = w_buf.shape[0]
    hw = wq.shape[2]
    side = math.isqrt(n)

    def fetches(i):
        b = block_at(info[0], i, side)
        return (
            pltpu.make_async_copy(wq.at[b], w_buf.at[i, :, pl.ds(0, hw)], sems.at[0, i]),
            pltpu.make_async_copy(wo.at[b], w_buf.at[i, :, pl.ds(hw, hw)], sems.at[1, i]),
        )

    def store(i):
        return pltpu.make_async_copy(w_buf.at[i], w_all.at[i], sems.at[2, i])

    @pl.loop(0, n)
    def _(i):
        for c in fetches(i):
            c.start()

    @pl.loop(0, n)
    def _(i):
        for c in fetches(i):
            c.wait()
        store(i).start()

    @pl.loop(0, n)
    def _(i):
        store(i).wait()


def arrange_weights(info, wq, wo):
    n, kb, hw = wq.shape
    hbm = pl.BlockSpec(memory_space=pltpu.HBM)
    out = jax.ShapeDtypeStruct((n, kb, 2 * hw), BF16)
    return pl.pallas_call(
        weights_kernel,
        out_shape=out,
        in_specs=[pl.BlockSpec(memory_space=pltpu.SMEM), hbm, hbm],
        out_specs=hbm,
        scratch_shapes=[pltpu.VMEM(out.shape, out.dtype), pltpu.SemaphoreType.DMA((3, n))],
        compiler_params=pltpu.CompilerParams(vmem_limit_bytes=60 * 2**20),
        cost_estimate=pl.CostEstimate(flops=10**9, bytes_accessed=2 * 10**7, transcendentals=0),
    )(info, wq, wo)


def kv_weights_kernel(core, kv, ko, kv_all):
    n, rows2, kb = kv_all.shape
    rows = rows2 // 2
    side = math.isqrt(n)
    for i in range(n):
        at = pl.ds(pl.multiple_of(block_at(core[0], i, side) * kb, kb), kb)
        kv_all[i, :rows, :] = kv[:, at]
        kv_all[i, rows:, :] = ko[:, at]


def kv_scale_kernel(core, kvs, kos, kvscale):
    rows = kvs.shape[1]
    width = kvscale.shape[1]

    def scales(ref):
        shape = (rows, rows)
        diagonal = lax.broadcasted_iota(jnp.int32, shape, 0) == lax.broadcasted_iota(
            jnp.int32, shape, 1
        )
        column = jnp.sum(
            jnp.where(diagonal, jnp.broadcast_to(ref[...], shape), 0.0), axis=1, keepdims=True
        )
        return jnp.broadcast_to(column, (rows, width))

    m, o = scales(kvs), scales(kos)
    first = core[0] == 0
    k = rows // 2
    for j, (lo, hi) in enumerate(((0, k), (k, 2 * k))):
        a, b = m[lo:hi], o[lo:hi]
        kvscale[2 * j * k : (2 * j + 1) * k, :] = jnp.where(first, a, b)
        kvscale[(2 * j + 1) * k : (2 * j + 2) * k, :] = jnp.where(first, b, a)


def high_kernel(gathered, high):
    side = gathered.shape[0]
    begin, n = parts(side)[1]
    half = gathered.shape[1] - STAT
    squares, largest = 0.0, 0.0
    for i in range(side):
        s = gathered[i, half:, :].astype(F32)
        squares = squares + (s[0:1] + s[1:2])
        largest = jnp.maximum(largest, s[2:3] + s[3:4])
        if i >= begin:
            high[(i - begin) * half : (i - begin + 1) * half, :] = gathered[i, :half, :]
    rows = [p.astype(F32) for v in (squares, largest) for p in split2(v)]
    rows.append(jnp.zeros((STAT - len(rows), rows[0].shape[1]), F32))
    high[n * half :, :] = jnp.concatenate(rows, axis=0).astype(BF16)


def kv_rows(xs, kvs, kv_in, st_in):
    half = kv_in.shape[1]
    total = kv_in[...]
    squares, largest = st_in[0:1, :], st_in[1:2, :]
    for x, w in zip(xs, kvs):
        n = len(w)
        for i in range(n):
            total = total + lax.dot_general(
                w[i],
                x[i * half : (i + 1) * half, :],
                (((1,), (1,)), ((), ())),
                preferred_element_type=F32,
            )
        if x.shape[0] > n * half:
            s = x[n * half :, :].astype(F32)
            squares = squares + (s[0:1] + s[1:2])
            largest = jnp.maximum(largest, s[2:3] + s[3:4])
    return total, squares, largest


def q_sum(xs, ws, q_in):
    half = q_in.shape[0]
    total = q_in[...]
    for x, w in zip(xs, ws):
        for i in range(len(w)):
            total = total + jnp.dot(
                x[i * half : (i + 1) * half, :],
                w[i],
                preferred_element_type=F32,
            )
    return total


def parts(side):
    low = side * 5 // 8
    return ((0, low), (low, side - low))


def places_of(info, shifts, side):
    found = []
    for s, k in shifts:
        first, n = parts(side)[k]
        found.append((lax.rem(info[1] + (side - s % side), side) * side + first, n))
    return found


def blocks_from(info, shifts, whole):
    side = math.isqrt(whole.shape[0])
    return [[whole[p + j] for j in range(n)] for p, n in places_of(info, shifts, side)]


def fetch(info, shifts, w_all, w_buf, sems):
    copies, at = [], 0
    for i, (p, n) in enumerate(places_of(info, shifts, math.isqrt(w_all.shape[0]))):
        copies.append(
            pltpu.make_async_copy(w_all.at[pl.ds(p, n)], w_buf.at[pl.ds(at, n)], sems.at[i])
        )
        at += n
    for c in copies:
        c.start()
    return copies


def weights_of(shifts, side, w_now):
    found, at = [], 0
    for _, k in shifts:
        n = parts(side)[k][1]
        found.append([w_now[at + j] for j in range(n)])
        at += n
    return found


def blocks_in(shifts, side):
    return sum(parts(side)[k][1] for _, k in shifts)


def ahead_kernel(shifts, info, w_all, w_next, sems):
    for c in fetch(info, shifts, w_all, w_next, sems):
        c.wait()


def first_weights(info, shifts, w_all):
    m = len(shifts)
    n = blocks_in(shifts, math.isqrt(w_all.shape[0]))
    hbm = pl.BlockSpec(memory_space=pltpu.HBM)
    return pl.pallas_call(
        lambda *refs: ahead_kernel(shifts, *refs),
        out_shape=jax.ShapeDtypeStruct((n,) + w_all.shape[1:], BF16),
        in_specs=[pl.BlockSpec(memory_space=pltpu.SMEM), hbm],
        out_specs=pl.BlockSpec(memory_space=pltpu.VMEM),
        scratch_shapes=[pltpu.SemaphoreType.DMA((m,))],
        compiler_params=pltpu.CompilerParams(vmem_limit_bytes=RING_VMEM),
        cost_estimate=pl.CostEstimate(flops=10**8, bytes_accessed=10**6, transcendentals=0),
    )(info, w_all)


def matmul_kernel(shifts, next_shifts, info, *refs):
    m = len(shifts)
    xs, w_now, w_all, kv_all = refs[:m], *refs[m : m + 3]
    q_out, kv_out, st_out, w_next, sems = refs[-5:]
    copies = fetch(info, next_shifts, w_all, w_next, sems)
    if len(refs) == m + 8:
        q_in, kv_in, st_in = q_out, kv_out, st_out
        for out in (q_out, kv_out, st_out):
            out[...] = jnp.zeros_like(out)
    else:
        q_in, kv_in, st_in = refs[m + 3 : m + 6]
    kvs = blocks_from(info, shifts, kv_all)
    total, squares, largest = kv_rows(xs, kvs, kv_in, st_in)
    kv_out[...] = total
    st_out[0:1, :] = squares
    st_out[1:2, :] = largest
    q_out[...] = q_sum(xs, weights_of(shifts, math.isqrt(w_all.shape[0]), w_now), q_in)
    for c in copies:
        c.wait()


def arrivals_call(kernel, out_shape, info, xs, hbm_args, rest, flops, aliases=None, scratch=()):
    vmem = pl.BlockSpec(memory_space=pltpu.VMEM)
    smem = pl.BlockSpec(memory_space=pltpu.SMEM)
    hbm = pl.BlockSpec(memory_space=pltpu.HBM)
    return pl.pallas_call(
        kernel,
        out_shape=out_shape,
        in_specs=[smem] + [vmem] * len(xs) + [hbm] * len(hbm_args) + [vmem] * len(rest),
        out_specs=tuple(vmem for _ in out_shape),
        scratch_shapes=list(scratch),
        input_output_aliases=aliases or {},
        compiler_params=pltpu.CompilerParams(vmem_limit_bytes=RING_VMEM),
        cost_estimate=pl.CostEstimate(flops=flops, bytes_accessed=10**6, transcendentals=0),
    )(info, *xs, *hbm_args, *rest)


def matmul(half, info, shifts, next_shifts, xs, w_now, w_all, kv_all, acc):
    m = len(xs)
    out_shape = (
        jax.ShapeDtypeStruct((half, w_all.shape[2]), F32),
        jax.ShapeDtypeStruct((kv_all.shape[1], half), F32),
        jax.ShapeDtypeStruct((8, half), F32),
        jax.ShapeDtypeStruct(
            (blocks_in(next_shifts, math.isqrt(w_all.shape[0])),) + w_now.shape[1:], w_now.dtype
        ),
    )
    return arrivals_call(
        lambda *refs: matmul_kernel(shifts, next_shifts, *refs),
        out_shape,
        info,
        [*xs, w_now],
        [w_all],
        [kv_all, *acc],
        2 * w_now.shape[0] * w_now.shape[1] * half * 288,
        {4 + m + i: i for i in range(len(acc))},
        [pltpu.SemaphoreType.DMA((len(next_shifts),))],
    )


def last_kv_kernel(d, shifts, info, *refs):
    m = len(shifts)
    xs, kv_all = refs[:m], refs[m]
    kv_in, st_in, kvscale, kcos, ksin, kvt, st_out = refs[m + 1 :]
    kvs = blocks_from(info, shifts, kv_all)
    t, squares, largest = kv_rows(xs, kvs, kv_in, st_in)
    st_out[0:1, :] = squares
    st_out[1:2, :] = largest
    t = t * (1.0 / jnp.sqrt(squares / d + norm_eps))
    first = info[0] == 0
    mk, mv, ok, ov = t[0:8], t[8:16], t[16:24], t[24:32]
    a = jnp.concatenate([jnp.where(first, mk, ok), jnp.where(first, ok, mk)], axis=0)
    b = jnp.concatenate([jnp.where(first, mv, ov), jnp.where(first, ov, mv)], axis=0)
    a = a * kvscale[:16, :]
    b = b * kvscale[16:, :]
    row = lax.broadcasted_iota(jnp.int32, a.shape, 0)
    swapped = jnp.where(row % 2 == 0, -pltpu.roll(a, a.shape[0] - 1, 0), pltpu.roll(a, 1, 0))
    a = a * kcos[...] + swapped * ksin[...]
    both = jnp.concatenate([a, b], axis=0).astype(BF16)
    for s in range(kvt.shape[0]):
        kvt[s] = both


def last_kv(d, copies, info, shifts, xs, kv_all, kv, st, kvscale, kcos, ksin):
    out_shape = (
        jax.ShapeDtypeStruct((copies,) + kv.shape, BF16),
        jax.ShapeDtypeStruct(st.shape, F32),
    )
    return arrivals_call(
        lambda *refs: last_kv_kernel(d, shifts, *refs),
        out_shape,
        info,
        xs,
        [],
        [kv_all, kv, st, kvscale, kcos, ksin],
        10**9,
    )


def last_q_kernel(d, side, shifts, info, *refs):
    m = len(shifts)
    xs, w_now = refs[:m], refs[m]
    q_in, st, wscale, cosine, sine, mine, msg = refs[m + 1 :]
    q = q_sum(xs, weights_of(shifts, side, w_now), q_in)
    half = q.shape[0]
    squares, largest = st[0:1, :], st[1:2, :]
    inv = columns_of(1.0 / jnp.sqrt(squares / d + norm_eps), 128)
    mine[...] = turn(q[:, :128] * inv * wscale[...], cosine[...], sine[...]).astype(BF16)
    msg[:half, :] = q[:, 128:] * inv
    msg[half:, :] = jnp.concatenate(
        [
            squares[:, :128],
            squares[:, 128:],
            largest[:, :128],
            largest[:, 128:],
            jnp.zeros((4, 128), F32),
        ],
        axis=0,
    )


def last_q(d, side, info, shifts, xs, w_now, q, st, wscale, cosine, sine):
    half = q.shape[0]
    out_shape = (
        jax.ShapeDtypeStruct((half, HD), BF16),
        jax.ShapeDtypeStruct((half + 8, HD), F32),
    )
    return arrivals_call(
        lambda *refs: last_q_kernel(d, side, shifts, *refs),
        out_shape,
        info,
        [*xs, w_now],
        [],
        [q, st, wscale, cosine, sine],
        10**9,
    )


def turn(v, cosine, sine):
    lane = lax.broadcasted_iota(jnp.int32, v.shape, 1)
    width = v.shape[1]
    swapped = jnp.where(
        lane % 2 == 0, -pltpu.roll(v, width - 1, 1), pltpu.roll(v, 1, 1)
    )
    return v * cosine + swapped * sine


def columns_of(row, width):
    return jnp.transpose(jnp.broadcast_to(row, (width, row.shape[1])))


def token_kernel(d, core, mine, msg, st, hidden, gain, wscale, cosine, sine, queries, payload, scale):
    half = mine.shape[0]
    c = core[0]
    own = pl.ds(pl.multiple_of(c * half, half), half)
    far = pl.ds(pl.multiple_of((1 - c) * half, half), half)
    queries[own, :] = mine[...]
    queries[far, :] = turn(msg[:half, :] * wscale[...], cosine[...], sine[...]).astype(BF16)
    wide = lambda r: jnp.concatenate(
        [msg[half + r : half + r + 1], msg[half + r + 1 : half + r + 2]], axis=1
    )
    for rows, squares, largest, place in (
        (own, st[0:1, :], st[1:2, :], c),
        (far, wide(0), wide(2), 1 - c),
    ):
        inverse = 1.0 / jnp.sqrt(squares / d + norm_eps)
        row_scale = largest * inverse + tiny_eps
        scale[pl.ds(2 * place, 1), :] = row_scale[:, :128]
        scale[pl.ds(2 * place + 1, 1), :] = row_scale[:, 128:]
        inv = columns_of(inverse, 128)
        rs = columns_of(row_scale, 128)
        normed = hidden[rows, :].astype(F32) * gain[...] * inv
        payload[rows, :] = (normed / rs).astype(BF16)


def head_kernel(order, kvr, keys, values, whole):
    half = kvr.shape[2]
    chips = kvr.shape[0] // 2
    n = KV_COLS_DEV
    for part in range(2):
        at = slice(part * half, (part + 1) * half)
        for i in range(chips):
            rows = kvr[2 * i + part].astype(F32)
            for which in range(2):
                for slot in range(2):
                    to = pl.ds(pl.multiple_of(order[2 * i + slot] * n, n), n)
                    lo = (2 * which + slot) * n
                    whole[which, to, :] = rows[lo : lo + n]
        for which, out in enumerate((keys, values)):
            out[at, :] = jnp.transpose(whole[which]).astype(BF16)


def call(kernel, out_shape, core, *args, flops=0, scratch=()):
    return pl.pallas_call(
        kernel,
        out_shape=out_shape,
        in_specs=[pl.BlockSpec(memory_space=pltpu.SMEM)]
        + [pl.BlockSpec(memory_space=pltpu.VMEM)] * len(args),
        scratch_shapes=list(scratch),
        compiler_params=pltpu.CompilerParams(vmem_limit_bytes=VMEM),
        cost_estimate=pl.CostEstimate(flops=flops or 10**8, bytes_accessed=10**6, transcendentals=0),
    )(core, *args)


def solution(mesh):
    tp = mesh.shape["tp"]
    side = math.isqrt(tp // 2)
    row = 2 * side

    def index(y, x, c):
        return (y % side) * row + (x % side) * 2 + c

    everyone = [(y, x, c) for y in range(side) for x in range(side) for c in range(2)]
    to_partner = [(index(y, x, c), index(y, x, 1 - c)) for y, x, c in everyone]
    heads = tp * KV_COLS_DEV // HD
    columns = side // 2

    def home(j):
        y, x = j // row, (j // 2) % side
        return index(j % heads, x - 1 + (y + x) % columns, y // columns)

    to_row = [(j, home(j)) for j in range(tp)]
    first_groups = [[index(y, x, 0) for x in range(side)] for y in range(side)]
    first_groups += [[index(y, x, 1) for y in range(side)] for x in range(side)]
    rows = [[y * row + i for i in range(row)] for y in range(side)]

    def second(v, s):
        pairs = [
            (index(y, x, c), index(y + s, x, c) if c == 0 else index(y, x + s, c))
            for y, x, c in everyone
        ]
        return lax.ppermute(v, "tp", pairs)

    def swap(v):
        return lax.ppermute(v, "tp", to_partner)

    def body(hidden, norm_gain, prefix, w_query, w_kv, w_scale):
        count, width = hidden.shape
        d = width * tp
        half = count // 2
        me = lax.axis_index("tp")
        core = me % 2
        x = (me // 2) % side
        y = me // row
        core1 = core[None].astype(jnp.int32)
        gain = norm_gain[None, :]

        def piece_at(xs, slot):
            base = y // 2
            h = jnp.where((xs - base + 1) % side < columns, 0, 1)
            source = base + columns * h
            o = (xs - source + 1) % side
            return 2 * ((o - source) % columns + columns * slot) + h

        blk = jax.ShapeDtypeStruct((half + STAT, width), BF16)
        keep, send = call(prep_kernel, (blk, blk), core1, hidden, gain)
        recv = swap(send)
        kv_mine = lax.ppermute(w_kv, "tp", to_row)
        kvs_mine = lax.ppermute(w_scale[None, HD:], "tp", to_row)
        wq_other = swap(w_query)
        slots = call(
            combine_kernel,
            jax.ShapeDtypeStruct((side, half + STAT, 2 * width), BF16),
            core1,
            keep,
            recv,
        )
        gathered = lax.all_to_all(
            slots, "tp", split_axis=0, concat_axis=0, tiled=False, axis_index_groups=first_groups
        )
        positions = (prefix[0] + jnp.arange(count, dtype=jnp.int32)).astype(F32)
        pos_own = lax.dynamic_slice_in_dim(positions, core * half, half)
        pos_far = lax.dynamic_slice_in_dim(positions, (1 - core) * half, half)

        def freq(columns):
            pair = (columns % HD // 2).astype(F32)
            return jnp.power(F32(rope_base), -(2.0 * pair) / HD)

        fq = freq(jnp.arange(HD, dtype=jnp.int32))
        ang_own = pos_own[:, None] * fq[None, :]
        ang_far = pos_far[:, None] * fq[None, :]
        slots_of = jnp.arange(2 * KV_COLS_DEV, dtype=jnp.int32)
        fk = freq(piece_at(x, slots_of // KV_COLS_DEV) * KV_COLS_DEV + slots_of % KV_COLS_DEV)
        seats = jnp.arange(row, dtype=jnp.int32)
        order = piece_at(seats // 2, seats % 2).astype(jnp.int32)
        ang_k = fk[:, None] * pos_own[None, :]
        qscale = w_scale[None, :HD]
        tables = (
            jnp.cos(ang_own),
            jnp.sin(ang_own),
            jnp.cos(ang_far),
            jnp.sin(ang_far),
            jnp.cos(ang_k),
            jnp.sin(ang_k),
        )
        coord = jnp.where(core == 0, y, x)

        info = jnp.stack([core, coord]).astype(jnp.int32)
        w_all = arrange_weights(
            info, w_query.reshape(-1, 2 * width, HD), wq_other.reshape(-1, 2 * width, HD)
        )
        w_now = first_weights(info, [(0, 0), (0, 1)], w_all)
        gathered, w_all, w_now, tables, info, order, qscale = lax.optimization_barrier(
            (gathered, w_all, w_now, tables, info, order, qscale)
        )
        cos_own, sin_own, cos_far, sin_far, cos_k, sin_k = tables

        (_, n_low), (_, n_high) = parts(side)
        low = gathered[:n_low, :half].reshape(n_low * half, -1)
        high = pl.pallas_call(
            high_kernel,
            out_shape=jax.ShapeDtypeStruct((n_high * half + STAT, gathered.shape[2]), BF16),
            compiler_params=pltpu.CompilerParams(vmem_limit_bytes=VMEM),
            cost_estimate=pl.CostEstimate(flops=10**8, bytes_accessed=10**6, transcendentals=0),
        )(gathered)

        last_round = side // 2
        plan = [[(0, 0), (0, 1)]]
        plan += [[(r, k), (-r, k)] for r in range(1, last_round) for k in range(2)]
        plan += [[(last_round, 0), (-last_round, 1)]]

        def mm(at, acc, w_now, xs):
            *acc, w_next = matmul(
                half, info, plan[at], plan[at + 1], xs, w_now, w_all, kv_all, acc
            )
            return acc, w_next

        up, down = [second(low, 1)], [second(low, -1)]
        up.append(second(high, 1))
        down.append(second(high, -1))
        kv_other = swap(kv_mine)
        kv_all = call(
            kv_weights_kernel,
            jax.ShapeDtypeStruct((d // (2 * width), 4 * KV_COLS_DEV, 2 * width), BF16),
            info,
            kv_mine,
            kv_other,
        )
        acc, w_now = mm(0, (), w_now, [low, high])
        at = 1
        for r in range(1, last_round):
            for k in range(2):
                xs = [up[k], down[k]]
                up[k], down[k], acc = lax.optimization_barrier((up[k], down[k], acc))
                if r + 1 < last_round:
                    up[k], down[k] = second(up[k], 1), second(down[k], -1)
                elif k == 0:
                    up[k] = second(up[k], 1)
                else:
                    down[k] = second(down[k], -1)
                acc, w_now = mm(at, acc, w_now, xs)
                at += 1
        xs = [up[0], down[1]]
        shifts = plan[-1]
        kvs_other = swap(kvs_mine)
        kvscale = call(
            kv_scale_kernel,
            jax.ShapeDtypeStruct((4 * KV_COLS_DEV, half), F32),
            info,
            kvs_mine,
            kvs_other,
        )
        kvt, st = last_kv(
            d, row, info, shifts, xs, kv_all, acc[1], acc[2], kvscale, cos_k, sin_k
        )
        kvr = lax.all_to_all(
            kvt, "tp", split_axis=0, concat_axis=0, tiled=False, axis_index_groups=rows
        )
        mine, msg = last_q(d, side, info, shifts, xs, w_now, acc[0], st, qscale, cos_own, sin_own)
        far = swap(msg)
        out = jax.ShapeDtypeStruct((count, HD), BF16)
        queries, payload, scale = call(
            lambda *r: token_kernel(d, *r),
            (out, out, jax.ShapeDtypeStruct((count // HD, HD), F32)),
            info,
            mine,
            far,
            st,
            hidden,
            gain,
            qscale,
            cos_far,
            sin_far,
        )
        keys, values = call(
            head_kernel, (out, out), order, kvr, scratch=[pltpu.VMEM((2, HD, half), F32)]
        )
        return queries, keys, values, payload, scale.reshape(count)

    return jax.shard_map(
        body,
        mesh=mesh,
        in_specs=(P("grp", "tp"), P("tp"), P("grp"), P(None, "tp"), P("tp", None), P("tp")),
        out_specs=(P("grp", "tp"), P("grp", "tp"), P("grp", "tp"), P("grp", "tp"), P("grp")),
        check_vma=False,
    )
```
